32 devices in a mesh: frame: 4 (over x, core), seq: 8 (over z, y).
Axes of the slice: x: 2, y: 2, z: 4, core: 2. Of those that a mesh axis runs over, the one named last changes fastest.
Arguments:
- vit_states: bfloat16 [64, 256, 1280], P(('frame', 'seq')), may hold values from -6 to 6
- frame_slot: int32 [32], replicated, may hold values from 0 to 63, as said below
- patch_count: int32 [32], replicated, may hold values from 208 to 256, as said below
- vis_start: int32 [32], replicated, may hold values from 0 to 4095, as said below
- text_embed: bfloat16 [128, 32, 4096], P(None, ('frame', 'seq')), may hold values from -6 to 6
- vit_ln_gain: float32 [1280], replicated, may hold values from 0.25 to 1.75
- vit_ln_bias: float32 [1280], replicated, may hold values from -1.5 to 1.5
- vit_qkv_w: bfloat16 [1280, 3840], P('seq'), may hold values from -0.15625 to 0.15625
- vit_qkv_b: float32 [3840], replicated, may hold values from -1.5 to 1.5
- vit_out_w: bfloat16 [1280, 1280], P('seq'), may hold values from -0.15625 to 0.15625
- vit_out_b: float32 [1280], replicated, may hold values from -1.5 to 1.5
- proj_w: bfloat16 [1280, 4096], replicated, may hold values from -0.15625 to 0.15625
- proj_b: float32 [4096], replicated, may hold values from -1.5 to 1.5
- attn_gain: float32 [4096], replicated, may hold values from 0.25 to 1.75
- wq: bfloat16 [4096, 2048], P(None, 'frame'), may hold values from -0.09375 to 0.09375
- wk: bfloat16 [4096, 1024], P(None, 'frame'), may hold values from -0.09375 to 0.09375
- wv: bfloat16 [4096, 1024], P(None, 'frame'), may hold values from -0.09375 to 0.09375
- wo: bfloat16 [2048, 4096], P('frame'), may hold values from -0.125 to 0.125
Outputs:
- mixed: bfloat16 [128, 32, 4096], P(None, ('frame', 'seq'))
The draws below stay inside these ranges and needn't reach their ends.
Inputs may be any that keep to these rules, and one draw needn't show every extreme that they name: Frame t sits in slot frame_slot[t]; slot k of the device with index d (axes frame then seq) is d * 2 + k; no slot holds two frames. The two devices with frame indices 2i and 2i+1 and the same seq index hold exactly two frames between them; some device holds 2 frames. `patch_count`: A multiple of 4; some frame has 256 patches. Frame t's patch_count[t] / 4 visual positions start at vis_start[t] and lie within positions t * 128 to (t + 1) * 128 - 1.
All inputs are finite; a program needn't handle non-finite values.
Results may differ from the reference program's by a relative error of at most 0.015.
Values may be sent and summed in bfloat16 or wider, within the bound.
A program may use at most 128 MiB of HBM per device.

```python
import math
import jax
import jax.numpy as jnp
from jax import lax

VW = 1280
VHEADS = 16
MODEL_WIDTH = 4096
QUERY_HEADS_HALF = 16
KEY_VALUE_HEADS = 8
HEAD_WIDTH = 128
FRAME_MAX = 256
SLOTS = 2
TOK_OWN = 128
VIS_MAX = 64
N_FRAME = 4
N_SEQ = 8
DEVICES = 32


def frame_spans(key):
    inner_key = jax.random.fold_in(key, 5)
    count_key, place_key = jax.random.split(inner_key)
    lowest = VIS_MAX - VIS_MAX // 5
    tokens = jax.random.randint(count_key, (DEVICES,), lowest, VIS_MAX + 1).astype(jnp.int32)
    tokens = tokens.at[0].set(VIS_MAX)
    spare = TOK_OWN - tokens
    offsets = jax.random.randint(place_key, (DEVICES,), 0, spare + 1).astype(jnp.int32)
    starts = jnp.arange(DEVICES).astype(jnp.int32) * TOK_OWN + offsets
    return (tokens * 4, starts)


def draw_patch_count(key, part):
    counts, starts = frame_spans(key)
    return counts


def draw_vis_start(key, part):
    counts, starts = frame_spans(key)
    return starts


def draw_frame_slot(key, part):
    pairs_n = DEVICES // 2
    order_key, slot_key = jax.random.split(jax.random.fold_in(key, 3))
    frames_perm = jax.random.permutation(order_key, DEVICES).astype(jnp.int32)
    scores = jax.random.randint(slot_key, (pairs_n, 4), 0, 1 << 20) * 4 + jnp.arange(4).astype(jnp.int32)[None, :]
    chosen = jnp.argsort(scores, axis=1)[:, :2].astype(jnp.int32)
    chosen = chosen.at[0].set(jnp.array([0, 1], jnp.int32))
    earlier_slot = jnp.min(chosen, axis=1)
    later_slot = jnp.max(chosen, axis=1)
    pair_ids = jnp.arange(pairs_n).astype(jnp.int32)
    low_device = pair_ids // N_SEQ * 2 * N_SEQ + pair_ids % N_SEQ
    first_slots = (low_device + earlier_slot // 2 * N_SEQ) * 2 + earlier_slot % 2
    second_slots = (low_device + later_slot // 2 * N_SEQ) * 2 + later_slot % 2
    result = jnp.zeros((DEVICES,), jnp.int32)
    result = result.at[frames_perm[0::2]].set(first_slots)
    result = result.at[frames_perm[1::2]].set(second_slots)
    return result


def level_of(own_key, dims, shards, smallest, largest):
    def one(position, shards_of):
        steps = jax.random.uniform(jax.random.fold_in(jax.random.fold_in(own_key, 6), position), (shards_of,), jnp.float32, smallest / len(shards), largest / len(shards))
        return jnp.repeat(jnp.exp(steps), dims[position] // shards_of).reshape((-1,) + (1,) * (len(dims) - position - 1))

    gain = one(*shards[0])
    for cut in shards[1:]:
        gain = gain * one(*cut)
    return gain


def normal_values(stream_key, extent, scale, limit, cuts=(), held_as=jnp.bfloat16):
    values = jax.random.normal(stream_key, extent, jnp.float32) * scale
    if len(cuts) > 0:
        values = level_of(stream_key, extent, cuts, -0.22, 0.18) * values
    return jnp.clip(values, min=-limit, max=limit).astype(held_as)


def setup_inputs(seed: int = 0) -> dict:
    key_list = jax.random.split(jax.random.key(seed), 19)
    return {
        "vit_states": normal_values(key_list[0], (DEVICES * SLOTS, FRAME_MAX, VW), 1.0, 6.0, ((0, 32),)),
        "frame_slot": draw_frame_slot(jax.random.fold_in(key_list[18], 71), 0),
        "patch_count": draw_patch_count(jax.random.fold_in(key_list[18], 71), 0),
        "vis_start": draw_vis_start(jax.random.fold_in(key_list[18], 71), 0),
        "text_embed": normal_values(key_list[4], (TOK_OWN, DEVICES, MODEL_WIDTH), 1.0, 6.0, ((1, 32),)),
        "vit_ln_gain": jnp.clip(1.0 + 0.15 * jax.random.normal(key_list[5], (VW,), jnp.float32), 0.25, 1.75),
        "vit_ln_bias": normal_values(key_list[6], (VW,), 0.3, 1.5, (), jnp.float32),
        "vit_qkv_w": normal_values(key_list[7], (VW, 3 * VW), VW ** -0.5, 0.15625, ((0, 8),)),
        "vit_qkv_b": normal_values(key_list[8], (3 * VW,), 0.3, 1.5, (), jnp.float32),
        "vit_out_w": normal_values(key_list[9], (VW, VW), VW ** -0.5, 0.15625, ((0, 8),)),
        "vit_out_b": normal_values(key_list[10], (VW,), 0.3, 1.5, (), jnp.float32),
        "proj_w": normal_values(key_list[11], (VW, MODEL_WIDTH), VW ** -0.5, 0.15625),
        "proj_b": normal_values(key_list[12], (MODEL_WIDTH,), 0.3, 1.5, (), jnp.float32),
        "attn_gain": jnp.clip(1.0 + 0.15 * jax.random.normal(key_list[13], (MODEL_WIDTH,), jnp.float32), 0.25, 1.75),
        "wq": normal_values(key_list[14], (MODEL_WIDTH, QUERY_HEADS_HALF * HEAD_WIDTH), MODEL_WIDTH ** -0.5, 0.09375, ((1, 4),)),
        "wk": normal_values(key_list[15], (MODEL_WIDTH, KEY_VALUE_HEADS * HEAD_WIDTH), MODEL_WIDTH ** -0.5, 0.09375, ((1, 4),)),
        "wv": normal_values(key_list[16], (MODEL_WIDTH, KEY_VALUE_HEADS * HEAD_WIDTH), MODEL_WIDTH ** -0.5, 0.09375, ((1, 4),)),
        "wo": normal_values(key_list[17], (QUERY_HEADS_HALF * HEAD_WIDTH, MODEL_WIDTH), (QUERY_HEADS_HALF * HEAD_WIDTH) ** -0.5, 0.125, ((0, 4),)),
    }


rope_theta = 500000.0
vit_epsilon = 1e-06
norm_epsilon = 1e-05
masked_score = -1e+30

def apply_rotary(values, rotary_angles):
    half_width = values.shape[-1] // 2
    first_half = values[..., :half_width]
    second_half = values[..., half_width:]
    cosine = jnp.cos(rotary_angles)
    sine_part = jnp.sin(rotary_angles)
    return jnp.concatenate([first_half * cosine - second_half * sine_part, second_half * cosine + first_half * sine_part], axis=-1)

def rope_angles(positions, head_size):
    exponents = jnp.arange(0, head_size, 2).astype(jnp.float32) / head_size
    inverse = jnp.power(jnp.float32(rope_theta), -exponents)
    return positions.astype(jnp.float32)[:, None] * inverse[None, :]

def vit_frame(states, patches, ln_gain, ln_bias, qkv_weight, qkv_bias, out_weight, out_bias):
    frame_max = states.shape[0]
    width_vit = states.shape[1]
    states_wide = states.astype(jnp.float32)
    average = lax.optimization_barrier(jnp.mean(states_wide, axis=1, keepdims=True))
    centred = states_wide - average
    spread = lax.optimization_barrier(jnp.mean(centred * centred, axis=1, keepdims=True))
    normed_states = (centred * lax.rsqrt(spread + vit_epsilon) * ln_gain + ln_bias).astype(jnp.bfloat16)
    projected = (jnp.dot(normed_states, qkv_weight, preferred_element_type=jnp.float32) + qkv_bias).astype(jnp.bfloat16)
    head_size = width_vit // VHEADS
    shaped = projected.reshape(frame_max, 3, VHEADS, head_size).astype(jnp.float32)
    scores = jnp.einsum('qhd,khd->hqk', shaped[:, 0], shaped[:, 1]) / math.sqrt(head_size)
    key_live = jnp.arange(frame_max).astype(jnp.int32) < patches
    scores = jnp.where(key_live[None, None, :], scores, masked_score)
    highest = lax.optimization_barrier(jnp.max(scores, axis=-1, keepdims=True))
    weights = jnp.exp(scores - highest)
    probabilities = (weights / lax.optimization_barrier(jnp.sum(weights, axis=-1, keepdims=True))).astype(jnp.bfloat16)
    context = jnp.einsum('hqk,khd->qhd', probabilities.astype(jnp.float32), shaped[:, 2]).astype(jnp.bfloat16)
    attended = jnp.dot(context.reshape(frame_max, width_vit), out_weight, preferred_element_type=jnp.float32)
    hidden = (states_wide + attended + out_bias).astype(jnp.bfloat16)
    return lax.optimization_barrier(jnp.mean(hidden.astype(jnp.float32).reshape(frame_max // 4, 4, width_vit), axis=1)).astype(jnp.bfloat16)

def reference(vit_states, frame_slot, patch_count, vis_start, text_embed, vit_ln_gain, vit_ln_bias, vit_qkv_w, vit_qkv_b, vit_out_w, vit_out_b, proj_w, proj_b, attn_gain, wq, wk, wv, wo):
    frame_states = vit_states[frame_slot]

    def encode(operands):
        states, patches = operands
        pooled = vit_frame(states, patches, vit_ln_gain, vit_ln_bias, vit_qkv_w, vit_qkv_b, vit_out_w, vit_out_b)
        return (jnp.dot(pooled, proj_w, preferred_element_type=jnp.float32) + proj_b).astype(jnp.bfloat16)
    visual = lax.map(encode, (frame_states, patch_count))
    sequence_length = TOK_OWN * DEVICES
    positions = jnp.arange(sequence_length).astype(jnp.int32)
    token_frame = positions // TOK_OWN
    within = positions - vis_start[token_frame]
    is_visual = (within >= 0) & (within < patch_count[token_frame] // 4)
    within_clip = jnp.clip(within, 0, VIS_MAX - 1)
    visual_rows = visual[token_frame, within_clip]
    merged = jnp.where(is_visual[:, None], visual_rows, text_embed.reshape(sequence_length, MODEL_WIDTH))
    merged_wide = merged.astype(jnp.float32)
    normed_states = (merged_wide * lax.rsqrt(lax.optimization_barrier(jnp.mean(merged_wide * merged_wide, axis=1, keepdims=True)) + norm_epsilon) * attn_gain).astype(jnp.bfloat16)
    rotary_angles = rope_angles(positions, HEAD_WIDTH)[:, None, :]
    query_matrix = apply_rotary(jnp.dot(normed_states, wq, preferred_element_type=jnp.float32).reshape(sequence_length, QUERY_HEADS_HALF, HEAD_WIDTH), rotary_angles).astype(jnp.bfloat16)
    keys_complete = apply_rotary(jnp.dot(normed_states, wk, preferred_element_type=jnp.float32).reshape(sequence_length, KEY_VALUE_HEADS, HEAD_WIDTH), rotary_angles).astype(jnp.bfloat16)
    values_complete = jnp.dot(normed_states, wv, preferred_element_type=jnp.float32).astype(jnp.bfloat16).reshape(sequence_length, KEY_VALUE_HEADS, HEAD_WIDTH)
    keys_wide = keys_complete.astype(jnp.float32)
    values_wide = values_complete.astype(jnp.float32)
    grouped_rows = query_matrix.reshape(sequence_length, KEY_VALUE_HEADS, QUERY_HEADS_HALF // KEY_VALUE_HEADS, HEAD_WIDTH)
    query_rows = 128

    def attend(block_index):
        offset = block_index * query_rows
        query_block = lax.dynamic_slice_in_dim(grouped_rows, offset, query_rows, 0).astype(jnp.float32)
        scores = jnp.einsum('qkgd,nkd->kgqn', query_block, keys_wide) / math.sqrt(HEAD_WIDTH)
        query_positions = offset + jnp.arange(query_rows).astype(jnp.int32)
        allowed = positions[None, :] <= query_positions[:, None]
        scores = jnp.where(allowed[None, None], scores, masked_score)
        highest = lax.optimization_barrier(jnp.max(scores, axis=-1, keepdims=True))
        weights = jnp.where(allowed[None, None], jnp.exp(scores - highest), 0.0)
        denominator = lax.optimization_barrier(jnp.sum(weights, axis=-1))
        numerator = jnp.einsum('kgqn,nkd->kgqd', weights.astype(jnp.bfloat16).astype(jnp.float32), values_wide)
        context_block = (numerator / denominator[..., None]).astype(jnp.bfloat16)
        return jnp.transpose(context_block, (2, 0, 1, 3)).reshape(query_rows, QUERY_HEADS_HALF * HEAD_WIDTH)
    context = lax.map(attend, jnp.arange(sequence_length // query_rows).astype(jnp.int32)).reshape(sequence_length, QUERY_HEADS_HALF * HEAD_WIDTH)
    group_width = QUERY_HEADS_HALF * HEAD_WIDTH // N_FRAME
    summed = jnp.zeros((sequence_length, MODEL_WIDTH), jnp.float32)
    for head_group in range(N_FRAME):
        columns = context[:, head_group * group_width:(head_group + 1) * group_width]
        partial_sum = jnp.dot(columns, wo[head_group * group_width:(head_group + 1) * group_width], preferred_element_type=jnp.float32)
        rounded = lax.optimization_barrier(partial_sum.astype(jnp.bfloat16))
        summed = summed + rounded.astype(jnp.float32)
    return summed.astype(jnp.bfloat16).reshape(TOK_OWN, DEVICES, MODEL_WIDTH)
```

```python
import functools
import math

import jax
import jax.numpy as jnp
from jax import lax
from jax.experimental import pallas as pl
from jax.experimental.layout import Layout, with_layout_constraint
from jax.experimental.pallas import tpu as pltpu
from jax.sharding import PartitionSpec as P

VHEADS = 16
HEAD_WIDTH = 128

rope_theta = 500000.0
vit_epsilon = 1e-06
norm_epsilon = 1e-05
masked_score = -1e30
LOG2E = math.log2(math.e)


def dot32(a, b):
    return jnp.dot(a, b, preferred_element_type=jnp.float32)


def from_relative(value, dx, dc):
    n = lax.axis_size("frame")
    chips = n // 2
    pairs = []
    for dst in range(n):
        src = ((dst // 2 + dx) % chips) * 2 + ((dst % 2) ^ dc)
        pairs.append((src, dst))
    return lax.ppermute(value, "frame", pairs)


def gather_relative(value):
    chips = lax.axis_size("frame") // 2
    out = []
    for dx in range(chips):
        same = value if dx == 0 else from_relative(value, dx, 0)
        out.append(same)
        out.append(from_relative(same, 0, 1))
    return out


def to_absolute(parts):
    n = len(parts)
    chips = n // 2
    me = lax.axis_index("frame")
    stack = jnp.stack(parts)
    out = []
    for g in range(n):
        dx = jnp.mod(g // 2 - me // 2, chips)
        dc = (g % 2) ^ (me % 2)
        out.append(lax.dynamic_index_in_dim(stack, dx * 2 + dc, 0, keepdims=False))
    return jnp.stack(out)


def ceil_to(value, step):
    return -(-value // step) * step


def vit_kernel(
    count_ref, x_ref, w_ref, gain_ref, shift_ref, qb_ref, ctx_ref, pst_ref, *, heads, head_size
):
    frame = pl.program_id(0)
    frames = pl.num_programs(0)
    me = lax.axis_index("frame")
    rows, width = x_ref.shape[1], x_ref.shape[2]
    cols = heads * head_size
    out_rows = ctx_ref.shape[1]
    states = x_ref[0]
    wide = states.astype(jnp.float32)
    average = jnp.mean(wide, axis=1, keepdims=True)
    centred = wide - average
    spread = jnp.mean(centred * centred, axis=1, keepdims=True)
    normed = centred * lax.rsqrt(spread + vit_epsilon) * gain_ref[...] + shift_ref[...]
    w = w_ref[:, : 3 * cols]
    proj = (dot32(normed.astype(jnp.bfloat16), w) + qb_ref[...]).astype(jnp.bfloat16)
    q, k, v = (proj[:, i * cols : (i + 1) * cols] for i in range(3))
    live = lax.broadcasted_iota(jnp.int32, (1, rows), 1) < count_ref[frame]
    blocks = [None] * pl.cdiv(cols, 128)
    scale = LOG2E / math.sqrt(head_size)
    for h in range(heads):
        low, high = h * head_size, (h + 1) * head_size
        start, stop = low // 128 * 128, min(ceil_to(high, 128), cols)
        lane = lax.broadcasted_iota(jnp.int32, (1, stop - start), 1) + start
        mine = jnp.where((lane >= low) & (lane < high), 1.0, 0.0).astype(jnp.bfloat16)
        s = lax.dot_general(
            q[:, start:stop] * mine,
            k[:, start:stop],
            (((1,), (1,)), ((), ())),
            preferred_element_type=jnp.float32,
        )
        s = jnp.where(live, s * scale, masked_score)
        e = jnp.exp2(s - jnp.max(s, axis=1, keepdims=True))
        p = (e * (1.0 / jnp.sum(e, axis=1, keepdims=True))).astype(jnp.bfloat16)
        o = dot32(p, v[:, start:stop] * mine)
        for b in range(start // 128, pl.cdiv(stop, 128)):
            part = o[:, b * 128 - start : min((b + 1) * 128, stop) - start]
            blocks[b] = part if blocks[b] is None else blocks[b] + part
    context = jnp.concatenate(blocks, axis=1).astype(jnp.bfloat16)
    pr = lax.broadcasted_iota(jnp.int32, (out_rows, rows), 0)
    pc = lax.broadcasted_iota(jnp.int32, (out_rows, rows), 1)
    pool = jnp.where(pc // 4 == pr, 0.25, 0.0).astype(jnp.bfloat16)
    ctx_ref[0] = dot32(pool, context).astype(jnp.bfloat16)
    pooled = dot32(pool, states)
    total = jnp.zeros((out_rows, cols), jnp.float32)
    for f in range(width // cols):
        total = total + jnp.where(me == f, 1.0, 0.0) * pooled[:, f * cols : (f + 1) * cols]
    pst_ref[0] = total


def vit_attention(counts, states, weights, gain, shift, qkv_bias, heads, head_size):
    frames, rows, width = states.shape
    cols = heads * head_size
    whole = lambda x: pl.BlockSpec(x.shape, lambda i: (0,) * x.ndim)
    out = pl.BlockSpec((1, rows // 4, cols), lambda i: (i, 0, 0))
    return pl.pallas_call(
        functools.partial(vit_kernel, heads=heads, head_size=head_size),
        grid=(frames,),
        in_specs=[
            pl.BlockSpec(memory_space=pltpu.SMEM),
            pl.BlockSpec((1, rows, width), lambda i: (i, 0, 0)),
            whole(weights),
            whole(gain),
            whole(shift),
            whole(qkv_bias),
        ],
        out_specs=[out, out],
        out_shape=[
            jax.ShapeDtypeStruct((frames, rows // 4, cols), jnp.bfloat16),
            jax.ShapeDtypeStruct((frames, rows // 4, cols), jnp.float32),
        ],
        compiler_params=pltpu.CompilerParams(vmem_limit_bytes=32 * 1024 * 1024),
        cost_estimate=pl.CostEstimate(
            flops=2 * frames * rows * width * 3 * cols,
            bytes_accessed=2 * states.size,
            transcendentals=frames * heads * rows * rows,
        ),
        name="vit_attention",
    )(counts, states, weights, gain, shift, qkv_bias)


MESH = pl.DeviceIdType.MESH


def remote(src, dst, send, recv, axis, index):
    return pltpu.make_async_remote_copy(
        src_ref=src,
        dst_ref=dst,
        send_sem=send,
        recv_sem=recv,
        device_id={axis: index},
        device_id_type=MESH,
    )


def frame_peers():
    frames = lax.axis_size("frame")
    me = lax.axis_index("frame")
    chips = frames // 2
    chip, core = me // 2, me % 2
    partner = chip * 2 + (1 - core)
    ahead = [((chip + dx) % chips) * 2 + core for dx in range(1, chips)]
    behind = [((chip + chips - dx) % chips) * 2 + core for dx in range(1, chips)]
    return me, partner, ahead, behind


def greet(barrier, axis, index):
    pl.semaphore_signal(barrier, inc=1, device_id={axis: index}, device_id_type=MESH)


class FrameSpread:
    def __init__(self, out_ref, sems):
        self.out = out_ref
        self.send, self.recv = sems
        self.me, self.partner, self.ahead, self.behind = frame_peers()
        self.started = []

    def go(self, src, slot, k, target):
        copy = remote(src, self.out.at[slot], self.send.at[k], self.recv.at[k], "frame", target)
        copy.start()
        self.started.append(copy)

    def arrived(self, slot, k):
        ref = self.out.at[slot]
        remote(ref, ref, self.send.at[k], self.recv.at[k], "frame", self.partner).wait_recv()

    def send_across(self, src):
        for i, target in enumerate(self.ahead):
            self.go(src, self.me, 1 + i, target)

    def send_partner(self, src):
        self.go(src, self.me, 0, self.partner)

    def forward(self):
        n = len(self.ahead)
        for i, source in enumerate(self.behind):
            self.arrived(source, 1 + i)
            self.go(self.out.at[source], source, 1 + n + i, self.partner)

    def finish(self, partner_sent=True):
        n = len(self.ahead)
        if partner_sent:
            self.arrived(self.partner, 0)
        for i, source in enumerate(self.behind):
            other = source + 1 - 2 * (self.me % 2)
            self.arrived(other, 1 + n + i)
        for copy in self.started:
            copy.wait_send()


def front_kernel(
    order_ref,
    w_ref,
    states_ref,
    text_ref,
    w_out,
    states_out,
    text_out,
    pair,
    local,
    pair_sems,
    state_sems_a,
    state_sems_b,
    text_sems_a,
    text_sems_b,
    *relay_sems,
    count,
):
    relay = SeqRelay(w_ref, w_out, relay_sems, count)
    states = FrameSpread(states_out, (state_sems_a, state_sems_b))
    text = FrameSpread(text_out, (text_sems_a, text_sems_b))
    me, partner, ahead, behind = frame_peers()
    barrier = pltpu.get_barrier_semaphore()
    relay.greet(barrier)
    for peer in [partner] + ahead:
        greet(barrier, "frame", peer)
    pl.semaphore_wait(barrier, relay.peers() + (1 + len(ahead)))
    swap = remote(states_ref, pair, pair_sems.at[0], pair_sems.at[1], "frame", partner)
    swap.start()
    relay.first()
    pltpu.make_async_copy(w_ref, w_out.at[relay.me], local.at[0]).start()
    pltpu.make_async_copy(text_ref, text_out.at[me], local.at[1]).start()
    swap.wait()
    core = me % 2
    slots = states_ref.shape[0]
    rows = states_ref.shape[1]
    step = math.gcd(rows, 32)
    keep = [
        [
            jnp.where(order_ref[j] == side * slots + k, 1.0, 0.0)
            for side in (core, 1 - core)
            for k in range(slots)
        ]
        for j in range(2)
    ]

    def choose(i, carry):
        at = pl.ds(pl.multiple_of(i * step, step), step)
        values = [states_ref[k, at].astype(jnp.float32) for k in range(slots)]
        values += [pair[k, at].astype(jnp.float32) for k in range(slots)]
        for j, slot in enumerate((me, partner)):
            total = keep[j][0] * values[0]
            for weight, value in zip(keep[j][1:], values[1:]):
                total = total + weight * value
            states_out[slot, at] = total.astype(states_out.dtype)
        return carry

    lax.fori_loop(0, rows // step, choose, 0)
    states.send_across(states_out.at[me])
    text.send_across(text_ref)
    text.send_partner(text_ref)
    for k in range(1, relay.length):
        relay.step(k)
    states.forward()
    text.forward()
    pltpu.make_async_copy(w_ref, w_out.at[relay.me], local.at[0]).wait()
    pltpu.make_async_copy(text_ref, text_out.at[me], local.at[1]).wait()
    states.finish(partner_sent=False)
    text.finish()
    relay.finish()


def relay_scratch(chunks):
    seqs = lax.axis_size("seq")
    length = seqs // 2 if seqs % 2 == 0 else seqs
    return [pltpu.SemaphoreType.DMA((chunks, length))] * 6


def front(orders, weights, states, text):
    seqs, frames = lax.axis_size("seq"), lax.axis_size("frame")
    vmem = pl.BlockSpec(memory_space=pltpu.VMEM)
    spread = [pltpu.SemaphoreType.DMA((max(1, frames - 1),))] * 4
    chunks = 2
    return pl.pallas_call(
        functools.partial(front_kernel, count=chunks),
        in_specs=[pl.BlockSpec(memory_space=pltpu.SMEM)] + [vmem] * 3,
        out_specs=[vmem] * 3,
        out_shape=[
            jax.ShapeDtypeStruct((seqs,) + weights.shape, weights.dtype),
            jax.ShapeDtypeStruct((frames,) + states.shape[1:], states.dtype),
            jax.ShapeDtypeStruct((frames,) + text.shape, text.dtype),
        ],
        scratch_shapes=[
            pltpu.VMEM(states.shape, states.dtype),
            pltpu.SemaphoreType.DMA((2,)),
            pltpu.SemaphoreType.DMA((2,)),
        ]
        + spread
        + relay_scratch(chunks),
        compiler_params=pltpu.CompilerParams(
            collective_id=1, has_side_effects=True, vmem_limit_bytes=36 * 1024 * 1024
        ),
        cost_estimate=pl.CostEstimate(
            flops=40_000_000_000, bytes_accessed=0, transcendentals=0
        ),
        name="front",
    )(orders, weights, states, text)


def route_kernel(
    start_ref,
    ctx_ref,
    pst_ref,
    w_ref,
    ob_ref,
    table_out,
    ctx_all,
    outgoing,
    local,
    ctx_sems_a,
    ctx_sems_b,
    table_sems_a,
    table_sems_b,
    seq_send,
    seq_recv,
    *,
    vis_max,
):
    frames, seqs = lax.axis_size("frame"), lax.axis_size("seq")
    seq = lax.axis_index("seq")
    me, partner, ahead, behind = frame_peers()
    cols = ctx_ref.shape[1]
    share = outgoing.shape[0] // seqs
    laps = share // frames
    barrier = pltpu.get_barrier_semaphore()
    for peer in [partner] + ahead:
        greet(barrier, "frame", peer)
    others = [(seq + d) % seqs for d in range(1, seqs)]
    for other in others:
        greet(barrier, "seq", other)
    pl.semaphore_wait(barrier, frames // 2 + seqs - 1)
    context = FrameSpread(ctx_all, (ctx_sems_a, ctx_sems_b))
    context.send_across(ctx_ref)
    context.send_partner(ctx_ref)
    pltpu.make_async_copy(ctx_ref, ctx_all.at[me], local.at[0]).start()

    rows = outgoing.shape[0]
    r = lax.broadcasted_iota(jnp.int32, (rows, 1), 0)
    dest, frame, lap = r // share, r // laps % frames, r % laps
    begin = jnp.zeros((rows, 1), jnp.int32)
    for f in range(frames):
        begin = begin + jnp.where(frame == f, start_ref[f], 0)
    token = (dest + seqs - begin % seqs) % seqs + lap * seqs + frame * vis_max
    c = lax.broadcasted_iota(jnp.int32, (1, frames * vis_max), 1)
    pick = jnp.where(token == c, 1.0, 0.0).astype(jnp.bfloat16)

    context.forward()
    pltpu.make_async_copy(ctx_ref, ctx_all.at[me], local.at[0]).wait()
    context.finish()
    total = pst_ref[...] + ob_ref[...]
    for f in range(frames):
        total = total + dot32(ctx_all[f], w_ref[f * cols : (f + 1) * cols, 3 * cols : 4 * cols])
    outgoing[...] = dot32(pick, total.astype(jnp.bfloat16)).astype(jnp.bfloat16)

    def part(index):
        return pl.ds(pl.multiple_of(index * share, share), share)

    mine = table_out.at[me]
    sends = []
    for d, other in enumerate(others):
        copy = remote(
            outgoing.at[part(other)],
            mine.at[part(seq)],
            seq_send.at[d],
            seq_recv.at[d],
            "seq",
            other,
        )
        copy.start()
        sends.append(copy)
    keep = pltpu.make_async_copy(outgoing.at[part(seq)], mine.at[part(seq)], local.at[1])
    keep.start()
    keep.wait()
    for d in range(seqs - 1):
        source = (seq + seqs - 1 - d) % seqs
        ref = mine.at[part(source)]
        remote(ref, ref, seq_send.at[d], seq_recv.at[d], "seq", source).wait_recv()
    table = FrameSpread(table_out, (table_sems_a, table_sems_b))
    table.send_across(mine)
    table.send_partner(mine)
    table.forward()
    table.finish()
    for copy in sends:
        copy.wait_send()


def route(starts, context, pooled_states, weights, out_bias, vis_max):
    frames, seqs = lax.axis_size("frame"), lax.axis_size("seq")
    cols = context.shape[1]
    rows = frames * vis_max
    vmem = pl.BlockSpec(memory_space=pltpu.VMEM)
    spread = [pltpu.SemaphoreType.DMA((max(1, frames - 1),))] * 4
    return pl.pallas_call(
        functools.partial(route_kernel, vis_max=vis_max),
        in_specs=[pl.BlockSpec(memory_space=pltpu.SMEM)] + [vmem] * 4,
        out_specs=vmem,
        out_shape=jax.ShapeDtypeStruct((frames, rows, cols), jnp.bfloat16),
        scratch_shapes=[
            pltpu.VMEM((frames, rows, cols), jnp.bfloat16),
            pltpu.VMEM((rows, cols), jnp.bfloat16),
            pltpu.SemaphoreType.DMA((2,)),
        ]
        + spread
        + [pltpu.SemaphoreType.DMA((seqs - 1,))] * 2,
        compiler_params=pltpu.CompilerParams(
            collective_id=2, has_side_effects=True, vmem_limit_bytes=24 * 1024 * 1024
        ),
        cost_estimate=pl.CostEstimate(
            flops=12_000_000_000, bytes_accessed=0, transcendentals=0
        ),
        name="route",
    )(starts, context, pooled_states, weights, out_bias)


def merge_kernel(
    begin_ref,
    length_ref,
    base_ref,
    table_ref,
    pw_ref,
    pb_ref,
    text_ref,
    gain_ref,
    wq_ref,
    wk_ref,
    wv_ref,
    cos_ref,
    sin_ref,
    q_ref,
    kv_ref,
    hot,
    visual_mask,
    merged,
    squares,
    acc,
    *,
    steps,
):
    j = pl.program_id(0)
    frames, seqs = lax.axis_size("frame"), lax.axis_size("seq")
    my_seq = lax.axis_index("seq")
    rows = acc.shape[0]
    own_rows = rows // frames
    cols = table_ref.shape[2]
    block = pb_ref.shape[1]
    model_width = steps * block
    head = HEAD_WIDTH

    @pl.when(j == 0)
    def _():
        i = lax.broadcasted_iota(jnp.int32, (rows, 1), 0)
        position = i % own_rows * (frames * seqs) + i // own_rows * seqs + my_seq
        t = lax.broadcasted_iota(jnp.int32, (1, begin_ref.shape[1]), 1)
        mine = position // own_rows == t

        def of_frame(ref):
            return jnp.sum(jnp.where(mine, ref[...], 0), axis=1, keepdims=True)

        within = position - of_frame(begin_ref)
        visual = (within >= 0) & (within < of_frame(length_ref))
        row = of_frame(base_ref) + jnp.maximum(within, 0) // seqs
        c = lax.broadcasted_iota(jnp.int32, (1, hot.shape[1]), 1)
        hot[...] = jnp.where(visual & (row == c), 1.0, 0.0).astype(jnp.bfloat16)
        visual_mask[...] = jnp.where(visual, 1.0, 0.0)
        squares[...] = jnp.zeros_like(squares)
        acc[...] = jnp.zeros_like(acc)

    @pl.when(j < steps)
    def _():
        total = pb_ref[...] + jnp.zeros((table_ref.shape[1], block), jnp.float32)
        for f in range(frames):
            total = total + dot32(table_ref[f], pw_ref[f * cols : (f + 1) * cols])
        fetched = dot32(hot[...], total.astype(jnp.bfloat16))
        text = text_ref[...].reshape(rows, block).astype(jnp.float32)
        value = jnp.where(visual_mask[...] > 0.5, fetched, text)
        squares[...] += jnp.sum(value * value, axis=1, keepdims=True)
        merged[j] = value.astype(jnp.bfloat16)

    @pl.when(j >= steps)
    def _():
        scale = lax.rsqrt(squares[...] * (1.0 / model_width) + norm_epsilon)
        normed = merged[j - steps].astype(jnp.float32) * scale * gain_ref[...]
        normed = normed.astype(jnp.bfloat16)
        qw, kw = wq_ref.shape[1], wk_ref.shape[1]
        acc[:, :qw] += dot32(normed, wq_ref[...])
        acc[:, qw : qw + kw] += dot32(normed, wk_ref[...])
        acc[:, qw + kw :] += dot32(normed, wv_ref[...])

    @pl.when(j == 2 * steps - 1)
    def _():
        qw, kw = wq_ref.shape[1], wk_ref.shape[1]
        cosine, sine = cos_ref[...], sin_ref[...]

        def turn(at, factor):
            x = acc[:, at : at + head]
            x = x * cosine + pltpu.roll(x, head // 2, 1) * sine
            return (x * factor if factor != 1.0 else x).astype(jnp.bfloat16)

        for h in range(qw // head):
            q_ref[:, h * head : (h + 1) * head] = turn(h * head, LOG2E / math.sqrt(head))
        for h in range(kw // head):
            kv_ref[:, h * head : (h + 1) * head] = turn(qw + h * head, 1.0)
        kv_ref[:, kw:] = acc[:, qw + kw :].astype(jnp.bfloat16)


def merge(begin, length, base, table, proj_w, proj_b, text, gain, wq, wk, wv, cosine, sine):
    frames, own_rows, model_width = text.shape
    rows = frames * own_rows
    block = math.gcd(model_width, 512)
    steps = model_width // block
    qw, kw = wq.shape[1], wk.shape[1]
    first = lambda j: jnp.minimum(j, steps - 1)
    second = lambda j: jnp.maximum(j - steps, 0)
    whole = lambda x: pl.BlockSpec(x.shape, lambda j: (0,) * x.ndim)
    return pl.pallas_call(
        functools.partial(merge_kernel, steps=steps),
        grid=(2 * steps,),
        in_specs=[
            whole(begin),
            whole(length),
            whole(base),
            whole(table),
            pl.BlockSpec((proj_w.shape[0], block), lambda j: (0, first(j))),
            pl.BlockSpec((1, block), lambda j: (0, first(j))),
            pl.BlockSpec((frames, own_rows, block), lambda j: (0, 0, first(j))),
            pl.BlockSpec((1, block), lambda j: (0, second(j))),
            pl.BlockSpec((block, qw), lambda j: (second(j), 0)),
            pl.BlockSpec((block, kw), lambda j: (second(j), 0)),
            pl.BlockSpec((block, kw), lambda j: (second(j), 0)),
            whole(cosine),
            whole(sine),
        ],
        out_specs=[
            pl.BlockSpec((rows, qw), lambda j: (0, 0)),
            pl.BlockSpec((rows, 2 * kw), lambda j: (0, 0)),
        ],
        out_shape=[
            jax.ShapeDtypeStruct((rows, qw), jnp.bfloat16),
            jax.ShapeDtypeStruct((rows, 2 * kw), jnp.bfloat16),
        ],
        scratch_shapes=[
            pltpu.VMEM((rows, table.shape[1]), jnp.bfloat16),
            pltpu.VMEM((rows, 1), jnp.float32),
            pltpu.VMEM((steps, rows, block), jnp.bfloat16),
            pltpu.VMEM((rows, 1), jnp.float32),
            pltpu.VMEM((rows, qw + 2 * kw), jnp.float32),
        ],
        compiler_params=pltpu.CompilerParams(vmem_limit_bytes=40 * 1024 * 1024),
        cost_estimate=pl.CostEstimate(
            flops=2 * rows * model_width * (qw + 2 * kw) + 2 * proj_w.size * table.shape[1],
            bytes_accessed=2 * proj_w.size + 2 * model_width * (qw + 2 * kw),
            transcendentals=0,
        ),
        name="merge",
    )(begin, length, base, table, proj_w, proj_b, text, gain, wq, wk, wv, cosine, sine)


def text_kernel(q_ref, kv_ref, o_ref, *, kv_heads, group, sub, seq_step):
    frames_n, own_rows = q_ref.shape[0], q_ref.shape[1]
    seqs_n = kv_ref.shape[0]
    devices_n = frames_n * seqs_n
    me = lax.axis_index("seq")
    head = HEAD_WIDTH
    q_rows = frames_n * sub
    keys_n = seq_step * frames_n * sub
    rows = group * q_rows
    ones = jnp.ones((keys_n, head), jnp.bfloat16)

    def tile(h, q, state, kb, sg, diagonal, qb):
        m, acc = state
        at = pl.ds(pl.multiple_of(kb * sub, sub), sub)
        seqs = pl.ds(sg * seq_step, seq_step)
        k = kv_ref[seqs, :, at, h * head : (h + 1) * head].reshape(keys_n, head)
        v = kv_ref[seqs, :, at, (kv_heads + h) * head : (kv_heads + h + 1) * head]
        v = jnp.concatenate([v.reshape(keys_n, head), ones], axis=1)
        s = lax.dot_general(q, k, (((1,), (1,)), ((), ())), preferred_element_type=jnp.float32)
        if diagonal:
            qi = lax.broadcasted_iota(jnp.int32, (rows, 1), 0) % q_rows
            qpos = (qi % sub) * devices_n + (qi // sub) * seqs_n + me
            ki = lax.broadcasted_iota(jnp.int32, (1, keys_n), 1)
            kpos = (ki % sub) * devices_n + (ki // sub % frames_n) * seqs_n
            kpos = kpos + ki // (sub * frames_n) + sg * seq_step
            s = jnp.where(kpos <= qpos, s, masked_score)
        new = jnp.maximum(m, jnp.max(s, axis=1, keepdims=True))
        e = jnp.exp2(s - new).astype(jnp.bfloat16)
        acc = acc * jnp.exp2(m - new) + dot32(e, v)
        return new, acc

    def one_block(qb, carry):
        at = pl.ds(pl.multiple_of(qb * sub, sub), sub)
        qs = []
        for h in range(kv_heads):
            parts = [
                q_ref[:, at, (h * group + g) * head : (h * group + g + 1) * head].reshape(q_rows, head)
                for g in range(group)
            ]
            qs.append(jnp.concatenate(parts, axis=0))
        steps = seqs_n // seq_step
        state = tuple(
            (jnp.full((rows, 1), masked_score, jnp.float32), jnp.zeros((rows, 2 * head), jnp.float32))
            for _ in range(kv_heads)
        )

        def diag_step(sg, st):
            return tuple(tile(h, qs[h], st[h], qb, sg, True, qb) for h in range(kv_heads))

        state = diag_step(0, state) if steps == 1 else lax.fori_loop(0, steps, diag_step, state)

        def full_step(i, st):
            return tuple(
                tile(h, qs[h], st[h], i // steps, i % steps, False, qb) for h in range(kv_heads)
            )

        state = lax.fori_loop(0, qb * steps, full_step, state)
        for h in range(kv_heads):
            m, acc = state[h]
            out = (acc[:, :head] / acc[:, head:]).astype(jnp.bfloat16)
            for g in range(group):
                piece = out[g * q_rows : (g + 1) * q_rows].reshape(frames_n, sub, head)
                o_ref[:, at, (h * group + g) * head : (h * group + g + 1) * head] = piece
        return carry

    lax.fori_loop(0, own_rows // sub, one_block, 0)


def text_attention(q, kv, kv_heads, group):
    frames_n, own_rows, width = q.shape
    seqs_n = kv.shape[0]
    sub = math.gcd(own_rows, 32)
    seq_step = math.gcd(seqs_n, max(1, 1024 // (sub * frames_n)))
    return pl.pallas_call(
        functools.partial(
            text_kernel, kv_heads=kv_heads, group=group, sub=sub, seq_step=seq_step
        ),
        in_specs=[pl.BlockSpec(memory_space=pltpu.VMEM)] * 2,
        out_specs=pl.BlockSpec(memory_space=pltpu.VMEM),
        out_shape=jax.ShapeDtypeStruct(q.shape, jnp.bfloat16),
        compiler_params=pltpu.CompilerParams(vmem_limit_bytes=50 * 1024 * 1024),
        cost_estimate=pl.CostEstimate(
            flops=4 * seqs_n * frames_n * own_rows * frames_n * own_rows * width,
            bytes_accessed=4 * q.size + 2 * kv.size,
            transcendentals=0,
        ),
        name="text_attention",
    )(q, kv)


def mix_kernel(*refs, groups, pieces):
    blocks, weights, o_ref = refs[:groups], refs[groups:-1], refs[-1]
    total = jnp.zeros(o_ref.shape, jnp.float32)
    for g in range(groups):
        for i in range(pieces):
            w = weights[g * pieces + i]
            depth = w.shape[0]
            total = total + dot32(blocks[g][:, i * depth : (i + 1) * depth], w[...])
    o_ref[...] = total.astype(o_ref.dtype)


def mix(blocks, weights):
    rows, depth = blocks[0].shape
    out_cols = weights[0].shape[1]
    step = math.gcd(out_cols, 512)
    whole = pl.BlockSpec((rows, depth), lambda j: (0, 0))
    column = pl.BlockSpec((weights[0].shape[0], step), lambda j: (0, j))
    return pl.pallas_call(
        functools.partial(
            mix_kernel, groups=len(blocks), pieces=len(weights) // len(blocks)
        ),
        grid=(out_cols // step,),
        in_specs=[whole] * len(blocks) + [column] * len(weights),
        out_specs=pl.BlockSpec((rows, step), lambda j: (0, j)),
        out_shape=jax.ShapeDtypeStruct((rows, out_cols), jnp.bfloat16),
        name="mix",
    )(*blocks, *weights)


class SeqRelay:
    def __init__(self, x_ref, out_ref, sems, count):
        seqs = lax.axis_size("seq")
        self.x, self.out, self.count = x_ref, out_ref, count
        self.send_r, self.recv_r, self.send_l, self.recv_l, self.send_y, self.recv_y = sems
        self.depth = x_ref.shape[0] // count
        self.breadth = 2 if seqs % 2 == 0 else 1
        self.length = seqs // self.breadth
        self.me = lax.axis_index("seq")
        self.a, self.b = self.me // self.breadth, self.me % self.breadth
        self.across = self.a * self.breadth + (self.breadth - 1 - self.b)
        self.has_right, self.has_left = self.a + 1 < self.length, self.a > 0

    def greet(self, barrier):
        breadth = self.breadth
        pl.when(self.has_right)(lambda: greet(barrier, "seq", self.me + breadth))
        pl.when(self.has_left)(lambda: greet(barrier, "seq", self.me - breadth))
        if breadth == 2:
            greet(barrier, "seq", self.across)

    def peers(self):
        sides = self.has_right.astype(jnp.int32) + self.has_left.astype(jnp.int32)
        return sides + (self.breadth - 1)

    def slot(self, source, b, i):
        return self.out.at[source * self.breadth + b, pl.ds(i * self.depth, self.depth)]

    def own(self, i):
        return self.x.at[pl.ds(i * self.depth, self.depth)]

    def shift(self, i, k, right):
        slot = self.slot(self.a - k if right else self.a + k, self.b, i)
        send, recv = (self.send_r, self.recv_r) if right else (self.send_l, self.recv_l)
        src = self.own(i) if k == 0 else slot
        target = self.me + self.breadth if right else self.me - self.breadth
        return remote(src, slot, send.at[i, k], recv.at[i, k], "seq", target)

    def cross(self, i, source, own):
        slot = self.slot(source, self.b, i)
        src = self.own(i) if own else slot
        return remote(src, slot, self.send_y.at[i, source], self.recv_y.at[i, source], "seq", self.across)

    def incoming(self, i, k, right):
        slot = self.slot(self.a - k if right else self.a + k, self.b, i)
        recv = self.recv_r if right else self.recv_l
        return remote(slot, slot, self.send_r.at[i, 0], recv.at[i, k - 1], "seq", self.across)

    def incoming_cross(self, i, source):
        slot = self.slot(source, self.breadth - 1 - self.b, i)
        return remote(slot, slot, self.send_r.at[i, 0], self.recv_y.at[i, source], "seq", self.across)

    def held(self, k, right):
        held = (self.a >= k) if right else (self.a + k < self.length)
        return held, held & (self.has_right if right else self.has_left)

    def first(self):
        for i in range(self.count):
            for right in (True, False):
                pl.when(self.held(0, right)[1])(lambda: self.shift(i, 0, right).start())
            if self.breadth == 2:
                self.cross(i, self.a, True).start()

    def step(self, k):
        for i in range(self.count):
            for right in (True, False):
                held, onward = self.held(k, right)
                source = self.a - k if right else self.a + k
                pl.when(held)(lambda: self.incoming(i, k, right).wait_recv())
                pl.when(onward)(lambda: self.shift(i, k, right).start())
                if self.breadth == 2:
                    pl.when(held)(lambda: self.cross(i, source, False).start())

    def finish(self):
        for i in range(self.count):
            for k in range(self.length):
                for right in (True, False):
                    onward = self.held(k, right)[1]
                    pl.when(onward)(lambda: self.shift(i, k, right).wait_send())
                if self.breadth == 2:
                    self.incoming_cross(i, k).wait_recv()
                    self.cross(i, k, False).wait_send()


def gather_kernel(x_ref, out_ref, local, *sems, count):
    relay = SeqRelay(x_ref, out_ref, sems, count)
    barrier = pltpu.get_barrier_semaphore()
    relay.greet(barrier)
    pl.semaphore_wait(barrier, relay.peers())
    relay.first()
    keep = pltpu.make_async_copy(x_ref, out_ref.at[relay.me], local.at[0])
    keep.start()
    for k in range(1, relay.length):
        relay.step(k)
    keep.wait()
    relay.finish()


def seq_gather(x, chunks, collective_id, name):
    seqs = lax.axis_size("seq")
    vmem = pl.BlockSpec(memory_space=pltpu.VMEM)
    return pl.pallas_call(
        functools.partial(gather_kernel, count=chunks),
        in_specs=[vmem],
        out_specs=vmem,
        out_shape=jax.ShapeDtypeStruct((seqs,) + x.shape, x.dtype),
        scratch_shapes=[pltpu.SemaphoreType.DMA((1,))] + relay_scratch(chunks),
        compiler_params=pltpu.CompilerParams(
            collective_id=collective_id,
            has_side_effects=True,
            vmem_limit_bytes=24 * 1024 * 1024,
        ),
        cost_estimate=pl.CostEstimate(
            flops=40_000_000_000, bytes_accessed=0, transcendentals=0
        ),
        name=name,
    )(x)


def rotate(values, cosine, sine):
    half = HEAD_WIDTH // 2
    first, second = values[..., :half], values[..., half:]
    return jnp.concatenate(
        [first * cosine - second * sine, second * cosine + first * sine], axis=-1
    )


def per_device(
    vit_states,
    frame_slot,
    patch_count,
    vis_start,
    text_embed,
    vit_ln_gain,
    vit_ln_bias,
    vit_qkv_w,
    vit_qkv_b,
    vit_out_w,
    vit_out_b,
    proj_w,
    proj_b,
    attn_gain,
    wq,
    wk,
    wv,
    wo,
):
    frames_n = lax.axis_size("frame")
    seqs_n = lax.axis_size("seq")
    chips = frames_n // 2
    devices_n = frames_n * seqs_n
    me = lax.axis_index("frame")
    my_seq = lax.axis_index("seq")
    slots_held, frame_max, width_vit = vit_states.shape
    vis_max = frame_max // 4
    own_rows, model_width = text_embed.shape[0], text_embed.shape[2]
    head_size = width_vit // VHEADS
    my_heads = VHEADS // frames_n
    cols = width_vit // frames_n

    w_parts = [
        lax.dynamic_slice_in_dim(vit_qkv_w, i * width_vit + me * cols, cols, 1) for i in range(3)
    ]
    out_own = lax.dynamic_slice_in_dim(vit_out_w, me * cols, cols, 1)
    own_weights = jnp.concatenate(w_parts + [out_own], 1)
    qkv_bias = [
        lax.dynamic_slice_in_dim(vit_qkv_b, i * width_vit + me * cols, cols, 0) for i in range(3)
    ]
    out_bias = lax.dynamic_slice_in_dim(vit_out_b, me * cols, cols, 0)

    frame_ids = jnp.arange(frame_slot.shape[0])
    holder = frame_slot // slots_held
    holder_frame = holder // seqs_n
    pair_low = (holder_frame - holder_frame % 2) * seqs_n + holder % seqs_n
    pair_order = holder_frame % 2 * slots_held + frame_slot % slots_held
    same_pair = pair_low[:, None] == pair_low[None, :]
    earlier = pair_order[None, :] < pair_order[:, None]
    pair_rank = jnp.sum((same_pair & earlier).astype(jnp.int32), axis=1)
    source_frame = pair_low // seqs_n + pair_rank
    source_seq = pair_low % seqs_n
    mine_low = (source_seq == my_seq) & (pair_low // seqs_n == me - me % 2)
    orders = [
        jnp.sum(jnp.where(mine_low & (pair_rank == (me % 2 ^ i)), pair_order, 0)) for i in range(2)
    ]
    group_hit = (source_frame[None, :] == jnp.arange(frames_n)[:, None]) & (
        source_seq == my_seq
    )[None, :]
    group_count = jnp.sum(jnp.where(group_hit, patch_count[None, :], 0), axis=1)
    group_start = jnp.sum(jnp.where(group_hit, vis_start[None, :], 0), axis=1)

    both_weights, states, text_rows = front(
        jnp.stack(orders), own_weights, vit_states, text_embed.reshape(own_rows, model_width)
    )
    both_weights = both_weights.reshape(width_vit, 4 * cols)

    piece_rows = math.gcd(wo.shape[0], HEAD_WIDTH)
    pieces = wo.shape[0] // piece_rows
    wo_pieces = [wo[i * piece_rows : (i + 1) * piece_rows] for i in range(pieces)]

    context, pooled_states = vit_attention(
        group_count,
        states,
        both_weights,
        vit_ln_gain.reshape(1, width_vit),
        vit_ln_bias.reshape(1, width_vit),
        jnp.concatenate(qkv_bias).reshape(1, 3 * cols),
        my_heads,
        head_size,
    )
    laps = vis_max // seqs_n
    table = route(
        group_start,
        context.reshape(frames_n * vis_max, cols),
        pooled_states.reshape(frames_n * vis_max, cols),
        both_weights,
        out_bias.reshape(1, cols),
        vis_max,
    )
    table, later = lax.optimization_barrier((table, tuple(wo_pieces)))
    wo_across = [[from_relative(p, dx, 0) for dx in range(1, chips)] for p in later]
    wo_near = [from_relative(p, 0, 1) for p in later]

    group_rows = frames_n * own_rows
    row_ids = jnp.arange(group_rows)
    positions = row_ids % own_rows * devices_n + row_ids // own_rows * seqs_n + my_seq
    query_width, kv_width = wq.shape[1], wk.shape[1]
    kv_heads = kv_width // HEAD_WIDTH
    query_heads = query_width // HEAD_WIDTH
    exponents = jnp.arange(0, HEAD_WIDTH, 2).astype(jnp.float32) / HEAD_WIDTH
    inverse = jnp.power(jnp.float32(rope_theta), -exponents)
    angles = positions.astype(jnp.float32)[:, None] * inverse[None, :]
    cosine, sine = jnp.cos(angles), jnp.sin(angles)
    as_row = lambda x: x.astype(jnp.int32).reshape(1, -1)
    queries, own_kv = merge(
        as_row(vis_start),
        as_row(patch_count // 4),
        as_row((source_seq * frames_n + source_frame) * laps),
        table,
        proj_w,
        proj_b.reshape(1, model_width),
        text_rows,
        attn_gain.reshape(1, model_width),
        wq,
        wk,
        wv,
        jnp.concatenate([cosine, cosine], 1),
        jnp.concatenate([-sine, sine], 1),
    )
    kv = seq_gather(own_kv, 2, 3, "kv_gather")
    context_tok = text_attention(
        queries.reshape(frames_n, own_rows, query_width),
        kv.reshape(seqs_n, frames_n, own_rows, 2 * kv_width),
        kv_heads,
        query_heads // kv_heads,
    )

    context_tok, wo_across = lax.optimization_barrier((context_tok, wo_across))
    wo_gathered = []
    for piece, near, across in zip(wo_pieces, wo_near, wo_across):
        row = [piece, near]
        for same in across:
            row += [same, from_relative(same, 0, 1)]
        wo_gathered.append(row)
    blocks, mix_weights = [], []
    for dx in range(chips):
        for dc in range(2):
            to = jnp.mod(me // 2 - dx, chips) * 2 + (me % 2 ^ dc)
            block = lax.dynamic_index_in_dim(context_tok, to, 0, keepdims=False)
            if dx or dc:
                block = from_relative(block, dx, dc)
            blocks.append(block)
            mix_weights += [wo_gathered[i][dx * 2 + dc] for i in range(pieces)]
    mixed = mix(blocks, mix_weights)
    return mixed.reshape(own_rows, 1, wo.shape[1])


def solution(mesh):
    return jax.shard_map(
        per_device,
        mesh=mesh,
        in_specs=(
            P(("frame", "seq"), None, None),
            P(),
            P(),
            P(),
            P(None, ("frame", "seq"), None),
            P(),
            P(),
            P("seq", None),
            P(),
            P("seq", None),
            P(),
            P(),
            P(),
            P(),
            P(None, "frame"),
            P(None, "frame"),
            P(None, "frame"),
            P("frame", None),
        ),
        out_specs=P(None, ("frame", "seq"), None),
        check_vma=False,
    )
```

```python
import functools
import math

import jax
import jax.numpy as jnp
from jax import lax
from jax.experimental import pallas as pl
from jax.experimental.pallas import tpu as pltpu
from jax.sharding import PartitionSpec as P

VHEADS = 16
HEAD_WIDTH = 128

rope_theta = 500000.0
vit_epsilon = 1e-06
norm_epsilon = 1e-05
masked_score = -1e30
LOG2E = math.log2(math.e)


def dot32(a, b):
    return jnp.dot(a, b, preferred_element_type=jnp.float32)


def ceil_to(value, step):
    return -(-value // step) * step


def vit_kernel(
    count_ref, x_ref, w_ref, gain_ref, shift_ref, qb_ref, ctx_ref, pst_ref, *, heads, head_size
):
    frame = pl.program_id(0)
    frames = pl.num_programs(0)
    me = lax.axis_index("frame")
    rows, width = x_ref.shape[1], x_ref.shape[2]
    cols = heads * head_size
    out_rows = ctx_ref.shape[1]
    states = x_ref[0]
    wide = states.astype(jnp.float32)
    average = jnp.mean(wide, axis=1, keepdims=True)
    centred = wide - average
    spread = jnp.mean(centred * centred, axis=1, keepdims=True)
    normed = centred * lax.rsqrt(spread + vit_epsilon) * gain_ref[...] + shift_ref[...]
    w = w_ref[:, : 3 * cols]
    proj = (dot32(normed.astype(jnp.bfloat16), w) + qb_ref[...]).astype(jnp.bfloat16)
    q, k, v = (proj[:, i * cols : (i + 1) * cols] for i in range(3))
    live = lax.broadcasted_iota(jnp.int32, (1, rows), 1) < count_ref[frame]
    blocks = [None] * pl.cdiv(cols, 128)
    scale = LOG2E / math.sqrt(head_size)
    for h in range(heads):
        low, high = h * head_size, (h + 1) * head_size
        start, stop = low // 128 * 128, min(ceil_to(high, 128), cols)
        lane = lax.broadcasted_iota(jnp.int32, (1, stop - start), 1) + start
        mine = jnp.where((lane >= low) & (lane < high), 1.0, 0.0).astype(jnp.bfloat16)
        s = lax.dot_general(
            q[:, start:stop] * mine,
            k[:, start:stop],
            (((1,), (1,)), ((), ())),
            preferred_element_type=jnp.float32,
        )
        s = jnp.where(live, s * scale, masked_score)
        e = jnp.exp2(s - jnp.max(s, axis=1, keepdims=True))
        p = (e * (1.0 / jnp.sum(e, axis=1, keepdims=True))).astype(jnp.bfloat16)
        o = dot32(p, v[:, start:stop] * mine)
        for b in range(start // 128, pl.cdiv(stop, 128)):
            part = o[:, b * 128 - start : min((b + 1) * 128, stop) - start]
            blocks[b] = part if blocks[b] is None else blocks[b] + part
    context = jnp.concatenate(blocks, axis=1).astype(jnp.bfloat16)
    pr = lax.broadcasted_iota(jnp.int32, (out_rows, rows), 0)
    pc = lax.broadcasted_iota(jnp.int32, (out_rows, rows), 1)
    pool = jnp.where(pc // 4 == pr, 0.25, 0.0).astype(jnp.bfloat16)
    ctx_ref[0] = dot32(pool, context).astype(jnp.bfloat16)
    pooled = dot32(pool, states)
    total = jnp.zeros((out_rows, cols), jnp.float32)
    for f in range(width // cols):
        total = total + jnp.where(me == f, 1.0, 0.0) * pooled[:, f * cols : (f + 1) * cols]
    pst_ref[0] = total


def vit_attention(counts, states, weights, gain, shift, qkv_bias, heads, head_size):
    frames, rows, width = states.shape
    cols = heads * head_size
    whole = lambda x: pl.BlockSpec(x.shape, lambda i: (0,) * x.ndim)
    out = pl.BlockSpec((1, rows // 4, cols), lambda i: (i, 0, 0))
    return pl.pallas_call(
        functools.partial(vit_kernel, heads=heads, head_size=head_size),
        grid=(frames,),
        in_specs=[
            pl.BlockSpec(memory_space=pltpu.SMEM),
            pl.BlockSpec((1, rows, width), lambda i: (i, 0, 0)),
            whole(weights),
            whole(gain),
            whole(shift),
            whole(qkv_bias),
        ],
        out_specs=[out, out],
        out_shape=[
            jax.ShapeDtypeStruct((frames, rows // 4, cols), jnp.bfloat16),
            jax.ShapeDtypeStruct((frames, rows // 4, cols), jnp.float32),
        ],
        compiler_params=pltpu.CompilerParams(vmem_limit_bytes=32 * 1024 * 1024),
        cost_estimate=pl.CostEstimate(
            flops=2 * frames * rows * width * 3 * cols,
            bytes_accessed=2 * states.size,
            transcendentals=frames * heads * rows * rows,
        ),
        name="vit_attention",
    )(counts, states, weights, gain, shift, qkv_bias)


MESH = pl.DeviceIdType.MESH


def remote(src, dst, send, recv, axis, index):
    return pltpu.make_async_remote_copy(
        src_ref=src,
        dst_ref=dst,
        send_sem=send,
        recv_sem=recv,
        device_id={axis: index},
        device_id_type=MESH,
    )


def frame_peers():
    frames = lax.axis_size("frame")
    me = lax.axis_index("frame")
    chips = frames // 2
    chip, core = me // 2, me % 2
    partner = chip * 2 + (1 - core)
    ahead = [((chip + dx) % chips) * 2 + core for dx in range(1, chips)]
    behind = [((chip + chips - dx) % chips) * 2 + core for dx in range(1, chips)]
    return me, partner, ahead, behind


def greet(barrier, axis, index):
    pl.semaphore_signal(barrier, inc=1, device_id={axis: index}, device_id_type=MESH)


class FrameSpread:
    def __init__(self, out_ref, sems):
        self.out = out_ref
        self.send, self.recv = sems
        self.me, self.partner, self.ahead, self.behind = frame_peers()
        self.started = []

    def go(self, src, slot, k, target):
        copy = remote(src, self.out.at[slot], self.send.at[k], self.recv.at[k], "frame", target)
        copy.start()
        self.started.append(copy)

    def arrived(self, slot, k):
        ref = self.out.at[slot]
        remote(ref, ref, self.send.at[k], self.recv.at[k], "frame", self.partner).wait_recv()

    def send_across(self, src):
        for i, target in enumerate(self.ahead):
            self.go(src, self.me, 1 + i, target)

    def send_partner(self, src):
        self.go(src, self.me, 0, self.partner)

    def forward(self):
        n = len(self.ahead)
        for i, source in enumerate(self.behind):
            self.arrived(source, 1 + i)
            self.go(self.out.at[source], source, 1 + n + i, self.partner)

    def finish(self, partner_sent=True):
        n = len(self.ahead)
        if partner_sent:
            self.arrived(self.partner, 0)
        for i, source in enumerate(self.behind):
            other = source + 1 - 2 * (self.me % 2)
            self.arrived(other, 1 + n + i)
        for copy in self.started:
            copy.wait_send()


def front_kernel(
    order_ref,
    w_ref,
    states_ref,
    text_ref,
    w_out,
    states_out,
    text_out,
    pair,
    local,
    pair_sems,
    state_sems_a,
    state_sems_b,
    text_sems_a,
    text_sems_b,
    *relay_sems,
    count,
):
    relay = SeqRelay(w_ref, w_out, relay_sems, count)
    states = FrameSpread(states_out, (state_sems_a, state_sems_b))
    text = FrameSpread(text_out, (text_sems_a, text_sems_b))
    me, partner, ahead, behind = frame_peers()
    barrier = pltpu.get_barrier_semaphore()
    relay.greet(barrier)
    for peer in [partner] + ahead:
        greet(barrier, "frame", peer)
    pl.semaphore_wait(barrier, relay.peers() + (1 + len(ahead)))
    swap = remote(states_ref, pair, pair_sems.at[0], pair_sems.at[1], "frame", partner)
    swap.start()
    relay.first()
    pltpu.make_async_copy(w_ref, w_out.at[relay.me], local.at[0]).start()
    pltpu.make_async_copy(text_ref, text_out.at[me], local.at[1]).start()
    swap.wait()
    core = me % 2
    slots = states_ref.shape[0]
    rows = states_ref.shape[1]
    step = math.gcd(rows, 32)
    keep = [
        [
            jnp.where(order_ref[j] == side * slots + k, 1.0, 0.0)
            for side in (core, 1 - core)
            for k in range(slots)
        ]
        for j in range(2)
    ]

    def choose(i, carry):
        at = pl.ds(pl.multiple_of(i * step, step), step)
        values = [states_ref[k, at].astype(jnp.float32) for k in range(slots)]
        values += [pair[k, at].astype(jnp.float32) for k in range(slots)]
        for j, slot in enumerate((me, partner)):
            total = keep[j][0] * values[0]
            for weight, value in zip(keep[j][1:], values[1:]):
                total = total + weight * value
            states_out[slot, at] = total.astype(states_out.dtype)
        return carry

    lax.fori_loop(0, rows // step, choose, 0)
    states.send_across(states_out.at[me])
    text.send_across(text_ref)
    text.send_partner(text_ref)
    for k in range(1, relay.length):
        relay.step(k)
    states.forward()
    text.forward()
    pltpu.make_async_copy(w_ref, w_out.at[relay.me], local.at[0]).wait()
    pltpu.make_async_copy(text_ref, text_out.at[me], local.at[1]).wait()
    states.finish(partner_sent=False)
    text.finish()
    relay.finish()


def relay_scratch(chunks):
    seqs = lax.axis_size("seq")
    length = seqs // 2 if seqs % 2 == 0 else seqs
    return [pltpu.SemaphoreType.DMA((chunks, length))] * 6


def front(orders, weights, states, text):
    seqs, frames = lax.axis_size("seq"), lax.axis_size("frame")
    vmem = pl.BlockSpec(memory_space=pltpu.VMEM)
    spread = [pltpu.SemaphoreType.DMA((max(1, frames - 1),))] * 4
    chunks = 2
    return pl.pallas_call(
        functools.partial(front_kernel, count=chunks),
        in_specs=[pl.BlockSpec(memory_space=pltpu.SMEM)] + [vmem] * 3,
        out_specs=[vmem] * 3,
        out_shape=[
            jax.ShapeDtypeStruct((seqs,) + weights.shape, weights.dtype),
            jax.ShapeDtypeStruct((frames,) + states.shape[1:], states.dtype),
            jax.ShapeDtypeStruct((frames,) + text.shape, text.dtype),
        ],
        scratch_shapes=[
            pltpu.VMEM(states.shape, states.dtype),
            pltpu.SemaphoreType.DMA((2,)),
            pltpu.SemaphoreType.DMA((2,)),
        ]
        + spread
        + relay_scratch(chunks),
        compiler_params=pltpu.CompilerParams(
            collective_id=1, has_side_effects=True, vmem_limit_bytes=36 * 1024 * 1024
        ),
        cost_estimate=pl.CostEstimate(
            flops=40_000_000_000, bytes_accessed=0, transcendentals=0
        ),
        name="front",
    )(orders, weights, states, text)


def route_kernel(
    start_ref,
    ctx_ref,
    pst_ref,
    w_ref,
    ob_ref,
    table_out,
    ctx_all,
    outgoing,
    local,
    ctx_sems_a,
    ctx_sems_b,
    table_sems_a,
    table_sems_b,
    seq_send,
    seq_recv,
    *,
    vis_max,
):
    frames, seqs = lax.axis_size("frame"), lax.axis_size("seq")
    seq = lax.axis_index("seq")
    me, partner, ahead, behind = frame_peers()
    cols = ctx_ref.shape[1]
    share = outgoing.shape[0] // seqs
    laps = share // frames
    barrier = pltpu.get_barrier_semaphore()
    for peer in [partner] + ahead:
        greet(barrier, "frame", peer)
    others = [(seq + d) % seqs for d in range(1, seqs)]
    for other in others:
        greet(barrier, "seq", other)
    pl.semaphore_wait(barrier, frames // 2 + seqs - 1)
    context = FrameSpread(ctx_all, (ctx_sems_a, ctx_sems_b))
    context.send_across(ctx_ref)
    context.send_partner(ctx_ref)
    pltpu.make_async_copy(ctx_ref, ctx_all.at[me], local.at[0]).start()

    rows = outgoing.shape[0]
    r = lax.broadcasted_iota(jnp.int32, (rows, 1), 0)
    dest, frame, lap = r // share, r // laps % frames, r % laps
    begin = jnp.zeros((rows, 1), jnp.int32)
    for f in range(frames):
        begin = begin + jnp.where(frame == f, start_ref[f], 0)
    token = (dest + seqs - begin % seqs) % seqs + lap * seqs + frame * vis_max
    c = lax.broadcasted_iota(jnp.int32, (1, frames * vis_max), 1)
    pick = jnp.where(token == c, 1.0, 0.0).astype(jnp.bfloat16)

    context.forward()
    pltpu.make_async_copy(ctx_ref, ctx_all.at[me], local.at[0]).wait()
    context.finish()
    total = pst_ref[...] + ob_ref[...]
    for f in range(frames):
        total = total + dot32(ctx_all[f], w_ref[f * cols : (f + 1) * cols, 3 * cols : 4 * cols])
    outgoing[...] = dot32(pick, total.astype(jnp.bfloat16)).astype(jnp.bfloat16)

    def part(index):
        return pl.ds(pl.multiple_of(index * share, share), share)

    mine = table_out.at[me]
    sends = []
    for d, other in enumerate(others):
        copy = remote(
            outgoing.at[part(other)],
            mine.at[part(seq)],
            seq_send.at[d],
            seq_recv.at[d],
            "seq",
            other,
        )
        copy.start()
        sends.append(copy)
    keep = pltpu.make_async_copy(outgoing.at[part(seq)], mine.at[part(seq)], local.at[1])
    keep.start()
    keep.wait()
    for d in range(seqs - 1):
        source = (seq + seqs - 1 - d) % seqs
        ref = mine.at[part(source)]
        remote(ref, ref, seq_send.at[d], seq_recv.at[d], "seq", source).wait_recv()
    table = FrameSpread(table_out, (table_sems_a, table_sems_b))
    table.send_across(mine)
    table.send_partner(mine)
    table.forward()
    table.finish()
    for copy in sends:
        copy.wait_send()


def route(starts, context, pooled_states, weights, out_bias, vis_max):
    frames, seqs = lax.axis_size("frame"), lax.axis_size("seq")
    cols = context.shape[1]
    rows = frames * vis_max
    vmem = pl.BlockSpec(memory_space=pltpu.VMEM)
    spread = [pltpu.SemaphoreType.DMA((max(1, frames - 1),))] * 4
    return pl.pallas_call(
        functools.partial(route_kernel, vis_max=vis_max),
        in_specs=[pl.BlockSpec(memory_space=pltpu.SMEM)] + [vmem] * 4,
        out_specs=vmem,
        out_shape=jax.ShapeDtypeStruct((frames, rows, cols), jnp.bfloat16),
        scratch_shapes=[
            pltpu.VMEM((frames, rows, cols), jnp.bfloat16),
            pltpu.VMEM((rows, cols), jnp.bfloat16),
            pltpu.SemaphoreType.DMA((2,)),
        ]
        + spread
        + [pltpu.SemaphoreType.DMA((seqs - 1,))] * 2,
        compiler_params=pltpu.CompilerParams(
            collective_id=2, has_side_effects=True, vmem_limit_bytes=24 * 1024 * 1024
        ),
        cost_estimate=pl.CostEstimate(
            flops=12_000_000_000, bytes_accessed=0, transcendentals=0
        ),
        name="route",
    )(starts, context, pooled_states, weights, out_bias)


def merge_kernel(
    begin_ref,
    length_ref,
    base_ref,
    table_ref,
    pw_ref,
    pb_ref,
    text_ref,
    gain_ref,
    wq_ref,
    wk_ref,
    wv_ref,
    cos_ref,
    sin_ref,
    q_ref,
    kv_ref,
    hot,
    visual_mask,
    merged,
    squares,
    acc,
    *,
    steps,
):
    j = pl.program_id(0)
    frames, seqs = lax.axis_size("frame"), lax.axis_size("seq")
    my_seq = lax.axis_index("seq")
    rows = acc.shape[0]
    own_rows = rows // frames
    cols = table_ref.shape[2]
    block = pb_ref.shape[1]
    model_width = steps * block
    head = HEAD_WIDTH

    @pl.when(j == 0)
    def _():
        i = lax.broadcasted_iota(jnp.int32, (rows, 1), 0)
        position = i % own_rows * (frames * seqs) + i // own_rows * seqs + my_seq
        t = lax.broadcasted_iota(jnp.int32, (1, begin_ref.shape[1]), 1)
        mine = position // own_rows == t

        def of_frame(ref):
            return jnp.sum(jnp.where(mine, ref[...], 0), axis=1, keepdims=True)

        within = position - of_frame(begin_ref)
        visual = (within >= 0) & (within < of_frame(length_ref))
        row = of_frame(base_ref) + jnp.maximum(within, 0) // seqs
        c = lax.broadcasted_iota(jnp.int32, (1, hot.shape[1]), 1)
        hot[...] = jnp.where(visual & (row == c), 1.0, 0.0).astype(jnp.bfloat16)
        visual_mask[...] = jnp.where(visual, 1.0, 0.0)
        squares[...] = jnp.zeros_like(squares)
        acc[...] = jnp.zeros_like(acc)

    @pl.when(j < steps)
    def _():
        total = pb_ref[...] + jnp.zeros((table_ref.shape[1], block), jnp.float32)
        for f in range(frames):
            total = total + dot32(table_ref[f], pw_ref[f * cols : (f + 1) * cols])
        fetched = dot32(hot[...], total.astype(jnp.bfloat16))
        text = text_ref[...].reshape(rows, block).astype(jnp.float32)
        value = jnp.where(visual_mask[...] > 0.5, fetched, text)
        squares[...] += jnp.sum(value * value, axis=1, keepdims=True)
        merged[j] = value.astype(jnp.bfloat16)

    @pl.when(j >= steps)
    def _():
        scale = lax.rsqrt(squares[...] * (1.0 / model_width) + norm_epsilon)
        normed = merged[j - steps].astype(jnp.float32) * scale * gain_ref[...]
        normed = normed.astype(jnp.bfloat16)
        qw, kw = wq_ref.shape[1], wk_ref.shape[1]
        acc[:, :qw] += dot32(normed, wq_ref[...])
        acc[:, qw : qw + kw] += dot32(normed, wk_ref[...])
        acc[:, qw + kw :] += dot32(normed, wv_ref[...])

    @pl.when(j == 2 * steps - 1)
    def _():
        qw, kw = wq_ref.shape[1], wk_ref.shape[1]
        cosine, sine = cos_ref[...], sin_ref[...]

        def turn(at, factor):
            x = acc[:, at : at + head]
            x = x * cosine + pltpu.roll(x, head // 2, 1) * sine
            return (x * factor if factor != 1.0 else x).astype(jnp.bfloat16)

        for h in range(qw // head):
            q_ref[:, h * head : (h + 1) * head] = turn(h * head, LOG2E / math.sqrt(head))
        for h in range(kw // head):
            kv_ref[:, h * head : (h + 1) * head] = turn(qw + h * head, 1.0)
        kv_ref[:, kw:] = acc[:, qw + kw :].astype(jnp.bfloat16)


def merge(begin, length, base, table, proj_w, proj_b, text, gain, wq, wk, wv, cosine, sine):
    frames, own_rows, model_width = text.shape
    rows = frames * own_rows
    block = math.gcd(model_width, 512)
    steps = model_width // block
    qw, kw = wq.shape[1], wk.shape[1]
    first = lambda j: jnp.minimum(j, steps - 1)
    second = lambda j: jnp.maximum(j - steps, 0)
    whole = lambda x: pl.BlockSpec(x.shape, lambda j: (0,) * x.ndim)
    return pl.pallas_call(
        functools.partial(merge_kernel, steps=steps),
        grid=(2 * steps,),
        in_specs=[
            whole(begin),
            whole(length),
            whole(base),
            whole(table),
            pl.BlockSpec((proj_w.shape[0], block), lambda j: (0, first(j))),
            pl.BlockSpec((1, block), lambda j: (0, first(j))),
            pl.BlockSpec((frames, own_rows, block), lambda j: (0, 0, first(j))),
            pl.BlockSpec((1, block), lambda j: (0, second(j))),
            pl.BlockSpec((block, qw), lambda j: (second(j), 0)),
            pl.BlockSpec((block, kw), lambda j: (second(j), 0)),
            pl.BlockSpec((block, kw), lambda j: (second(j), 0)),
            whole(cosine),
            whole(sine),
        ],
        out_specs=[
            pl.BlockSpec((rows, qw), lambda j: (0, 0)),
            pl.BlockSpec((rows, 2 * kw), lambda j: (0, 0)),
        ],
        out_shape=[
            jax.ShapeDtypeStruct((rows, qw), jnp.bfloat16),
            jax.ShapeDtypeStruct((rows, 2 * kw), jnp.bfloat16),
        ],
        scratch_shapes=[
            pltpu.VMEM((rows, table.shape[1]), jnp.bfloat16),
            pltpu.VMEM((rows, 1), jnp.float32),
            pltpu.VMEM((steps, rows, block), jnp.bfloat16),
            pltpu.VMEM((rows, 1), jnp.float32),
            pltpu.VMEM((rows, qw + 2 * kw), jnp.float32),
        ],
        compiler_params=pltpu.CompilerParams(vmem_limit_bytes=40 * 1024 * 1024),
        cost_estimate=pl.CostEstimate(
            flops=2 * rows * model_width * (qw + 2 * kw) + 2 * proj_w.size * table.shape[1],
            bytes_accessed=2 * proj_w.size + 2 * model_width * (qw + 2 * kw),
            transcendentals=0,
        ),
        name="merge",
    )(begin, length, base, table, proj_w, proj_b, text, gain, wq, wk, wv, cosine, sine)


def exchange_slots(index, frames):
    return [(index + d) % frames for d in range(1, frames)], [
        (index + frames - d) % frames for d in range(1, frames)
    ]


def attend_kernel(
    q_ref,
    x_ref,
    wo_ref,
    mixed_ref,
    kv,
    qs,
    highest,
    acc,
    heads_out,
    context,
    shared,
    near_context,
    wo_all,
    wo_rest,
    arriving,
    local,
    wo_sems_a,
    wo_sems_b,
    rest_sems,
    ctx_send,
    ctx_recv,
    near_sems_a,
    near_sems_b,
    part_send,
    part_recv,
    *relay_sems,
    count,
    kv_heads,
    group,
    sub,
):
    frames, seqs = lax.axis_size("frame"), lax.axis_size("seq")
    devices = frames * seqs
    my_seq = lax.axis_index("seq")
    me, partner, ahead, behind = frame_peers()
    head = HEAD_WIDTH
    own_rows = q_ref.shape[1]
    blocks = own_rows // sub
    q_rows = frames * sub
    rows = group * q_rows
    cut = wo_all.shape[2]
    relay = SeqRelay(x_ref, kv, relay_sems, count)
    spread = FrameSpread(wo_all, (wo_sems_a, wo_sems_b))
    barrier = pltpu.get_barrier_semaphore()
    relay.greet(barrier)
    for d in range(1, frames):
        greet(barrier, "frame", (me + d) % frames)
    pl.semaphore_wait(barrier, relay.peers() + (frames - 1))
    relay.first()
    keep = pltpu.make_async_copy(x_ref, kv.at[relay.me], local.at[0])
    keep.start()
    wo_cut, wo_tail = wo_ref.at[:, pl.ds(0, cut)], wo_ref.at[:, pl.ds(cut, wo_rest.shape[2])]
    spread.send_across(wo_cut)
    spread.send_partner(wo_cut)
    rest = remote(wo_tail, wo_rest.at[1], rest_sems.at[0], rest_sems.at[1], "frame", partner)
    rest.start()
    keep_cut = pltpu.make_async_copy(wo_cut, wo_all.at[me], local.at[1])
    keep_cut.start()
    keep_tail = pltpu.make_async_copy(wo_tail, wo_rest.at[0], local.at[2])
    keep_tail.start()

    for h in range(kv_heads):
        for b in range(blocks):
            parts = [
                q_ref[:, b * sub : (b + 1) * sub, (h * group + g) * head : (h * group + g + 1) * head]
                .reshape(q_rows, head)
                for g in range(group)
            ]
            qs[h, b] = jnp.concatenate(parts, axis=0)
    highest[...] = jnp.full(highest.shape, masked_score, jnp.float32)
    acc[...] = jnp.zeros(acc.shape, jnp.float32)

    def process(source):
        for b in range(blocks):
            n = (b + 1) * sub
            keys_n = frames * n
            qi = lax.broadcasted_iota(jnp.int32, (rows, 1), 0) % q_rows
            q_at = (b * sub + qi % sub) * devices + (qi // sub) * seqs + my_seq
            ki = lax.broadcasted_iota(jnp.int32, (1, keys_n), 1)
            k_at = ki % n * devices + ki // n * seqs + source
            seen = k_at <= q_at
            ones = jnp.ones((keys_n, head), jnp.bfloat16)
            for h in range(kv_heads):
                k = kv[source, :, :n, h * head : (h + 1) * head].reshape(keys_n, head)
                v = kv[source, :, :n, (kv_heads + h) * head : (kv_heads + h + 1) * head]
                v = jnp.concatenate([v.reshape(keys_n, head), ones], axis=1)
                s = lax.dot_general(
                    qs[h, b], k, (((1,), (1,)), ((), ())), preferred_element_type=jnp.float32
                )
                s = jnp.where(seen, s, masked_score)
                m = highest[h, b]
                new = jnp.maximum(m, jnp.max(s, axis=1, keepdims=True))
                e = jnp.exp2(s - new).astype(jnp.bfloat16)
                acc[h, b] = acc[h, b] * jnp.exp2(m - new) + dot32(e, v)
                highest[h, b] = new

    keep.wait()

    def step(k, carry):
        pl.when((k > 0) & (k < relay.length))(lambda: relay.step(k))

        def one(i, c):
            crossed, side = i // 2, i % 2
            distance = k - crossed
            source = relay.a - distance + 2 * distance * side
            valid = (source >= 0) & (source < relay.length) & (distance >= 0)
            valid = valid & ((distance > 0) | (side == 0))

            @pl.when(valid)
            def _():
                if relay.breadth == 2:

                    @pl.when(crossed == 1)
                    def _():
                        for chunk in range(count):
                            relay.incoming_cross(chunk, source).wait_recv()

                row = relay.b + crossed * (1 - 2 * relay.b)
                process(source * relay.breadth + row)

            return c

        return lax.fori_loop(0, 2 * relay.breadth, one, carry)

    lax.fori_loop(0, relay.length + relay.breadth - 1, step, 0)
    for h in range(kv_heads):
        for b in range(blocks):
            out = (acc[h, b, :, :head] / acc[h, b, :, head:]).astype(jnp.bfloat16)
            for g in range(group):
                piece = out[g * q_rows : (g + 1) * q_rows].reshape(frames, sub, head)
                at = (h * group + g) * head
                heads_out[:, b * sub : (b + 1) * sub, at : at + head] = piece

    targets, sources = exchange_slots(me, frames)
    copies = []
    near = []
    for i, target in enumerate(ahead):
        near.append(
            remote(
                heads_out.at[target + 1 - 2 * (me % 2)],
                near_context.at[i],
                near_sems_a.at[i],
                near_sems_b.at[i],
                "frame",
                partner,
            )
        )
        near[-1].start()
    for d, target in enumerate(targets):
        copies.append(
            remote(
                heads_out.at[target],
                context.at[me],
                ctx_send.at[d],
                ctx_recv.at[d],
                "frame",
                target,
            )
        )
        copies[-1].start()
    keep_own = pltpu.make_async_copy(heads_out.at[me], context.at[me], local.at[0])
    keep_own.start()
    keep_cut.wait()
    keep_tail.wait()
    rest.wait_recv()
    spread.forward()
    spread.finish()
    sent = []
    for i, target in enumerate(ahead):
        near[i].wait_recv()
        total = dot32(heads_out[target], wo_rest[0]) + dot32(near_context[i], wo_rest[1])
        shared[i] = total.astype(jnp.bfloat16)
        copy = remote(
            shared.at[i], arriving.at[i], part_send.at[i], part_recv.at[i], "frame", target
        )
        copy.start()
        sent.append(copy)
    keep_own.wait()
    for d, source in enumerate(sources):
        ref = context.at[source]
        remote(ref, ref, ctx_send.at[d], ctx_recv.at[d], "frame", partner).wait_recv()
    wide = math.gcd(cut, 512)
    for c in range(cut // wide):
        total = dot32(context[0], wo_all[0, :, c * wide : (c + 1) * wide])
        for f in range(1, frames):
            total = total + dot32(context[f], wo_all[f, :, c * wide : (c + 1) * wide])
        mixed_ref[:, c * wide : (c + 1) * wide] = total.astype(mixed_ref.dtype)
    total = dot32(context[me], wo_rest[0]) + dot32(context[partner], wo_rest[1])
    for i in range(len(ahead)):
        ref = arriving.at[i]
        remote(ref, ref, part_send.at[i], part_recv.at[i], "frame", partner).wait_recv()
        total = total + arriving[i].astype(jnp.float32)
    mixed_ref[:, cut:] = total.astype(mixed_ref.dtype)
    rest.wait_send()
    for copy in copies + near + sent:
        copy.wait_send()
    relay.finish(crossed=False)


def attend(q, kv, wo, kv_heads, group):
    frames, own_rows, width = q.shape
    seqs = lax.axis_size("seq")
    depth, out_cols = wo.shape
    cut = out_cols // 2
    rest = out_cols - cut
    sub = math.gcd(own_rows, 32)
    blocks, rows = own_rows // sub, group * frames * sub
    head = HEAD_WIDTH
    others = max(1, frames // 2 - 1)
    chunks = 2
    dma = pltpu.SemaphoreType.DMA
    vmem = pl.BlockSpec(memory_space=pltpu.VMEM)
    return pl.pallas_call(
        functools.partial(
            attend_kernel, count=chunks, kv_heads=kv_heads, group=group, sub=sub
        ),
        in_specs=[vmem, vmem, pl.BlockSpec(memory_space=pl.ANY)],
        out_specs=vmem,
        out_shape=jax.ShapeDtypeStruct((own_rows, out_cols), jnp.bfloat16),
        scratch_shapes=[
            pltpu.VMEM((seqs,) + kv.shape, kv.dtype),
            pltpu.VMEM((kv_heads, blocks, rows, head), jnp.bfloat16),
            pltpu.VMEM((kv_heads, blocks, rows, 1), jnp.float32),
            pltpu.VMEM((kv_heads, blocks, rows, 2 * head), jnp.float32),
            pltpu.VMEM(q.shape, jnp.bfloat16),
            pltpu.VMEM(q.shape, jnp.bfloat16),
            pltpu.VMEM((others, own_rows, rest), jnp.bfloat16),
            pltpu.VMEM((others, own_rows, width), jnp.bfloat16),
            pltpu.VMEM((frames, depth, cut), jnp.bfloat16),
            pltpu.VMEM((2, depth, rest), jnp.bfloat16),
            pltpu.VMEM((others, own_rows, rest), jnp.bfloat16),
            dma((3,)),
            dma((frames - 1,)),
            dma((frames - 1,)),
            dma((2,)),
            dma((frames - 1,)),
            dma((frames - 1,)),
            dma((others,)),
            dma((others,)),
            dma((others,)),
            dma((others,)),
        ]
        + relay_scratch(chunks),
        compiler_params=pltpu.CompilerParams(
            collective_id=3, has_side_effects=True, vmem_limit_bytes=56 * 1024 * 1024
        ),
        cost_estimate=pl.CostEstimate(
            flops=40_000_000_000, bytes_accessed=0, transcendentals=0
        ),
        name="attend",
    )(q, kv, wo)


class SeqRelay:
    def __init__(self, x_ref, out_ref, sems, count):
        seqs = lax.axis_size("seq")
        self.x, self.out, self.count = x_ref, out_ref, count
        self.send_r, self.recv_r, self.send_l, self.recv_l, self.send_y, self.recv_y = sems
        self.depth = x_ref.shape[0] // count
        self.breadth = 2 if seqs % 2 == 0 else 1
        self.length = seqs // self.breadth
        self.me = lax.axis_index("seq")
        self.a, self.b = self.me // self.breadth, self.me % self.breadth
        self.across = self.a * self.breadth + (self.breadth - 1 - self.b)
        self.has_right, self.has_left = self.a + 1 < self.length, self.a > 0

    def greet(self, barrier):
        breadth = self.breadth
        pl.when(self.has_right)(lambda: greet(barrier, "seq", self.me + breadth))
        pl.when(self.has_left)(lambda: greet(barrier, "seq", self.me - breadth))
        if breadth == 2:
            greet(barrier, "seq", self.across)

    def peers(self):
        sides = self.has_right.astype(jnp.int32) + self.has_left.astype(jnp.int32)
        return sides + (self.breadth - 1)

    def slot(self, source, b, i):
        return self.out.at[source * self.breadth + b, pl.ds(i * self.depth, self.depth)]

    def own(self, i):
        return self.x.at[pl.ds(i * self.depth, self.depth)]

    def shift(self, i, k, right, own=False):
        slot = self.slot(self.a - k if right else self.a + k, self.b, i)
        send, recv = (self.send_r, self.recv_r) if right else (self.send_l, self.recv_l)
        src = self.own(i) if own else slot
        target = self.me + self.breadth if right else self.me - self.breadth
        return remote(src, slot, send.at[i, k], recv.at[i, k], "seq", target)

    def cross(self, i, source, own):
        slot = self.slot(source, self.b, i)
        src = self.own(i) if own else slot
        return remote(src, slot, self.send_y.at[i, source], self.recv_y.at[i, source], "seq", self.across)

    def incoming(self, i, k, right):
        slot = self.slot(self.a - k if right else self.a + k, self.b, i)
        recv = self.recv_r if right else self.recv_l
        return remote(slot, slot, self.send_r.at[i, 0], recv.at[i, k - 1], "seq", self.across)

    def incoming_cross(self, i, source):
        slot = self.slot(source, self.breadth - 1 - self.b, i)
        return remote(slot, slot, self.send_r.at[i, 0], self.recv_y.at[i, source], "seq", self.across)

    def held(self, k, right):
        held = (self.a >= k) if right else (self.a + k < self.length)
        return held, held & (self.has_right if right else self.has_left)

    def first(self):
        for i in range(self.count):
            for right in (True, False):
                pl.when(self.held(0, right)[1])(lambda: self.shift(i, 0, right, True).start())
            if self.breadth == 2:
                self.cross(i, self.a, True).start()

    def step(self, k):
        for i in range(self.count):
            for right in (True, False):
                held, onward = self.held(k, right)
                source = self.a - k if right else self.a + k
                pl.when(held)(lambda: self.incoming(i, k, right).wait_recv())
                pl.when(onward)(lambda: self.shift(i, k, right).start())
                if self.breadth == 2:
                    pl.when(held)(lambda: self.cross(i, source, False).start())

    def finish(self, crossed=True):
        for i in range(self.count):
            for k in range(self.length):
                for right in (True, False):
                    onward = self.held(k, right)[1]
                    pl.when(onward)(lambda: self.shift(i, k, right).wait_send())
                if self.breadth == 2:
                    if crossed:
                        self.incoming_cross(i, k).wait_recv()
                    self.cross(i, k, False).wait_send()


def per_device(
    vit_states,
    frame_slot,
    patch_count,
    vis_start,
    text_embed,
    vit_ln_gain,
    vit_ln_bias,
    vit_qkv_w,
    vit_qkv_b,
    vit_out_w,
    vit_out_b,
    proj_w,
    proj_b,
    attn_gain,
    wq,
    wk,
    wv,
    wo,
):
    frames_n = lax.axis_size("frame")
    seqs_n = lax.axis_size("seq")
    chips = frames_n // 2
    devices_n = frames_n * seqs_n
    me = lax.axis_index("frame")
    my_seq = lax.axis_index("seq")
    slots_held, frame_max, width_vit = vit_states.shape
    vis_max = frame_max // 4
    own_rows, model_width = text_embed.shape[0], text_embed.shape[2]
    head_size = width_vit // VHEADS
    my_heads = VHEADS // frames_n
    cols = width_vit // frames_n

    w_parts = [
        lax.dynamic_slice_in_dim(vit_qkv_w, i * width_vit + me * cols, cols, 1) for i in range(3)
    ]
    out_own = lax.dynamic_slice_in_dim(vit_out_w, me * cols, cols, 1)
    own_weights = jnp.concatenate(w_parts + [out_own], 1)
    qkv_bias = [
        lax.dynamic_slice_in_dim(vit_qkv_b, i * width_vit + me * cols, cols, 0) for i in range(3)
    ]
    out_bias = lax.dynamic_slice_in_dim(vit_out_b, me * cols, cols, 0)

    frame_ids = jnp.arange(frame_slot.shape[0])
    holder = frame_slot // slots_held
    holder_frame = holder // seqs_n
    pair_low = (holder_frame - holder_frame % 2) * seqs_n + holder % seqs_n
    pair_order = holder_frame % 2 * slots_held + frame_slot % slots_held
    same_pair = pair_low[:, None] == pair_low[None, :]
    earlier = pair_order[None, :] < pair_order[:, None]
    pair_rank = jnp.sum((same_pair & earlier).astype(jnp.int32), axis=1)
    source_frame = pair_low // seqs_n + pair_rank
    source_seq = pair_low % seqs_n
    mine_low = (source_seq == my_seq) & (pair_low // seqs_n == me - me % 2)
    orders = [
        jnp.sum(jnp.where(mine_low & (pair_rank == (me % 2 ^ i)), pair_order, 0)) for i in range(2)
    ]
    group_hit = (source_frame[None, :] == jnp.arange(frames_n)[:, None]) & (
        source_seq == my_seq
    )[None, :]
    group_count = jnp.sum(jnp.where(group_hit, patch_count[None, :], 0), axis=1)
    group_start = jnp.sum(jnp.where(group_hit, vis_start[None, :], 0), axis=1)

    both_weights, states, text_rows = front(
        jnp.stack(orders), own_weights, vit_states, text_embed.reshape(own_rows, model_width)
    )
    both_weights = both_weights.reshape(width_vit, 4 * cols)

    context, pooled_states = vit_attention(
        group_count,
        states,
        both_weights,
        vit_ln_gain.reshape(1, width_vit),
        vit_ln_bias.reshape(1, width_vit),
        jnp.concatenate(qkv_bias).reshape(1, 3 * cols),
        my_heads,
        head_size,
    )
    laps = vis_max // seqs_n
    table = route(
        group_start,
        context.reshape(frames_n * vis_max, cols),
        pooled_states.reshape(frames_n * vis_max, cols),
        both_weights,
        out_bias.reshape(1, cols),
        vis_max,
    )
    group_rows = frames_n * own_rows
    row_ids = jnp.arange(group_rows)
    positions = row_ids % own_rows * devices_n + row_ids // own_rows * seqs_n + my_seq
    query_width, kv_width = wq.shape[1], wk.shape[1]
    kv_heads = kv_width // HEAD_WIDTH
    query_heads = query_width // HEAD_WIDTH
    exponents = jnp.arange(0, HEAD_WIDTH, 2).astype(jnp.float32) / HEAD_WIDTH
    inverse = jnp.power(jnp.float32(rope_theta), -exponents)
    angles = positions.astype(jnp.float32)[:, None] * inverse[None, :]
    cosine, sine = jnp.cos(angles), jnp.sin(angles)
    as_row = lambda x: x.astype(jnp.int32).reshape(1, -1)
    queries, own_kv = merge(
        as_row(vis_start),
        as_row(patch_count // 4),
        as_row((source_seq * frames_n + source_frame) * laps),
        table,
        proj_w,
        proj_b.reshape(1, model_width),
        text_rows,
        attn_gain.reshape(1, model_width),
        wq,
        wk,
        wv,
        jnp.concatenate([cosine, cosine], 1),
        jnp.concatenate([-sine, sine], 1),
    )
    mixed = attend(
        queries.reshape(frames_n, own_rows, query_width),
        own_kv.reshape(frames_n, own_rows, 2 * kv_width),
        wo,
        kv_heads,
        query_heads // kv_heads,
    )
    return mixed.reshape(own_rows, 1, wo.shape[1])


def solution(mesh):
    return jax.shard_map(
        per_device,
        mesh=mesh,
        in_specs=(
            P(("frame", "seq"), None, None),
            P(),
            P(),
            P(),
            P(None, ("frame", "seq"), None),
            P(),
            P(),
            P("seq", None),
            P(),
            P("seq", None),
            P(),
            P(),
            P(),
            P(),
            P(None, "frame"),
            P(None, "frame"),
            P(None, "frame"),
            P("frame", None),
        ),
        out_specs=P(None, ("frame", "seq"), None),
        check_vma=False,
    )
```

```python
import functools
import math

import jax
import jax.numpy as jnp
from jax import lax
from jax.experimental import pallas as pl
from jax.experimental.pallas import tpu as pltpu
from jax.sharding import PartitionSpec as P

VHEADS = 16
HEAD_WIDTH = 128

rope_theta = 500000.0
vit_epsilon = 1e-06
norm_epsilon = 1e-05
masked_score = -1e30
LOG2E = math.log2(math.e)


def dot32(a, b):
    return jnp.dot(a, b, preferred_element_type=jnp.float32)


def ceil_to(value, step):
    return -(-value // step) * step


def encode(normed, w, qb, count, heads, head_size):
    rows = normed.shape[0]
    cols = heads * head_size
    proj = (dot32(normed, w) + qb).astype(jnp.bfloat16)
    q, k, v = (proj[:, i * cols : (i + 1) * cols] for i in range(3))
    live = lax.broadcasted_iota(jnp.int32, (1, rows), 1) < count
    blocks = [None] * pl.cdiv(cols, 128)
    scale = LOG2E / math.sqrt(head_size)
    for h in range(heads):
        low, high = h * head_size, (h + 1) * head_size
        start, stop = low // 128 * 128, min(ceil_to(high, 128), cols)
        lane = lax.broadcasted_iota(jnp.int32, (1, stop - start), 1) + start
        mine = jnp.where((lane >= low) & (lane < high), 1.0, 0.0).astype(jnp.bfloat16)
        s = lax.dot_general(
            q[:, start:stop] * mine,
            k[:, start:stop],
            (((1,), (1,)), ((), ())),
            preferred_element_type=jnp.float32,
        )
        s = jnp.where(live, s * scale, masked_score)
        e = jnp.exp2(s - jnp.max(s, axis=1, keepdims=True))
        p = (e * (1.0 / jnp.sum(e, axis=1, keepdims=True))).astype(jnp.bfloat16)
        o = dot32(p, v[:, start:stop] * mine)
        for b in range(start // 128, pl.cdiv(stop, 128)):
            part = o[:, b * 128 - start : min((b + 1) * 128, stop) - start]
            blocks[b] = part if blocks[b] is None else blocks[b] + part
    return jnp.concatenate(blocks, axis=1).astype(jnp.bfloat16)


MESH = pl.DeviceIdType.MESH


def remote(src, dst, send, recv, axis, index):
    return pltpu.make_async_remote_copy(
        src_ref=src,
        dst_ref=dst,
        send_sem=send,
        recv_sem=recv,
        device_id={axis: index},
        device_id_type=MESH,
    )


def frame_peers():
    frames = lax.axis_size("frame")
    me = lax.axis_index("frame")
    chips = frames // 2
    chip, core = me // 2, me % 2
    partner = chip * 2 + (1 - core)
    ahead = [((chip + dx) % chips) * 2 + core for dx in range(1, chips)]
    behind = [((chip + chips - dx) % chips) * 2 + core for dx in range(1, chips)]
    return me, partner, ahead, behind


def greet(barrier, axis, index):
    pl.semaphore_signal(barrier, inc=1, device_id={axis: index}, device_id_type=MESH)


class FrameSpread:
    def __init__(self, view, sems, direct=True):
        self.view = view
        self.send, self.recv = sems
        self.me, self.partner, self.ahead, self.behind = frame_peers()
        self.n = len(self.ahead)
        self.direct = direct

    def copy(self, src, slot, part, k, target):
        return remote(
            src, self.view(slot, part), self.send.at[k, part], self.recv.at[k, part], "frame", target
        )

    def arrived(self, slot, part, k):
        self.copy(self.view(slot, part), slot, part, k, self.partner).wait_recv()

    def publish(self, src, part=0):
        for i, target in enumerate(self.ahead):
            self.copy(src, self.me, part, 1 + i, target).start()
        if self.direct:
            self.copy(src, self.me, part, 0, self.partner).start()

    def forward(self, part=0):
        for i, source in enumerate(self.behind):
            self.arrived(source, part, 1 + i)
            self.copy(self.view(source, part), source, part, 1 + self.n + i, self.partner).start()

    def settle(self, part=0):
        if self.direct:
            self.arrived(self.partner, part, 0)
        for i, source in enumerate(self.behind):
            self.arrived(source + 1 - 2 * (self.me % 2), part, 1 + self.n + i)

    def drain(self, parts=1):
        for part in range(parts):
            for k in range(0 if self.direct else 1, 2 * self.n + 1):
                self.copy(self.view(self.me, part), self.me, part, k, self.partner).wait_send()


def relay_scratch(chunks):
    seqs = lax.axis_size("seq")
    length = seqs // 2 if seqs % 2 == 0 else seqs
    return [pltpu.SemaphoreType.DMA((chunks, length))] * 6 + [pltpu.SemaphoreType.DMA((2,))] * 2


def vision_kernel(
    facts_ref,
    w_ref,
    states_ref,
    text_ref,
    params_ref,
    table_out,
    text_out,
    w_all,
    states_all,
    pair,
    normed,
    ctx_all,
    pooled,
    outgoing,
    local,
    pair_sems,
    state_a,
    state_b,
    text_a,
    text_b,
    ctx_a,
    ctx_b,
    table_a,
    table_b,
    seq_send,
    seq_recv,
    *relay_sems,
    heads,
    head_size,
    chunks,
):
    frames, seqs = lax.axis_size("frame"), lax.axis_size("seq")
    seq = lax.axis_index("seq")
    me, partner, ahead, behind = frame_peers()
    core = me % 2
    slots, rows, width = states_ref.shape
    cols = heads * head_size
    vis_max = rows // 4
    depth = w_ref.shape[0]
    first_cols = ceil_to(3 * cols, 128)
    relay = SeqRelay(w_ref, w_all, relay_sems[:8], chunks, 0, first_cols)
    relay_rest = SeqRelay(w_ref, w_all, relay_sems[8:], 2, first_cols, 4 * cols - first_cols)
    states = FrameSpread(lambda slot, part: states_all.at[slot], (state_a, state_b), False)
    text = FrameSpread(lambda slot, part: text_out.at[slot], (text_a, text_b))
    context = FrameSpread(lambda slot, part: ctx_all.at[slot, part], (ctx_a, ctx_b))
    share = vis_max // seqs * frames
    laps = share // frames

    def part_of(index):
        return pl.ds(pl.multiple_of(index * share, share), share)

    table = FrameSpread(lambda slot, part: table_out.at[slot, part_of(part)], (table_a, table_b))
    others = [(seq + d) % seqs for d in range(1, seqs)]
    barrier = pltpu.get_barrier_semaphore()
    for other in others:
        greet(barrier, "seq", other)
    for peer in [partner] + ahead:
        greet(barrier, "frame", peer)
    pl.semaphore_wait(barrier, seqs - 1 + frames // 2)
    swap = remote(states_ref, pair, pair_sems.at[0], pair_sems.at[1], "frame", partner)
    swap.start()
    relay.first()
    keep_w = pltpu.make_async_copy(w_ref, w_all.at[seq], local.at[0])
    keep_w.start()
    keep_text = pltpu.make_async_copy(text_ref, text_out.at[me], local.at[1])
    keep_text.start()
    swap.wait()
    step = math.gcd(rows, 32)
    keep = [
        [
            jnp.where(facts_ref[j] == side * slots + k, 1.0, 0.0)
            for side in (core, 1 - core)
            for k in range(slots)
        ]
        for j in range(2)
    ]

    def choose(i, carry):
        at = pl.ds(pl.multiple_of(i * step, step), step)
        values = [states_ref[k, at].astype(jnp.float32) for k in range(slots)]
        values += [pair[k, at].astype(jnp.float32) for k in range(slots)]
        for j, slot in enumerate((me, partner)):
            total = keep[j][0] * values[0]
            for weight, value in zip(keep[j][1:], values[1:]):
                total = total + weight * value
            states_all[slot, at] = total.astype(states_all.dtype)
        return carry

    lax.fori_loop(0, rows // step, choose, 0)
    states.publish(states_all.at[me])
    text.publish(text_ref)
    gain, shift = params_ref[:, :width], params_ref[:, width : 2 * width]

    def own_part(at):
        total = jnp.zeros((1, cols), jnp.float32)
        for f in range(frames):
            low = at + f * cols
            total = total + jnp.where(me == f, 1.0, 0.0) * params_ref[:, low : low + cols]
        return total

    qkv_bias = jnp.concatenate([own_part((2 + i) * width) for i in range(3)], axis=1)
    out_bias = own_part(5 * width)

    def normalize(slot):
        def one(i, carry):
            at = pl.ds(pl.multiple_of(i * step, step), step)
            wide = states_all[slot, at].astype(jnp.float32)
            average = jnp.mean(wide, axis=1, keepdims=True)
            centred = wide - average
            spread = jnp.mean(centred * centred, axis=1, keepdims=True)
            value = centred * lax.rsqrt(spread + vit_epsilon) * gain + shift
            normed[slot, at] = value.astype(jnp.bfloat16)
            return carry

        lax.fori_loop(0, rows // step, one, 0)

    normalize(me)
    relay.step(1)
    normalize(partner)
    for k in range(2, relay.length):
        relay.step(k)
        if k == 2:
            states.forward()
            for source in behind:
                normalize(source)
    if relay.length <= 2:
        states.forward()
        for source in behind:
            normalize(source)
    relay_rest.first()
    states.settle()
    for source in behind:
        normalize(source + 1 - 2 * core)
    keep_w.wait()
    relay.settle()

    pr = lax.broadcasted_iota(jnp.int32, (vis_max, rows), 0)
    pc = lax.broadcasted_iota(jnp.int32, (vis_max, rows), 1)
    pool = jnp.where(pc // 4 == pr, 0.25, 0.0).astype(jnp.bfloat16)

    batch = 2 if frames % 2 == 0 else 1

    def some_frames(step_at, carry):
        f0 = step_at * batch
        w = w_all[:, :, : 3 * cols].reshape(width, 3 * cols)
        contexts, totals = [], []
        for i in range(batch):
            f = f0 + i
            result = encode(normed[f], w, qkv_bias, facts_ref[2 + f], heads, head_size)
            contexts.append(dot32(pool, result).astype(jnp.bfloat16))
            averaged = dot32(pool, states_all[f])
            total = jnp.zeros((vis_max, cols), jnp.float32)
            for g in range(frames):
                mask = jnp.where(me == g, 1.0, 0.0)
                total = total + mask * averaged[:, g * cols : (g + 1) * cols]
            totals.append(total)
        for i in range(batch):
            ctx_all[me, f0 + i] = contexts[i]
            pooled[f0 + i] = totals[i]
        for i in range(batch):
            context.publish(ctx_all.at[me, f0 + i], f0 + i)
        for i in range(batch):
            k = f0 + i + 1
            pl.when(k < relay.length)(lambda: relay_rest.step(k))
        for i in range(batch):
            k = f0 + i - batch
            pl.when(k >= 0)(lambda: context.forward(k))
        return carry

    lax.fori_loop(0, frames // batch, some_frames, 0)
    for k in range(frames + 1, relay.length):
        relay_rest.step(k)
    r = lax.broadcasted_iota(jnp.int32, (seqs * share, 1), 0)
    dest, frame, lap = r // share, r // laps % frames, r % laps
    begin = jnp.zeros((seqs * share, 1), jnp.int32)
    for f in range(frames):
        begin = begin + jnp.where(frame == f, facts_ref[2 + frames + f], 0)
    token = (dest + seqs - begin % seqs) % seqs + lap * seqs + frame * vis_max
    c = lax.broadcasted_iota(jnp.int32, (1, frames * vis_max), 1)
    pick = jnp.where(token == c, 1.0, 0.0).astype(jnp.bfloat16)
    for f in range(frames - batch, frames):
        context.forward(f)
    relay_rest.settle()
    total = pooled[...].reshape(frames * vis_max, cols) + out_bias
    for f in range(frames):
        context.settle(f)
    per = cols // depth if cols % depth == 0 else 0
    for g in range(frames):
        ctx = ctx_all[g].reshape(frames * vis_max, cols)
        if per:
            w = w_all[g * per : (g + 1) * per, :, 3 * cols :].reshape(cols, cols)
        else:
            w = w_all[:, :, 3 * cols :].reshape(width, cols)[g * cols : (g + 1) * cols]
        total = total + dot32(ctx, w)
    outgoing[...] = dot32(pick, total.astype(jnp.bfloat16)).astype(jnp.bfloat16)

    mine = table_out.at[me]
    sends = []
    for d, other in enumerate(others):
        copy = remote(
            outgoing.at[part_of(other)],
            mine.at[part_of(seq)],
            seq_send.at[d],
            seq_recv.at[d],
            "seq",
            other,
        )
        copy.start()
        sends.append(copy)
    own = pltpu.make_async_copy(outgoing.at[part_of(seq)], mine.at[part_of(seq)], local.at[2])
    own.start()
    table.publish(outgoing.at[part_of(seq)], seq)
    text.forward()
    for d in range(seqs - 1):
        source = (seq + seqs - 1 - d) % seqs
        ref = mine.at[part_of(source)]
        remote(ref, ref, seq_send.at[d], seq_recv.at[d], "seq", source).wait_recv()
        table.publish(ref, source)
    own.wait()
    keep_text.wait()
    for d in range(seqs):
        table.forward((seq + seqs - d) % seqs)
    for part in range(seqs):
        table.settle(part)
    text.settle()
    for copy in sends:
        copy.wait_send()
    states.drain()
    text.drain()
    context.drain(frames)
    table.drain(seqs)
    relay.drain()
    relay_rest.drain()


def vision(facts, weights, states, text, params, cols, heads):
    seqs, frames = lax.axis_size("seq"), lax.axis_size("frame")
    slots, rows, width = states.shape
    vis_max = rows // 4
    vmem = pl.BlockSpec(memory_space=pltpu.VMEM)
    smem = pl.BlockSpec(memory_space=pltpu.SMEM)
    dma = pltpu.SemaphoreType.DMA
    links = max(1, frames - 1)
    chunks = 2
    return pl.pallas_call(
        functools.partial(
            vision_kernel, heads=heads, head_size=cols // heads, chunks=chunks
        ),
        in_specs=[smem] + [vmem] * 4,
        out_specs=[vmem] * 2,
        out_shape=[
            jax.ShapeDtypeStruct((frames, frames * vis_max, cols), jnp.bfloat16),
            jax.ShapeDtypeStruct((frames,) + text.shape, text.dtype),
        ],
        scratch_shapes=[
            pltpu.VMEM((seqs,) + weights.shape, weights.dtype),
            pltpu.VMEM((frames, rows, width), states.dtype),
            pltpu.VMEM(states.shape, states.dtype),
            pltpu.VMEM((frames, rows, width), jnp.bfloat16),
            pltpu.VMEM((frames, frames, vis_max, cols), jnp.bfloat16),
            pltpu.VMEM((frames, vis_max, cols), jnp.float32),
            pltpu.VMEM((frames * vis_max, cols), jnp.bfloat16),
            dma((3,)),
            dma((2,)),
        ]
        + [dma((links, 1))] * 4
        + [dma((links, frames))] * 2
        + [dma((links, seqs))] * 2
        + [dma((seqs - 1,))] * 2
        + relay_scratch(chunks)
        + relay_scratch(2),
        compiler_params=pltpu.CompilerParams(
            collective_id=1, has_side_effects=True, vmem_limit_bytes=48 * 1024 * 1024
        ),
        cost_estimate=pl.CostEstimate(
            flops=40_000_000_000, bytes_accessed=0, transcendentals=0
        ),
        name="vision",
    )(facts, weights, states, text, params)


def exchange_slots(index, frames):
    return [(index + d) % frames for d in range(1, frames)], [
        (index + frames - d) % frames for d in range(1, frames)
    ]


def attend_kernel(
    begin_ref,
    length_ref,
    base_ref,
    table_ref,
    pw_ref,
    pb_ref,
    text_ref,
    gain_ref,
    wq_ref,
    wk_ref,
    wv_ref,
    cos_ref,
    sin_ref,
    wo_ref,
    mixed_ref,
    pw,
    tokens,
    hot,
    joined,
    visual_mask,
    squares,
    wk,
    wv,
    wq,
    sums,
    kv,
    qs,
    highest,
    acc,
    heads_out,
    context,
    shared,
    near_context,
    wo_all,
    wo_rest,
    arriving,
    local,
    wo_sems_a,
    wo_sems_b,
    rest_sems,
    ctx_send,
    ctx_recv,
    near_sems_a,
    near_sems_b,
    part_send,
    part_recv,
    *relay_sems,
    count,
    kv_heads,
    group,
    sub,
):
    frames, seqs = lax.axis_size("frame"), lax.axis_size("seq")
    devices = frames * seqs
    my_seq = lax.axis_index("seq")
    me, partner, ahead, behind = frame_peers()
    head = HEAD_WIDTH
    own_rows = text_ref.shape[1]
    group_rows = frames * own_rows
    steps, block = tokens.shape[0], tokens.shape[3]
    model_width = steps * block
    blocks = own_rows // sub
    q_rows = frames * sub
    rows = group * q_rows
    cut = wo_all.shape[2]
    relay = SeqRelay(kv.at[my_seq], kv, relay_sems[1:], count)
    loads = relay_sems[0]
    kv_acc, q_acc = sums.at[:, : 2 * wk.shape[1]], sums.at[:, : wq.shape[1]]
    spread = FrameSpread(lambda slot, part: wo_all.at[slot], (wo_sems_a, wo_sems_b))
    barrier = pltpu.get_barrier_semaphore()
    relay.greet(barrier)
    for d in range(1, frames):
        greet(barrier, "frame", (me + d) % frames)

    def load(i, which):
        at = pl.ds(pl.multiple_of(i * block, block), block)
        if which:
            return pltpu.make_async_copy(text_ref.at[:, :, at], tokens.at[i], loads.at[1, i])
        return pltpu.make_async_copy(pw_ref.at[:, at], pw.at[i], loads.at[0, i])

    for i in range(steps):
        load(i, 0).start()
        load(i, 1).start()
    fetch = [
        pltpu.make_async_copy(src, dst, local.at[3 + i])
        for i, (src, dst) in enumerate(((wk_ref, wk), (wv_ref, wv), (wq_ref, wq)))
    ]
    for copy in fetch:
        copy.start()

    i = lax.broadcasted_iota(jnp.int32, (group_rows, 1), 0)
    position = i % own_rows * devices + i // own_rows * seqs + my_seq
    t = lax.broadcasted_iota(jnp.int32, (1, begin_ref.shape[1]), 1)
    within_frame = position // own_rows == t

    def of_frame(ref):
        return jnp.sum(jnp.where(within_frame, ref[...], 0), axis=1, keepdims=True)

    within = position - of_frame(begin_ref)
    visual = (within >= 0) & (within < of_frame(length_ref))
    row = of_frame(base_ref) + jnp.maximum(within, 0) // seqs
    c = lax.broadcasted_iota(jnp.int32, (1, hot.shape[1]), 1)
    hot[...] = jnp.where(visual & (row == c), 1.0, 0.0).astype(jnp.bfloat16)
    visual_mask[...] = jnp.where(visual, 1.0, 0.0)
    squares[...] = jnp.zeros(squares.shape, jnp.float32)
    kv_acc[...] = jnp.zeros(kv_acc.shape, jnp.float32)
    joined[...] = jnp.concatenate([table_ref[f] for f in range(frames)], axis=1)
    pl.semaphore_wait(barrier, relay.peers() + (frames - 1))
    wo_cut, wo_tail = wo_ref.at[:, pl.ds(0, cut)], wo_ref.at[:, pl.ds(cut, wo_rest.shape[2])]
    spread.publish(wo_cut)
    rest = remote(wo_tail, wo_rest.at[1], rest_sems.at[0], rest_sems.at[1], "frame", partner)
    rest.start()
    keep_cut = pltpu.make_async_copy(wo_cut, wo_all.at[me], local.at[1])
    keep_cut.start()
    keep_tail = pltpu.make_async_copy(wo_tail, wo_rest.at[0], local.at[2])
    keep_tail.start()

    def combine(i, carry):
        load(i, 0).wait()
        load(i, 1).wait()
        total = dot32(joined[...], pw[i]) + pb_ref[i]
        fetched = dot32(hot[...], total.astype(jnp.bfloat16))
        words = tokens[i].reshape(group_rows, block).astype(jnp.float32)
        value = jnp.where(visual_mask[...] > 0.5, fetched, words)
        squares[...] += jnp.sum(value * value, axis=1, keepdims=True)
        tokens[i] = value.astype(jnp.bfloat16).reshape(frames, own_rows, block)
        return carry

    lax.fori_loop(0, steps, combine, 0)
    for copy in fetch[:2]:
        copy.wait()
    squares[...] = lax.rsqrt(squares[...] * (1.0 / model_width) + norm_epsilon)
    kw = wk.shape[1]

    def project_kv(i, carry):
        at = pl.ds(pl.multiple_of(i * block, block), block)
        value = tokens[i].reshape(group_rows, block).astype(jnp.float32)
        value = (value * squares[...] * gain_ref[i]).astype(jnp.bfloat16)
        tokens[i] = value.reshape(frames, own_rows, block)
        kv_acc[:, :kw] += dot32(value, wk[at])
        kv_acc[:, kw:] += dot32(value, wv[at])
        return carry

    lax.fori_loop(0, steps, project_kv, 0)
    for h in range(kv_heads):
        x = kv_acc[:, h * head : (h + 1) * head]
        x = x * cos_ref[...] + pltpu.roll(x, head // 2, 1) * sin_ref[...]
        x = x.astype(jnp.bfloat16).reshape(frames, own_rows, head)
        kv[my_seq, :, :, h * head : (h + 1) * head] = x
    x = kv_acc[:, kw:].astype(jnp.bfloat16).reshape(frames, own_rows, kw)
    kv[my_seq, :, :, kw:] = x
    relay.first()
    fetch[2].wait()
    q_acc[...] = jnp.zeros(q_acc.shape, jnp.float32)

    def project(i, carry):
        at = pl.ds(pl.multiple_of(i * block, block), block)
        q_acc[...] += dot32(tokens[i].reshape(group_rows, block), wq[at])
        return carry

    lax.fori_loop(0, tokens.shape[0], project, 0)
    for h in range(kv_heads * group):
        x = q_acc[:, h * head : (h + 1) * head]
        x = x * cos_ref[...] + pltpu.roll(x, head // 2, 1) * sin_ref[...]
        x = (x * (LOG2E / math.sqrt(head))).astype(jnp.bfloat16)
        heads_out[:, :, h * head : (h + 1) * head] = x.reshape(frames, own_rows, head)
    for h in range(kv_heads):
        for b in range(blocks):
            parts = [
                heads_out[:, b * sub : (b + 1) * sub, (h * group + g) * head : (h * group + g + 1) * head]
                .reshape(q_rows, head)
                for g in range(group)
            ]
            qs[h, b] = jnp.concatenate(parts, axis=0)
    highest[...] = jnp.full(highest.shape, masked_score, jnp.float32)
    acc[...] = jnp.zeros(acc.shape, jnp.float32)

    def process(source):
        for b in range(blocks):
            n = (b + 1) * sub
            keys_n = frames * n
            qi = lax.broadcasted_iota(jnp.int32, (rows, 1), 0) % q_rows
            q_at = (b * sub + qi % sub) * devices + (qi // sub) * seqs + my_seq
            ki = lax.broadcasted_iota(jnp.int32, (1, keys_n), 1)
            k_at = ki % n * devices + ki // n * seqs + source
            seen = k_at <= q_at
            ones = jnp.ones((keys_n, head), jnp.bfloat16)
            for h in range(kv_heads):
                k = kv[source, :, :n, h * head : (h + 1) * head].reshape(keys_n, head)
                v = kv[source, :, :n, (kv_heads + h) * head : (kv_heads + h + 1) * head]
                v = jnp.concatenate([v.reshape(keys_n, head), ones], axis=1)
                s = lax.dot_general(
                    qs[h, b], k, (((1,), (1,)), ((), ())), preferred_element_type=jnp.float32
                )
                s = jnp.where(seen, s, masked_score)
                m = highest[h, b]
                new = jnp.maximum(m, jnp.max(s, axis=1, keepdims=True))
                e = jnp.exp2(s - new).astype(jnp.bfloat16)
                acc[h, b] = acc[h, b] * jnp.exp2(m - new) + dot32(e, v)
                highest[h, b] = new

    def step(k, carry):
        pl.when((k > 0) & (k < relay.length))(lambda: relay.step(k))

        def one(i, c):
            crossed, side = i // 2, i % 2
            distance = k - crossed
            source = relay.a - distance + 2 * distance * side
            valid = (source >= 0) & (source < relay.length) & (distance >= 0)
            valid = valid & ((distance > 0) | (side == 0))

            @pl.when(valid)
            def _():
                if relay.breadth == 2:

                    @pl.when(crossed == 1)
                    def _():
                        relay.await_cross(source)

                row = relay.b + crossed * (1 - 2 * relay.b)
                process(source * relay.breadth + row)

            return c

        return lax.fori_loop(0, 2 * relay.breadth, one, carry)

    lax.fori_loop(0, relay.length + relay.breadth - 1, step, 0)
    for h in range(kv_heads):
        for b in range(blocks):
            out = (acc[h, b, :, :head] / acc[h, b, :, head:]).astype(jnp.bfloat16)
            for g in range(group):
                piece = out[g * q_rows : (g + 1) * q_rows].reshape(frames, sub, head)
                at = (h * group + g) * head
                heads_out[:, b * sub : (b + 1) * sub, at : at + head] = piece

    targets, sources = exchange_slots(me, frames)
    copies = []
    near = []
    for i, target in enumerate(ahead):
        near.append(
            remote(
                heads_out.at[target + 1 - 2 * (me % 2)],
                near_context.at[i],
                near_sems_a.at[i],
                near_sems_b.at[i],
                "frame",
                partner,
            )
        )
        near[-1].start()
    for d, target in enumerate(targets):
        copies.append(
            remote(
                heads_out.at[target],
                context.at[me],
                ctx_send.at[d],
                ctx_recv.at[d],
                "frame",
                target,
            )
        )
        copies[-1].start()
    keep_own = pltpu.make_async_copy(heads_out.at[me], context.at[me], local.at[0])
    keep_own.start()
    keep_tail.wait()
    rest.wait_recv()
    sent = []
    for i, target in enumerate(ahead):
        near[i].wait_recv()
        total = dot32(heads_out[target], wo_rest[0]) + dot32(near_context[i], wo_rest[1])
        shared[i] = total.astype(jnp.bfloat16)
        copy = remote(
            shared.at[i], arriving.at[i], part_send.at[i], part_recv.at[i], "frame", target
        )
        copy.start()
        sent.append(copy)
    keep_cut.wait()
    spread.forward()
    keep_own.wait()
    for d, source in enumerate(sources):
        ref = context.at[source]
        remote(ref, ref, ctx_send.at[d], ctx_recv.at[d], "frame", partner).wait_recv()
    spread.settle()
    wide = math.gcd(cut, 512)
    for c in range(cut // wide):
        total = dot32(context[0], wo_all[0, :, c * wide : (c + 1) * wide])
        for f in range(1, frames):
            total = total + dot32(context[f], wo_all[f, :, c * wide : (c + 1) * wide])
        mixed_ref[:, c * wide : (c + 1) * wide] = total.astype(mixed_ref.dtype)
    total = dot32(context[me], wo_rest[0]) + dot32(context[partner], wo_rest[1])
    for i in range(len(ahead)):
        ref = arriving.at[i]
        remote(ref, ref, part_send.at[i], part_recv.at[i], "frame", partner).wait_recv()
        total = total + arriving[i].astype(jnp.float32)
    mixed_ref[:, cut:] = total.astype(mixed_ref.dtype)
    rest.wait_send()
    spread.drain()
    for copy in copies + near + sent:
        copy.wait_send()
    relay.drain()


def attend(
    begin, length, base, table, proj_w, proj_b, text, gain, wq, wk, wv, cosine, sine, wo
):
    frames, own_rows, model_width = text.shape
    width, kw = wq.shape[1], wk.shape[1]
    kv_heads = kw // HEAD_WIDTH
    group = width // kw
    group_rows = frames * own_rows
    block = math.gcd(model_width, 512)
    steps = model_width // block
    seqs = lax.axis_size("seq")
    depth, out_cols = wo.shape
    cut = ceil_to(out_cols * 5 // 8, 512) if frames <= 4 else out_cols // 4
    rest = out_cols - cut
    sub = math.gcd(own_rows, 32)
    blocks, rows = own_rows // sub, group * frames * sub
    head = HEAD_WIDTH
    others = max(1, frames // 2 - 1)
    chunks = 2
    dma = pltpu.SemaphoreType.DMA
    vmem = pl.BlockSpec(memory_space=pltpu.VMEM)
    anywhere = pl.BlockSpec(memory_space=pl.ANY)
    return pl.pallas_call(
        functools.partial(
            attend_kernel, count=chunks, kv_heads=kv_heads, group=group, sub=sub
        ),
        in_specs=[vmem] * 4
        + [anywhere, vmem, anywhere, vmem]
        + [anywhere] * 3
        + [vmem, vmem, anywhere],
        out_specs=vmem,
        out_shape=jax.ShapeDtypeStruct((own_rows, out_cols), jnp.bfloat16),
        scratch_shapes=[
            pltpu.VMEM((steps, proj_w.shape[0], block), jnp.bfloat16),
            pltpu.VMEM((steps, frames, own_rows, block), jnp.bfloat16),
            pltpu.VMEM((group_rows, table.shape[1]), jnp.bfloat16),
            pltpu.VMEM((table.shape[1], frames * table.shape[2]), jnp.bfloat16),
            pltpu.VMEM((group_rows, 1), jnp.float32),
            pltpu.VMEM((group_rows, 1), jnp.float32),
            pltpu.VMEM(wk.shape, wk.dtype),
            pltpu.VMEM(wv.shape, wv.dtype),
            pltpu.VMEM(wq.shape, wq.dtype),
            pltpu.VMEM((group_rows, max(width, 2 * kw)), jnp.float32),
            pltpu.VMEM((seqs, frames, own_rows, 2 * kw), jnp.bfloat16),
            pltpu.VMEM((kv_heads, blocks, rows, head), jnp.bfloat16),
            pltpu.VMEM((kv_heads, blocks, rows, 1), jnp.float32),
            pltpu.VMEM((kv_heads, blocks, rows, 2 * head), jnp.float32),
            pltpu.VMEM((frames, own_rows, width), jnp.bfloat16),
            pltpu.VMEM((frames, own_rows, width), jnp.bfloat16),
            pltpu.VMEM((others, own_rows, rest), jnp.bfloat16),
            pltpu.VMEM((others, own_rows, width), jnp.bfloat16),
            pltpu.VMEM((frames, depth, cut), jnp.bfloat16),
            pltpu.VMEM((2, depth, rest), jnp.bfloat16),
            pltpu.VMEM((others, own_rows, rest), jnp.bfloat16),
            dma((6,)),
            dma((frames - 1, 1)),
            dma((frames - 1, 1)),
            dma((2,)),
            dma((frames - 1,)),
            dma((frames - 1,)),
            dma((others,)),
            dma((others,)),
            dma((others,)),
            dma((others,)),
        ]
        + [dma((2, steps))]
        + relay_scratch(chunks),
        compiler_params=pltpu.CompilerParams(
            collective_id=3, has_side_effects=True, vmem_limit_bytes=63 * 1024 * 1024
        ),
        cost_estimate=pl.CostEstimate(
            flops=40_000_000_000, bytes_accessed=0, transcendentals=0
        ),
        name="attend",
    )(
        begin,
        length,
        base,
        table,
        proj_w,
        proj_b.reshape(steps, 1, block),
        text,
        gain.reshape(steps, 1, block),
        wq,
        wk,
        wv,
        cosine,
        sine,
        wo,
    )


class SeqRelay:
    def __init__(self, x_ref, out_ref, sems, count, low=None, wide=None):
        seqs = lax.axis_size("seq")
        self.x, self.out, self.count = x_ref, out_ref, count
        self.send_r, self.recv_r, self.send_l, self.recv_l, self.send_y, self.recv_y = sems[:6]
        self.send_e, self.recv_e = sems[6:]
        self.depth = x_ref.shape[0] // count
        self.tail = () if low is None else (pl.ds(low, wide),)
        self.breadth = 2 if seqs % 2 == 0 else 1
        self.length = seqs // self.breadth
        self.me = lax.axis_index("seq")
        self.a, self.b = self.me // self.breadth, self.me % self.breadth
        self.across = self.a * self.breadth + (self.breadth - 1 - self.b)
        self.has_right, self.has_left = self.a + 1 < self.length, self.a > 0

    def greet(self, barrier):
        breadth = self.breadth
        pl.when(self.has_right)(lambda: greet(barrier, "seq", self.me + breadth))
        pl.when(self.has_left)(lambda: greet(barrier, "seq", self.me - breadth))
        if breadth == 2:
            greet(barrier, "seq", self.across)

    def peers(self):
        sides = self.has_right.astype(jnp.int32) + self.has_left.astype(jnp.int32)
        return sides + (self.breadth - 1)

    def cut(self, i):
        rows = pl.ds(i * self.depth, self.depth)
        return (rows, slice(None)) + self.tail if not self.tail else (rows,) + self.tail

    def slot(self, source, b, i):
        return self.out.at[(source * self.breadth + b,) + self.cut(i)]

    def own(self, i):
        return self.x.at[self.cut(i)]

    def shift(self, i, k, right, own=False):
        slot = self.slot(self.a - k if right else self.a + k, self.b, i)
        send, recv = (self.send_r, self.recv_r) if right else (self.send_l, self.recv_l)
        src = self.own(i) if own else slot
        target = self.me + self.breadth if right else self.me - self.breadth
        return remote(src, slot, send.at[i, k], recv.at[i, k], "seq", target)

    def cross(self, i, source, own):
        slot = self.slot(source, self.b, i)
        src = self.own(i) if own else slot
        return remote(src, slot, self.send_y.at[i, source], self.recv_y.at[i, source], "seq", self.across)

    def incoming(self, i, k, right):
        slot = self.slot(self.a - k if right else self.a + k, self.b, i)
        recv = self.recv_r if right else self.recv_l
        return remote(slot, slot, self.send_r.at[i, 0], recv.at[i, k - 1], "seq", self.across)

    def incoming_cross(self, i, source):
        slot = self.slot(source, self.breadth - 1 - self.b, i)
        return remote(slot, slot, self.send_r.at[i, 0], self.recv_y.at[i, source], "seq", self.across)

    def held(self, k, right):
        held = (self.a >= k) if right else (self.a + k < self.length)
        return held, held & (self.has_right if right else self.has_left)

    def first(self):
        for i in range(self.count):
            for right in (True, False):
                pl.when(self.held(0, right)[1])(lambda: self.shift(i, 0, right, True).start())
            if self.breadth == 2:
                self.cross(i, self.a, True).start()

    def balanced(self):
        return self.breadth == 2 and self.length > 1

    def extra(self, right):
        source = 0 if right else self.length - 1
        slot = self.slot(source, self.breadth - 1 - self.b, self.count - 1)
        side = 0 if right else 1
        target = self.me + self.breadth if right else self.me - self.breadth
        return remote(slot, slot, self.send_e.at[side], self.recv_e.at[side], "seq", target)

    def at_end(self, right):
        return self.a == (0 if right else self.length - 1)

    def onward(self, i, source, start):
        if self.balanced() and i == self.count - 1:
            end = (source == 0) | (source == self.length - 1)
            pl.when(jnp.logical_not(end))(start)
        else:
            start()

    def step(self, k):
        for i in range(self.count):
            for right in (True, False):
                held, onward = self.held(k, right)
                source = self.a - k if right else self.a + k
                pl.when(held)(lambda: self.incoming(i, k, right).wait_recv())
                pl.when(onward)(lambda: self.shift(i, k, right).start())
                if self.breadth == 2:

                    @pl.when(held)
                    def _():
                        self.onward(i, source, lambda: self.cross(i, source, False).start())

        if self.balanced():
            for right in (True, False):
                distance = self.a if right else self.length - 1 - self.a

                @pl.when(distance == k - 1)
                def _():
                    @pl.when(distance == 0)
                    def _():
                        self.incoming_cross(self.count - 1, self.a).wait_recv()

                    pl.when(distance > 0)(lambda: self.extra(right).wait_recv())
                    self.extra(right).start()

    def await_cross(self, source):
        for i in range(self.count):
            if self.balanced() and i == self.count - 1:
                end = (source == 0) | (source == self.length - 1)
                pl.when(jnp.logical_not(end))(
                    lambda: self.incoming_cross(i, source).wait_recv()
                )
                for right in (True, False):
                    last = self.at_end(not right) & (source == (0 if right else self.length - 1))
                    pl.when(last)(lambda: self.extra(right).wait_recv())
            else:
                self.incoming_cross(i, source).wait_recv()

    def settle(self):
        if self.breadth == 2:
            for k in range(self.length):
                self.await_cross(k)

    def drain(self):
        for i in range(self.count):
            for k in range(self.length):
                for right in (True, False):
                    onward = self.held(k, right)[1]
                    pl.when(onward)(lambda: self.shift(i, k, right).wait_send())
                if self.breadth == 2:
                    if self.balanced() and i == self.count - 1:
                        end = k == 0 or k == self.length - 1
                        pl.when((self.a == k) | (not end))(
                            lambda: self.cross(i, k, False).wait_send()
                        )
                    else:
                        self.cross(i, k, False).wait_send()
        if self.balanced():
            for right in (True, False):
                far = self.at_end(not right)
                pl.when(jnp.logical_not(far))(lambda: self.extra(right).wait_send())


def per_device(
    vit_states,
    frame_slot,
    patch_count,
    vis_start,
    text_embed,
    vit_ln_gain,
    vit_ln_bias,
    vit_qkv_w,
    vit_qkv_b,
    vit_out_w,
    vit_out_b,
    proj_w,
    proj_b,
    attn_gain,
    wq,
    wk,
    wv,
    wo,
):
    frames_n = lax.axis_size("frame")
    seqs_n = lax.axis_size("seq")
    chips = frames_n // 2
    devices_n = frames_n * seqs_n
    me = lax.axis_index("frame")
    my_seq = lax.axis_index("seq")
    slots_held, frame_max, width_vit = vit_states.shape
    vis_max = frame_max // 4
    own_rows, model_width = text_embed.shape[0], text_embed.shape[2]
    head_size = width_vit // VHEADS
    my_heads = VHEADS // frames_n
    cols = width_vit // frames_n

    w_parts = [
        lax.dynamic_slice_in_dim(vit_qkv_w, i * width_vit + me * cols, cols, 1) for i in range(3)
    ]
    out_own = lax.dynamic_slice_in_dim(vit_out_w, me * cols, cols, 1)
    own_weights = jnp.concatenate(w_parts + [out_own], 1)
    params = jnp.concatenate([vit_ln_gain, vit_ln_bias, vit_qkv_b, vit_out_b]).reshape(1, -1)

    holder = frame_slot // slots_held
    holder_frame = holder // seqs_n
    pair_low = (holder_frame - holder_frame % 2) * seqs_n + holder % seqs_n
    pair_order = holder_frame % 2 * slots_held + frame_slot % slots_held
    same_pair = pair_low[:, None] == pair_low[None, :]
    earlier = pair_order[None, :] < pair_order[:, None]
    pair_rank = jnp.sum((same_pair & earlier).astype(jnp.int32), axis=1)
    source_frame = pair_low // seqs_n + pair_rank
    source_seq = pair_low % seqs_n
    entry = jnp.arange(2 + 2 * frames_n)[:, None]
    wanted = jnp.where(entry < 2, me - me % 2 + (me % 2 + entry) % 2, (entry - 2) % frames_n)
    chosen = (source_frame[None, :] == wanted) & (source_seq[None, :] == my_seq)
    kind = jnp.where(
        entry < 2,
        pair_order[None, :],
        jnp.where(entry < 2 + frames_n, patch_count[None, :], vis_start[None, :]),
    )
    facts = jnp.sum(jnp.where(chosen, kind, 0), axis=1)

    table, text_rows = vision(
        facts,
        own_weights,
        vit_states,
        text_embed.reshape(own_rows, model_width),
        params,
        cols,
        my_heads,
    )
    laps = vis_max // seqs_n
    group_rows = frames_n * own_rows
    row_ids = jnp.arange(group_rows)
    positions = row_ids % own_rows * devices_n + row_ids // own_rows * seqs_n + my_seq
    exponents = jnp.arange(0, HEAD_WIDTH, 2).astype(jnp.float32) / HEAD_WIDTH
    inverse = jnp.power(jnp.float32(rope_theta), -exponents)
    angles = positions.astype(jnp.float32)[:, None] * inverse[None, :]
    cosine, sine = jnp.cos(angles), jnp.sin(angles)
    as_row = lambda x: x.astype(jnp.int32).reshape(1, -1)
    cosine, sine = jnp.concatenate([cosine, cosine], 1), jnp.concatenate([-sine, sine], 1)
    mixed = attend(
        as_row(vis_start),
        as_row(patch_count // 4),
        as_row((source_seq * frames_n + source_frame) * laps),
        table,
        proj_w,
        proj_b,
        text_rows,
        attn_gain,
        wq,
        wk,
        wv,
        cosine,
        sine,
        wo,
    )
    return mixed.reshape(own_rows, 1, wo.shape[1])


def solution(mesh):
    return jax.shard_map(
        per_device,
        mesh=mesh,
        in_specs=(
            P(("frame", "seq"), None, None),
            P(),
            P(),
            P(),
            P(None, ("frame", "seq"), None),
            P(),
            P(),
            P("seq", None),
            P(),
            P("seq", None),
            P(),
            P(),
            P(),
            P(),
            P(None, "frame"),
            P(None, "frame"),
            P(None, "frame"),
            P("frame", None),
        ),
        out_specs=P(None, ("frame", "seq"), None),
        check_vma=False,
    )
```

```python
import functools
import math

import jax
import jax.numpy as jnp
import numpy as np
from jax import lax
from jax.experimental import pallas as pl
from jax.experimental.pallas import tpu as pltpu
from jax.sharding import PartitionSpec as P

VHEADS = 16
HEAD_WIDTH = 128

rope_theta = 500000.0
vit_epsilon = 1e-06
norm_epsilon = 1e-05
masked_score = -1e30
LOG2E = math.log2(math.e)


def dot32(a, b):
    return jnp.dot(a, b, preferred_element_type=jnp.float32)


def ceil_to(value, step):
    return -(-value // step) * step


def encode(normed, w, qb, count, heads, head_size):
    rows = normed.shape[0]
    cols = heads * head_size
    proj = (dot32(normed, w) + qb).astype(jnp.bfloat16)
    q, k, v = (proj[:, i * cols : (i + 1) * cols] for i in range(3))
    live = lax.broadcasted_iota(jnp.int32, (1, rows), 1) < count
    blocks = [None] * pl.cdiv(cols, 128)
    scale = LOG2E / math.sqrt(head_size)
    for h in range(heads):
        low, high = h * head_size, (h + 1) * head_size
        start, stop = low // 128 * 128, min(ceil_to(high, 128), cols)
        lane = lax.broadcasted_iota(jnp.int32, (1, stop - start), 1) + start
        mine = jnp.where((lane >= low) & (lane < high), 1.0, 0.0).astype(jnp.bfloat16)
        s = lax.dot_general(
            q[:, start:stop] * mine,
            k[:, start:stop],
            (((1,), (1,)), ((), ())),
            preferred_element_type=jnp.float32,
        )
        s = jnp.where(live, s * scale, masked_score)
        e = jnp.exp2(s - jnp.max(s, axis=1, keepdims=True))
        p = (e * (1.0 / jnp.sum(e, axis=1, keepdims=True))).astype(jnp.bfloat16)
        o = dot32(p, v[:, start:stop] * mine)
        for b in range(start // 128, pl.cdiv(stop, 128)):
            part = o[:, b * 128 - start : min((b + 1) * 128, stop) - start]
            blocks[b] = part if blocks[b] is None else blocks[b] + part
    return jnp.concatenate(blocks, axis=1).astype(jnp.bfloat16)


MESH = pl.DeviceIdType.MESH


def remote(src, dst, send, recv, axis, index):
    return pltpu.make_async_remote_copy(
        src_ref=src,
        dst_ref=dst,
        send_sem=send,
        recv_sem=recv,
        device_id={axis: index},
        device_id_type=MESH,
    )


def frame_peers():
    frames = lax.axis_size("frame")
    me = lax.axis_index("frame")
    chips = frames // 2
    chip, core = me // 2, me % 2
    partner = chip * 2 + (1 - core)
    ahead = [((chip + dx) % chips) * 2 + core for dx in range(1, chips)]
    behind = [((chip + chips - dx) % chips) * 2 + core for dx in range(1, chips)]
    return me, partner, ahead, behind


def greet(barrier, axis, index):
    pl.semaphore_signal(barrier, inc=1, device_id={axis: index}, device_id_type=MESH)


class FrameSpread:
    def __init__(self, view, sems, direct=True):
        self.view = view
        self.send, self.recv = sems
        self.me, self.partner, self.ahead, self.behind = frame_peers()
        self.n = len(self.ahead)
        self.direct = direct

    def copy(self, src, slot, part, k, target):
        return remote(
            src, self.view(slot, part), self.send.at[k, part], self.recv.at[k, part], "frame", target
        )

    def arrived(self, slot, part, k):
        self.copy(self.view(slot, part), slot, part, k, self.partner).wait_recv()

    def publish(self, src, part=0):
        for i, target in enumerate(self.ahead):
            self.copy(src, self.me, part, 1 + i, target).start()
        if self.direct:
            self.copy(src, self.me, part, 0, self.partner).start()

    def forward(self, part=0):
        for i, source in enumerate(self.behind):
            self.arrived(source, part, 1 + i)
            self.copy(self.view(source, part), source, part, 1 + self.n + i, self.partner).start()

    def settle(self, part=0):
        if self.direct:
            self.arrived(self.partner, part, 0)
        for i, source in enumerate(self.behind):
            self.arrived(source + 1 - 2 * (self.me % 2), part, 1 + self.n + i)

    def drain(self, parts=1):
        for part in range(parts):
            for k in range(0 if self.direct else 1, 2 * self.n + 1):
                self.copy(self.view(self.me, part), self.me, part, k, self.partner).wait_send()


def relay_scratch(chunks):
    seqs = lax.axis_size("seq")
    length = seqs // 2 if seqs % 2 == 0 else seqs
    return [pltpu.SemaphoreType.DMA((chunks, length))] * 6 + [pltpu.SemaphoreType.DMA((2,))] * 2


def vision_kernel(
    facts_ref,
    w_ref,
    states_ref,
    text_ref,
    params_ref,
    table_out,
    text_out,
    w_all,
    states_all,
    pair,
    normed,
    ctx_all,
    pooled,
    outgoing,
    local,
    pair_sems,
    state_a,
    state_b,
    text_a,
    text_b,
    ctx_a,
    ctx_b,
    table_a,
    table_b,
    seq_send,
    seq_recv,
    *relay_sems,
    heads,
    head_size,
    chunks,
):
    frames, seqs = lax.axis_size("frame"), lax.axis_size("seq")
    seq = lax.axis_index("seq")
    me, partner, ahead, behind = frame_peers()
    core = me % 2
    slots, rows, width = states_ref.shape
    cols = heads * head_size
    vis_max = rows // 4
    depth = w_ref.shape[0]
    first_cols = ceil_to(3 * cols, 128)
    relay = SeqRelay(w_ref, w_all, relay_sems[:8], chunks, 0, first_cols)
    relay_rest = SeqRelay(w_ref, w_all, relay_sems[8:], 2, first_cols, 4 * cols - first_cols)
    states = FrameSpread(lambda slot, part: states_all.at[slot], (state_a, state_b), False)
    pieces = text_a.shape[1]
    piece = text_ref.shape[0] // pieces

    def piece_of(part):
        return pl.ds(pl.multiple_of(part * piece, piece), piece)

    text = FrameSpread(lambda slot, part: text_out.at[slot, piece_of(part)], (text_a, text_b))

    def publish_text(part):
        text.publish(text_ref.at[piece_of(part)], part)

    context = FrameSpread(lambda slot, part: ctx_all.at[slot, part], (ctx_a, ctx_b))
    share = vis_max // seqs * frames
    laps = share // frames

    def part_of(index):
        return pl.ds(pl.multiple_of(index * share, share), share)

    table = FrameSpread(lambda slot, part: table_out.at[slot, part_of(part)], (table_a, table_b))
    others = [(seq + d) % seqs for d in range(1, seqs)]
    barrier = pltpu.get_barrier_semaphore()
    for other in others:
        greet(barrier, "seq", other)
    for peer in [partner] + ahead:
        greet(barrier, "frame", peer)
    pl.semaphore_wait(barrier, seqs - 1 + frames // 2)
    swap = remote(states_ref, pair, pair_sems.at[0], pair_sems.at[1], "frame", partner)
    swap.start()
    relay.first()
    keep_w = pltpu.make_async_copy(w_ref, w_all.at[seq], local.at[0])
    keep_w.start()
    keep_text = pltpu.make_async_copy(text_ref, text_out.at[me], local.at[1])
    keep_text.start()
    swap.wait()
    step = math.gcd(rows, 32)
    keep = [
        [
            jnp.where(facts_ref[j] == side * slots + k, 1.0, 0.0)
            for side in (core, 1 - core)
            for k in range(slots)
        ]
        for j in range(2)
    ]

    def choose(i, carry):
        at = pl.ds(pl.multiple_of(i * step, step), step)
        values = [states_ref[k, at].astype(jnp.float32) for k in range(slots)]
        values += [pair[k, at].astype(jnp.float32) for k in range(slots)]
        for j, slot in enumerate((me, partner)):
            total = keep[j][0] * values[0]
            for weight, value in zip(keep[j][1:], values[1:]):
                total = total + weight * value
            states_all[slot, at] = total.astype(states_all.dtype)
        return carry

    lax.fori_loop(0, rows // step, choose, 0)
    states.publish(states_all.at[me])
    early = max(pieces - 1, 1)
    for part in range(early):
        publish_text(part)
    gain, shift = params_ref[:, :width], params_ref[:, width : 2 * width]

    def own_part(at):
        total = jnp.zeros((1, cols), jnp.float32)
        for f in range(frames):
            low = at + f * cols
            total = total + jnp.where(me == f, 1.0, 0.0) * params_ref[:, low : low + cols]
        return total

    qkv_bias = jnp.concatenate([own_part((2 + i) * width) for i in range(3)], axis=1)
    out_bias = own_part(5 * width)

    def normalize(slot):
        def one(i, carry):
            at = pl.ds(pl.multiple_of(i * step, step), step)
            wide = states_all[slot, at].astype(jnp.float32)
            average = jnp.mean(wide, axis=1, keepdims=True)
            centred = wide - average
            spread = jnp.mean(centred * centred, axis=1, keepdims=True)
            value = centred * lax.rsqrt(spread + vit_epsilon) * gain + shift
            normed[slot, at] = value.astype(jnp.bfloat16)
            return carry

        lax.fori_loop(0, rows // step, one, 0)

    normalize(me)
    relay.step(1)
    normalize(partner)
    for k in range(2, relay.length):
        relay.step(k)
        if k == 2:
            states.forward()
            for source in behind:
                normalize(source)
    if relay.length <= 2:
        states.forward()
        for source in behind:
            normalize(source)
    relay_rest.first()
    states.settle()
    for source in behind:
        normalize(source + 1 - 2 * core)
    keep_w.wait()
    relay.settle()

    pr = lax.broadcasted_iota(jnp.int32, (vis_max, rows), 0)
    pc = lax.broadcasted_iota(jnp.int32, (vis_max, rows), 1)
    pool = jnp.where(pc // 4 == pr, 0.25, 0.0).astype(jnp.bfloat16)

    batch = 2 if frames % 2 == 0 else 1

    def some_frames(step_at, carry):
        f0 = step_at * batch
        w = w_all[:, :, : 3 * cols].reshape(width, 3 * cols)
        contexts, totals = [], []
        for i in range(batch):
            f = f0 + i
            result = encode(normed[f], w, qkv_bias, facts_ref[2 + f], heads, head_size)
            contexts.append(dot32(pool, result).astype(jnp.bfloat16))
            averaged = dot32(pool, states_all[f])
            total = jnp.zeros((vis_max, cols), jnp.float32)
            for g in range(frames):
                mask = jnp.where(me == g, 1.0, 0.0)
                total = total + mask * averaged[:, g * cols : (g + 1) * cols]
            totals.append(total)
        for i in range(batch):
            ctx_all[me, f0 + i] = contexts[i]
            pooled[f0 + i] = totals[i]
        for i in range(batch):
            context.publish(ctx_all.at[me, f0 + i], f0 + i)
        if early < pieces:
            pl.when(step_at == frames // batch - 1)(lambda: publish_text(pieces - 1))
        for i in range(batch):
            k = f0 + i + 1
            pl.when(k < relay.length)(lambda: relay_rest.step(k))
        for i in range(batch):
            k = f0 + i - batch
            pl.when(k >= 0)(lambda: context.forward(k))
        return carry

    lax.fori_loop(0, frames // batch, some_frames, 0)
    for k in range(frames + 1, relay.length):
        relay_rest.step(k)
    r = lax.broadcasted_iota(jnp.int32, (seqs * share, 1), 0)
    dest, frame, lap = r // share, r // laps % frames, r % laps
    begin = jnp.zeros((seqs * share, 1), jnp.int32)
    for f in range(frames):
        begin = begin + jnp.where(frame == f, facts_ref[2 + frames + f], 0)
    token = (dest + seqs - begin % seqs) % seqs + lap * seqs + frame * vis_max
    c = lax.broadcasted_iota(jnp.int32, (1, frames * vis_max), 1)
    pick = jnp.where(token == c, 1.0, 0.0).astype(jnp.bfloat16)
    for f in range(frames - batch, frames):
        context.forward(f)
    relay_rest.settle()
    total = pooled[...].reshape(frames * vis_max, cols) + out_bias
    for f in range(frames):
        context.settle(f)
    per = cols // depth if cols % depth == 0 else 0
    for g in range(frames):
        ctx = ctx_all[g].reshape(frames * vis_max, cols)
        if per:
            w = w_all[g * per : (g + 1) * per, :, 3 * cols :].reshape(cols, cols)
        else:
            w = w_all[:, :, 3 * cols :].reshape(width, cols)[g * cols : (g + 1) * cols]
        total = total + dot32(ctx, w)
    outgoing[...] = dot32(pick, total.astype(jnp.bfloat16)).astype(jnp.bfloat16)

    mine = table_out.at[me]
    sends = []
    for d, other in enumerate(others):
        copy = remote(
            outgoing.at[part_of(other)],
            mine.at[part_of(seq)],
            seq_send.at[d],
            seq_recv.at[d],
            "seq",
            other,
        )
        copy.start()
        sends.append(copy)
    own = pltpu.make_async_copy(outgoing.at[part_of(seq)], mine.at[part_of(seq)], local.at[2])
    own.start()
    table.publish(outgoing.at[part_of(seq)], seq)
    for part in range(pieces):
        text.forward(part)
    for d in range(seqs - 1):
        source = (seq + seqs - 1 - d) % seqs
        ref = mine.at[part_of(source)]
        remote(ref, ref, seq_send.at[d], seq_recv.at[d], "seq", source).wait_recv()
        table.publish(ref, source)
    own.wait()
    keep_text.wait()
    for d in range(seqs):
        table.forward((seq + seqs - d) % seqs)
    for part in range(seqs):
        table.settle(part)
    for part in range(pieces):
        text.settle(part)
    for copy in sends:
        copy.wait_send()
    states.drain()
    text.drain(pieces)
    context.drain(frames)
    table.drain(seqs)
    relay.drain()
    relay_rest.drain()


def vision(facts, weights, states, text, params, cols, heads):
    seqs, frames = lax.axis_size("seq"), lax.axis_size("frame")
    slots, rows, width = states.shape
    vis_max = rows // 4
    vmem = pl.BlockSpec(memory_space=pltpu.VMEM)
    smem = pl.BlockSpec(memory_space=pltpu.SMEM)
    dma = pltpu.SemaphoreType.DMA
    links = max(1, frames - 1)
    chunks = 2
    return pl.pallas_call(
        functools.partial(
            vision_kernel, heads=heads, head_size=cols // heads, chunks=chunks
        ),
        in_specs=[smem] + [vmem] * 4,
        out_specs=[vmem, pl.BlockSpec(memory_space=pl.ANY)],
        out_shape=[
            jax.ShapeDtypeStruct((frames, frames * vis_max, cols), jnp.bfloat16),
            jax.ShapeDtypeStruct((frames,) + text.shape, text.dtype),
        ],
        scratch_shapes=[
            pltpu.VMEM((seqs,) + weights.shape, weights.dtype),
            pltpu.VMEM((frames, rows, width), states.dtype),
            pltpu.VMEM(states.shape, states.dtype),
            pltpu.VMEM((frames, rows, width), jnp.bfloat16),
            pltpu.VMEM((frames, frames, vis_max, cols), jnp.bfloat16),
            pltpu.VMEM((frames, vis_max, cols), jnp.float32),
            pltpu.VMEM((frames * vis_max, cols), jnp.bfloat16),
            dma((3,)),
            dma((2,)),
        ]
        + [dma((links, 1))] * 2
        + [dma((links, math.gcd(text.shape[0], 4)))] * 2
        + [dma((links, frames))] * 2
        + [dma((links, seqs))] * 2
        + [dma((seqs - 1,))] * 2
        + relay_scratch(chunks)
        + relay_scratch(2),
        compiler_params=pltpu.CompilerParams(
            collective_id=1, has_side_effects=True, vmem_limit_bytes=48 * 1024 * 1024
        ),
        cost_estimate=pl.CostEstimate(
            flops=40_000_000_000, bytes_accessed=0, transcendentals=0
        ),
        name="vision",
    )(facts, weights, states, text, params)


def exchange_slots(index, frames):
    return [(index + d) % frames for d in range(1, frames)], [
        (index + frames - d) % frames for d in range(1, frames)
    ]


def attend_kernel(
    info_ref,
    table_ref,
    pw_ref,
    pb_ref,
    text_ref,
    gain_ref,
    wq_ref,
    wk_ref,
    wv_ref,
    base_turns_ref,
    seq_turns_ref,
    wo_ref,
    mixed_ref,
    pw,
    tokens,
    hot,
    joined,
    visual_mask,
    squares,
    wk,
    wv,
    wq,
    turns,
    sums,
    kv,
    qs,
    highest,
    acc,
    heads_out,
    context,
    shared,
    near_context,
    wo_all,
    wo_rest,
    arriving,
    local,
    wo_sems_a,
    wo_sems_b,
    rest_sems,
    ctx_send,
    ctx_recv,
    near_sems_a,
    near_sems_b,
    part_send,
    part_recv,
    *relay_sems,
    count,
    kv_heads,
    group,
    sub,
):
    frames, seqs = lax.axis_size("frame"), lax.axis_size("seq")
    devices = frames * seqs
    my_seq = lax.axis_index("seq")
    me, partner, ahead, behind = frame_peers()
    head = HEAD_WIDTH
    own_rows = text_ref.shape[1]
    group_rows = frames * own_rows
    steps, block = tokens.shape[0], tokens.shape[3]
    model_width = steps * block
    blocks = own_rows // sub
    q_rows = frames * sub
    rows = group * q_rows
    cut = wo_all.shape[2]
    relay = SeqRelay(kv.at[my_seq], kv, relay_sems[1:], count)
    loads = relay_sems[0]
    kv_acc, q_acc = sums.at[:, : 2 * wk.shape[1]], sums.at[:, : wq.shape[1]]
    spread = FrameSpread(lambda slot, part: wo_all.at[slot], (wo_sems_a, wo_sems_b))
    barrier = pltpu.get_barrier_semaphore()
    relay.greet(barrier)
    for d in range(1, frames):
        greet(barrier, "frame", (me + d) % frames)

    def load(i, which):
        at = pl.ds(pl.multiple_of(i * block, block), block)
        if which:
            return pltpu.make_async_copy(text_ref.at[:, :, at], tokens.at[i], loads.at[1, i])
        return pltpu.make_async_copy(pw_ref.at[:, at], pw.at[i], loads.at[0, i])

    fetch_turns = pltpu.make_async_copy(base_turns_ref, turns, local.at[6])
    fetch_turns.start()
    for i in range(steps):
        load(i, 0).start()
        load(i, 1).start()
    fetch = [
        pltpu.make_async_copy(src, dst, local.at[3 + i])
        for i, (src, dst) in enumerate(((wk_ref, wk), (wv_ref, wv), (wq_ref, wq)))
    ]
    for copy in fetch:
        copy.start()

    i = lax.broadcasted_iota(jnp.int32, (group_rows, 1), 0)
    position = i % own_rows * devices + i // own_rows * seqs + my_seq
    t = lax.broadcasted_iota(jnp.int32, (1, info_ref.shape[1]), 1)
    within_frame = position // own_rows == t

    def of_frame(k):
        return jnp.sum(jnp.where(within_frame, info_ref[k : k + 1], 0), axis=1, keepdims=True)

    within = position - of_frame(0)
    visual = (within >= 0) & (within < of_frame(1) // 4)
    row = of_frame(2) + jnp.maximum(within, 0) // seqs
    c = lax.broadcasted_iota(jnp.int32, (1, hot.shape[1]), 1)
    hot[...] = jnp.where(visual & (row == c), 1.0, 0.0).astype(jnp.bfloat16)
    visual_mask[...] = jnp.where(visual, 1.0, 0.0)
    squares[...] = jnp.zeros(squares.shape, jnp.float32)
    kv_acc[...] = jnp.zeros(kv_acc.shape, jnp.float32)
    joined[...] = jnp.concatenate([table_ref[f] for f in range(frames)], axis=1)
    pl.semaphore_wait(barrier, relay.peers() + (frames - 1))
    wo_cut, wo_tail = wo_ref.at[:, pl.ds(0, cut)], wo_ref.at[:, pl.ds(cut, wo_rest.shape[2])]
    spread.publish(wo_cut)
    rest = remote(wo_tail, wo_rest.at[1], rest_sems.at[0], rest_sems.at[1], "frame", partner)
    rest.start()
    keep_cut = pltpu.make_async_copy(wo_cut, wo_all.at[me], local.at[1])
    keep_cut.start()
    keep_tail = pltpu.make_async_copy(wo_tail, wo_rest.at[0], local.at[2])
    keep_tail.start()

    def combine(i, carry):
        load(i, 0).wait()
        load(i, 1).wait()
        total = dot32(joined[...], pw[i]) + pb_ref[i]
        fetched = dot32(hot[...], total.astype(jnp.bfloat16))
        words = tokens[i].reshape(group_rows, block).astype(jnp.float32)
        value = jnp.where(visual_mask[...] > 0.5, fetched, words)
        squares[...] += jnp.sum(value * value, axis=1, keepdims=True)
        tokens[i] = value.astype(jnp.bfloat16).reshape(frames, own_rows, block)
        return carry

    lax.fori_loop(0, steps, combine, 0)
    seq_cos = jnp.zeros((1, head), jnp.float32)
    seq_sin = jnp.zeros((1, head), jnp.float32)
    for k in range(seqs):
        mask = jnp.where(my_seq == k, 1.0, 0.0)
        seq_cos = seq_cos + mask * seq_turns_ref[0, k : k + 1]
        seq_sin = seq_sin + mask * seq_turns_ref[1, k : k + 1]
    lane = lax.broadcasted_iota(jnp.int32, (1, head), 1)
    flip = jnp.where(lane < head // 2, -1.0, 1.0)
    fetch_turns.wait()
    base_cos, base_sin = turns[0], turns[1]
    turns[0] = base_cos * seq_cos - base_sin * seq_sin
    turns[1] = (base_sin * seq_cos + base_cos * seq_sin) * flip
    for copy in fetch[:2]:
        copy.wait()
    squares[...] = lax.rsqrt(squares[...] * (1.0 / model_width) + norm_epsilon)
    kw = wk.shape[1]

    def project_kv(i, carry):
        at = pl.ds(pl.multiple_of(i * block, block), block)
        value = tokens[i].reshape(group_rows, block).astype(jnp.float32)
        value = (value * squares[...] * gain_ref[i]).astype(jnp.bfloat16)
        tokens[i] = value.reshape(frames, own_rows, block)
        kv_acc[:, :kw] += dot32(value, wk[at])
        kv_acc[:, kw:] += dot32(value, wv[at])
        return carry

    lax.fori_loop(0, steps, project_kv, 0)
    for h in range(kv_heads):
        x = kv_acc[:, h * head : (h + 1) * head]
        x = x * turns[0] + pltpu.roll(x, head // 2, 1) * turns[1]
        x = x.astype(jnp.bfloat16).reshape(frames, own_rows, head)
        kv[my_seq, :, :, h * head : (h + 1) * head] = x
    x = kv_acc[:, kw:].astype(jnp.bfloat16).reshape(frames, own_rows, kw)
    kv[my_seq, :, :, kw:] = x
    relay.first()
    fetch[2].wait()
    q_acc[...] = jnp.zeros(q_acc.shape, jnp.float32)

    def project(i, carry):
        at = pl.ds(pl.multiple_of(i * block, block), block)
        q_acc[...] += dot32(tokens[i].reshape(group_rows, block), wq[at])
        return carry

    lax.fori_loop(0, tokens.shape[0], project, 0)
    for h in range(kv_heads * group):
        x = q_acc[:, h * head : (h + 1) * head]
        x = x * turns[0] + pltpu.roll(x, head // 2, 1) * turns[1]
        x = (x * (LOG2E / math.sqrt(head))).astype(jnp.bfloat16)
        heads_out[:, :, h * head : (h + 1) * head] = x.reshape(frames, own_rows, head)
    for h in range(kv_heads):
        for b in range(blocks):
            parts = [
                heads_out[:, b * sub : (b + 1) * sub, (h * group + g) * head : (h * group + g + 1) * head]
                .reshape(q_rows, head)
                for g in range(group)
            ]
            qs[h, b] = jnp.concatenate(parts, axis=0)
    highest[...] = jnp.full(highest.shape, masked_score, jnp.float32)
    acc[...] = jnp.zeros(acc.shape, jnp.float32)

    def process(source):
        for b in range(blocks):
            n = (b + 1) * sub
            keys_n = frames * n
            qi = lax.broadcasted_iota(jnp.int32, (rows, 1), 0) % q_rows
            q_at = (b * sub + qi % sub) * devices + (qi // sub) * seqs + my_seq
            ki = lax.broadcasted_iota(jnp.int32, (1, keys_n), 1)
            k_at = ki % n * devices + ki // n * seqs + source
            seen = k_at <= q_at
            ones = jnp.ones((keys_n, head), jnp.bfloat16)
            for h in range(kv_heads):
                k = kv[source, :, :n, h * head : (h + 1) * head].reshape(keys_n, head)
                v = kv[source, :, :n, (kv_heads + h) * head : (kv_heads + h + 1) * head]
                v = jnp.concatenate([v.reshape(keys_n, head), ones], axis=1)
                s = lax.dot_general(
                    qs[h, b], k, (((1,), (1,)), ((), ())), preferred_element_type=jnp.float32
                )
                s = jnp.where(seen, s, masked_score)
                m = highest[h, b]
                new = jnp.maximum(m, jnp.max(s, axis=1, keepdims=True))
                e = jnp.exp2(s - new).astype(jnp.bfloat16)
                acc[h, b] = acc[h, b] * jnp.exp2(m - new) + dot32(e, v)
                highest[h, b] = new

    def step(k, carry):
        pl.when((k > 0) & (k < relay.length))(lambda: relay.step(k))

        def one(i, c):
            crossed, side = i // 2, i % 2
            distance = k - crossed
            source = relay.a - distance + 2 * distance * side
            valid = (source >= 0) & (source < relay.length) & (distance >= 0)
            valid = valid & ((distance > 0) | (side == 0))

            @pl.when(valid)
            def _():
                if relay.breadth == 2:

                    @pl.when(crossed == 1)
                    def _():
                        relay.await_cross(source)

                row = relay.b + crossed * (1 - 2 * relay.b)
                process(source * relay.breadth + row)

            return c

        return lax.fori_loop(0, 2 * relay.breadth, one, carry)

    lax.fori_loop(0, relay.length + relay.breadth - 1, step, 0)
    for h in range(kv_heads):
        for b in range(blocks):
            out = (acc[h, b, :, :head] / acc[h, b, :, head:]).astype(jnp.bfloat16)
            for g in range(group):
                piece = out[g * q_rows : (g + 1) * q_rows].reshape(frames, sub, head)
                at = (h * group + g) * head
                heads_out[:, b * sub : (b + 1) * sub, at : at + head] = piece

    targets, sources = exchange_slots(me, frames)
    copies = []
    near = []
    for i, target in enumerate(ahead):
        near.append(
            remote(
                heads_out.at[target + 1 - 2 * (me % 2)],
                near_context.at[i],
                near_sems_a.at[i],
                near_sems_b.at[i],
                "frame",
                partner,
            )
        )
        near[-1].start()
    for d, target in enumerate(targets):
        copies.append(
            remote(
                heads_out.at[target],
                context.at[me],
                ctx_send.at[d],
                ctx_recv.at[d],
                "frame",
                target,
            )
        )
        copies[-1].start()
    keep_own = pltpu.make_async_copy(heads_out.at[me], context.at[me], local.at[0])
    keep_own.start()
    keep_tail.wait()
    rest.wait_recv()
    sent = []
    for i, target in enumerate(ahead):
        near[i].wait_recv()
        total = dot32(heads_out[target], wo_rest[0]) + dot32(near_context[i], wo_rest[1])
        shared[i] = total.astype(jnp.bfloat16)
        copy = remote(
            shared.at[i], arriving.at[i], part_send.at[i], part_recv.at[i], "frame", target
        )
        copy.start()
        sent.append(copy)
    keep_cut.wait()
    spread.forward()
    keep_own.wait()
    for d, source in enumerate(sources):
        ref = context.at[source]
        remote(ref, ref, ctx_send.at[d], ctx_recv.at[d], "frame", partner).wait_recv()
    spread.settle()
    wide = math.gcd(cut, 512)
    for c in range(cut // wide):
        total = dot32(context[0], wo_all[0, :, c * wide : (c + 1) * wide])
        for f in range(1, frames):
            total = total + dot32(context[f], wo_all[f, :, c * wide : (c + 1) * wide])
        mixed_ref[:, c * wide : (c + 1) * wide] = total.astype(mixed_ref.dtype)
    total = dot32(context[me], wo_rest[0]) + dot32(context[partner], wo_rest[1])
    for i in range(len(ahead)):
        ref = arriving.at[i]
        remote(ref, ref, part_send.at[i], part_recv.at[i], "frame", partner).wait_recv()
        total = total + arriving[i].astype(jnp.float32)
    mixed_ref[:, cut:] = total.astype(mixed_ref.dtype)
    rest.wait_send()
    spread.drain()
    for copy in copies + near + sent:
        copy.wait_send()
    relay.drain()


def attend(
    info, table, proj_w, proj_b, text, gain, wq, wk, wv, base_turns, seq_turns, wo
):
    frames, own_rows, model_width = text.shape
    width, kw = wq.shape[1], wk.shape[1]
    kv_heads = kw // HEAD_WIDTH
    group = width // kw
    group_rows = frames * own_rows
    block = math.gcd(model_width, 512)
    steps = model_width // block
    seqs = lax.axis_size("seq")
    depth, out_cols = wo.shape
    cut = ceil_to(out_cols * 5 // 8, 512) if frames <= 4 else out_cols // 4
    rest = out_cols - cut
    sub = math.gcd(own_rows, 32)
    blocks, rows = own_rows // sub, group * frames * sub
    head = HEAD_WIDTH
    others = max(1, frames // 2 - 1)
    chunks = 2
    dma = pltpu.SemaphoreType.DMA
    vmem = pl.BlockSpec(memory_space=pltpu.VMEM)
    anywhere = pl.BlockSpec(memory_space=pl.ANY)
    return pl.pallas_call(
        functools.partial(
            attend_kernel, count=chunks, kv_heads=kv_heads, group=group, sub=sub
        ),
        in_specs=[vmem] * 2
        + [anywhere, vmem, anywhere, vmem]
        + [anywhere] * 3
        + [anywhere, vmem, anywhere],
        out_specs=vmem,
        out_shape=jax.ShapeDtypeStruct((own_rows, out_cols), jnp.bfloat16),
        scratch_shapes=[
            pltpu.VMEM((steps, proj_w.shape[0], block), jnp.bfloat16),
            pltpu.VMEM((steps, frames, own_rows, block), jnp.bfloat16),
            pltpu.VMEM((group_rows, table.shape[1]), jnp.bfloat16),
            pltpu.VMEM((table.shape[1], frames * table.shape[2]), jnp.bfloat16),
            pltpu.VMEM((group_rows, 1), jnp.float32),
            pltpu.VMEM((group_rows, 1), jnp.float32),
            pltpu.VMEM(wk.shape, wk.dtype),
            pltpu.VMEM(wv.shape, wv.dtype),
            pltpu.VMEM(wq.shape, wq.dtype),
            pltpu.VMEM((2, group_rows, HEAD_WIDTH), jnp.float32),
            pltpu.VMEM((group_rows, max(width, 2 * kw)), jnp.float32),
            pltpu.VMEM((seqs, frames, own_rows, 2 * kw), jnp.bfloat16),
            pltpu.VMEM((kv_heads, blocks, rows, head), jnp.bfloat16),
            pltpu.VMEM((kv_heads, blocks, rows, 1), jnp.float32),
            pltpu.VMEM((kv_heads, blocks, rows, 2 * head), jnp.float32),
            pltpu.VMEM((frames, own_rows, width), jnp.bfloat16),
            pltpu.VMEM((frames, own_rows, width), jnp.bfloat16),
            pltpu.VMEM((others, own_rows, rest), jnp.bfloat16),
            pltpu.VMEM((others, own_rows, width), jnp.bfloat16),
            pltpu.VMEM((frames, depth, cut), jnp.bfloat16),
            pltpu.VMEM((2, depth, rest), jnp.bfloat16),
            pltpu.VMEM((others, own_rows, rest), jnp.bfloat16),
            dma((7,)),
            dma((frames - 1, 1)),
            dma((frames - 1, 1)),
            dma((2,)),
            dma((frames - 1,)),
            dma((frames - 1,)),
            dma((others,)),
            dma((others,)),
            dma((others,)),
            dma((others,)),
        ]
        + [dma((2, steps))]
        + relay_scratch(chunks),
        compiler_params=pltpu.CompilerParams(
            collective_id=3, has_side_effects=True, vmem_limit_bytes=63 * 1024 * 1024
        ),
        cost_estimate=pl.CostEstimate(
            flops=40_000_000_000, bytes_accessed=0, transcendentals=0
        ),
        name="attend",
    )(
        info,
        table,
        proj_w,
        proj_b.reshape(steps, 1, block),
        text,
        gain.reshape(steps, 1, block),
        wq,
        wk,
        wv,
        base_turns,
        seq_turns,
        wo,
    )


class SeqRelay:
    def __init__(self, x_ref, out_ref, sems, count, low=None, wide=None):
        seqs = lax.axis_size("seq")
        self.x, self.out, self.count = x_ref, out_ref, count
        self.send_r, self.recv_r, self.send_l, self.recv_l, self.send_y, self.recv_y = sems[:6]
        self.send_e, self.recv_e = sems[6:]
        self.depth = x_ref.shape[0] // count
        self.tail = () if low is None else (pl.ds(low, wide),)
        self.breadth = 2 if seqs % 2 == 0 else 1
        self.length = seqs // self.breadth
        self.me = lax.axis_index("seq")
        self.a, self.b = self.me // self.breadth, self.me % self.breadth
        self.across = self.a * self.breadth + (self.breadth - 1 - self.b)
        self.has_right, self.has_left = self.a + 1 < self.length, self.a > 0

    def greet(self, barrier):
        breadth = self.breadth
        pl.when(self.has_right)(lambda: greet(barrier, "seq", self.me + breadth))
        pl.when(self.has_left)(lambda: greet(barrier, "seq", self.me - breadth))
        if breadth == 2:
            greet(barrier, "seq", self.across)

    def peers(self):
        sides = self.has_right.astype(jnp.int32) + self.has_left.astype(jnp.int32)
        return sides + (self.breadth - 1)

    def cut(self, i):
        rows = pl.ds(i * self.depth, self.depth)
        return (rows, slice(None)) + self.tail if not self.tail else (rows,) + self.tail

    def slot(self, source, b, i):
        return self.out.at[(source * self.breadth + b,) + self.cut(i)]

    def own(self, i):
        return self.x.at[self.cut(i)]

    def shift(self, i, k, right, own=False):
        slot = self.slot(self.a - k if right else self.a + k, self.b, i)
        send, recv = (self.send_r, self.recv_r) if right else (self.send_l, self.recv_l)
        src = self.own(i) if own else slot
        target = self.me + self.breadth if right else self.me - self.breadth
        return remote(src, slot, send.at[i, k], recv.at[i, k], "seq", target)

    def cross(self, i, source, own):
        slot = self.slot(source, self.b, i)
        src = self.own(i) if own else slot
        return remote(src, slot, self.send_y.at[i, source], self.recv_y.at[i, source], "seq", self.across)

    def incoming(self, i, k, right):
        slot = self.slot(self.a - k if right else self.a + k, self.b, i)
        recv = self.recv_r if right else self.recv_l
        return remote(slot, slot, self.send_r.at[i, 0], recv.at[i, k - 1], "seq", self.across)

    def incoming_cross(self, i, source):
        slot = self.slot(source, self.breadth - 1 - self.b, i)
        return remote(slot, slot, self.send_r.at[i, 0], self.recv_y.at[i, source], "seq", self.across)

    def held(self, k, right):
        held = (self.a >= k) if right else (self.a + k < self.length)
        return held, held & (self.has_right if right else self.has_left)

    def first(self):
        for i in range(self.count):
            for right in (True, False):
                pl.when(self.held(0, right)[1])(lambda: self.shift(i, 0, right, True).start())
            if self.breadth == 2:
                self.cross(i, self.a, True).start()

    def balanced(self):
        return self.breadth == 2 and self.length > 1

    def extra(self, right):
        source = 0 if right else self.length - 1
        slot = self.slot(source, self.breadth - 1 - self.b, self.count - 1)
        side = 0 if right else 1
        target = self.me + self.breadth if right else self.me - self.breadth
        return remote(slot, slot, self.send_e.at[side], self.recv_e.at[side], "seq", target)

    def at_end(self, right):
        return self.a == (0 if right else self.length - 1)

    def onward(self, i, source, start):
        if self.balanced() and i == self.count - 1:
            end = (source == 0) | (source == self.length - 1)
            pl.when(jnp.logical_not(end))(start)
        else:
            start()

    def step(self, k):
        for i in range(self.count):
            for right in (True, False):
                held, onward = self.held(k, right)
                source = self.a - k if right else self.a + k
                pl.when(held)(lambda: self.incoming(i, k, right).wait_recv())
                pl.when(onward)(lambda: self.shift(i, k, right).start())
                if self.breadth == 2:

                    @pl.when(held)
                    def _():
                        self.onward(i, source, lambda: self.cross(i, source, False).start())

        if self.balanced():
            for right in (True, False):
                distance = self.a if right else self.length - 1 - self.a

                @pl.when(distance == k - 1)
                def _():
                    @pl.when(distance == 0)
                    def _():
                        self.incoming_cross(self.count - 1, self.a).wait_recv()

                    pl.when(distance > 0)(lambda: self.extra(right).wait_recv())
                    self.extra(right).start()

    def await_cross(self, source):
        for i in range(self.count):
            if self.balanced() and i == self.count - 1:
                end = (source == 0) | (source == self.length - 1)
                pl.when(jnp.logical_not(end))(
                    lambda: self.incoming_cross(i, source).wait_recv()
                )
                for right in (True, False):
                    last = self.at_end(not right) & (source == (0 if right else self.length - 1))
                    pl.when(last)(lambda: self.extra(right).wait_recv())
            else:
                self.incoming_cross(i, source).wait_recv()

    def settle(self):
        if self.breadth == 2:
            for k in range(self.length):
                self.await_cross(k)

    def drain(self):
        for i in range(self.count):
            for k in range(self.length):
                for right in (True, False):
                    onward = self.held(k, right)[1]
                    pl.when(onward)(lambda: self.shift(i, k, right).wait_send())
                if self.breadth == 2:
                    if self.balanced() and i == self.count - 1:
                        end = k == 0 or k == self.length - 1
                        pl.when((self.a == k) | (not end))(
                            lambda: self.cross(i, k, False).wait_send()
                        )
                    else:
                        self.cross(i, k, False).wait_send()
        if self.balanced():
            for right in (True, False):
                far = self.at_end(not right)
                pl.when(jnp.logical_not(far))(lambda: self.extra(right).wait_send())


def per_device(
    vit_states,
    frame_slot,
    patch_count,
    vis_start,
    text_embed,
    vit_ln_gain,
    vit_ln_bias,
    vit_qkv_w,
    vit_qkv_b,
    vit_out_w,
    vit_out_b,
    proj_w,
    proj_b,
    attn_gain,
    wq,
    wk,
    wv,
    wo,
):
    frames_n = lax.axis_size("frame")
    seqs_n = lax.axis_size("seq")
    chips = frames_n // 2
    devices_n = frames_n * seqs_n
    me = lax.axis_index("frame")
    my_seq = lax.axis_index("seq")
    slots_held, frame_max, width_vit = vit_states.shape
    vis_max = frame_max // 4
    own_rows, model_width = text_embed.shape[0], text_embed.shape[2]
    head_size = width_vit // VHEADS
    my_heads = VHEADS // frames_n
    cols = width_vit // frames_n

    w_parts = [
        lax.dynamic_slice_in_dim(vit_qkv_w, i * width_vit + me * cols, cols, 1) for i in range(3)
    ]
    out_own = lax.dynamic_slice_in_dim(vit_out_w, me * cols, cols, 1)
    own_weights = jnp.concatenate(w_parts + [out_own], 1)
    params = jnp.concatenate([vit_ln_gain, vit_ln_bias, vit_qkv_b, vit_out_b]).reshape(1, -1)

    holder = frame_slot // slots_held
    holder_frame = holder // seqs_n
    pair_low = (holder_frame - holder_frame % 2) * seqs_n + holder % seqs_n
    pair_order = holder_frame % 2 * slots_held + frame_slot % slots_held
    same_pair = pair_low[:, None] == pair_low[None, :]
    earlier = pair_order[None, :] < pair_order[:, None]
    pair_rank = jnp.sum((same_pair & earlier).astype(jnp.int32), axis=1)
    source_frame = pair_low // seqs_n + pair_rank
    source_seq = pair_low % seqs_n
    entry = jnp.arange(2 + 2 * frames_n)[:, None]
    wanted = jnp.where(entry < 2, me - me % 2 + (me % 2 + entry) % 2, (entry - 2) % frames_n)
    chosen = (source_frame[None, :] == wanted) & (source_seq[None, :] == my_seq)
    kind = jnp.where(
        entry < 2,
        pair_order[None, :],
        jnp.where(entry < 2 + frames_n, patch_count[None, :], vis_start[None, :]),
    )
    facts = jnp.sum(jnp.where(chosen, kind, 0), axis=1)

    table, text_rows = vision(
        facts,
        own_weights,
        vit_states,
        text_embed.reshape(own_rows, model_width),
        params,
        cols,
        my_heads,
    )
    laps = vis_max // seqs_n
    group_rows = frames_n * own_rows
    row_ids = np.arange(group_rows)
    base = row_ids % own_rows * devices_n + row_ids // own_rows * seqs_n
    inverse = rope_theta ** (-np.arange(0, HEAD_WIDTH, 2) / HEAD_WIDTH)

    def turns(positions):
        angles = np.tile(positions[:, None] * inverse[None, :], (1, 2))
        return jnp.asarray(np.stack([np.cos(angles), np.sin(angles)]), jnp.float32)

    base_turns, seq_turns = turns(base), turns(np.arange(seqs_n))
    info = jnp.stack([vis_start, patch_count, (source_seq * frames_n + source_frame) * laps])
    mixed = attend(
        info,
        table,
        proj_w,
        proj_b,
        text_rows,
        attn_gain,
        wq,
        wk,
        wv,
        base_turns,
        seq_turns,
        wo,
    )
    return mixed.reshape(own_rows, 1, wo.shape[1])


def solution(mesh):
    return jax.shard_map(
        per_device,
        mesh=mesh,
        in_specs=(
            P(("frame", "seq"), None, None),
            P(),
            P(),
            P(),
            P(None, ("frame", "seq"), None),
            P(),
            P(),
            P("seq", None),
            P(),
            P("seq", None),
            P(),
            P(),
            P(),
            P(),
            P(None, "frame"),
            P(None, "frame"),
            P(None, "frame"),
            P("frame", None),
        ),
        out_specs=P(None, ("frame", "seq"), None),
        check_vma=False,
    )
```

```python
import functools
import math

import jax
import jax.numpy as jnp
import numpy as np
from jax import lax
from jax.experimental import pallas as pl
from jax.experimental.pallas import tpu as pltpu
from jax.sharding import PartitionSpec as P

VHEADS = 16
HEAD_WIDTH = 128

rope_theta = 500000.0
vit_epsilon = 1e-06
norm_epsilon = 1e-05
masked_score = -1e30
LOG2E = math.log2(math.e)


def dot32(a, b):
    return jnp.dot(a, b, preferred_element_type=jnp.float32)


def ceil_to(value, step):
    return -(-value // step) * step


def encode(normed, w, qb, count, heads, head_size):
    rows = normed.shape[0]
    cols = heads * head_size
    proj = (dot32(normed, w) + qb).astype(jnp.bfloat16)
    q, k, v = (proj[:, i * cols : (i + 1) * cols] for i in range(3))
    live = lax.broadcasted_iota(jnp.int32, (1, rows), 1) < count
    blocks = [None] * pl.cdiv(cols, 128)
    scale = LOG2E / math.sqrt(head_size)
    for h in range(heads):
        low, high = h * head_size, (h + 1) * head_size
        start, stop = low // 128 * 128, min(ceil_to(high, 128), cols)
        lane = lax.broadcasted_iota(jnp.int32, (1, stop - start), 1) + start
        mine = jnp.where((lane >= low) & (lane < high), 1.0, 0.0).astype(jnp.bfloat16)
        s = lax.dot_general(
            q[:, start:stop] * mine,
            k[:, start:stop],
            (((1,), (1,)), ((), ())),
            preferred_element_type=jnp.float32,
        )
        s = jnp.where(live, s * scale, masked_score)
        e = jnp.exp2(s - jnp.max(s, axis=1, keepdims=True))
        p = (e * (1.0 / jnp.sum(e, axis=1, keepdims=True))).astype(jnp.bfloat16)
        o = dot32(p, v[:, start:stop] * mine)
        for b in range(start // 128, pl.cdiv(stop, 128)):
            part = o[:, b * 128 - start : min((b + 1) * 128, stop) - start]
            blocks[b] = part if blocks[b] is None else blocks[b] + part
    return jnp.concatenate(blocks, axis=1).astype(jnp.bfloat16)


MESH = pl.DeviceIdType.MESH


def remote(src, dst, send, recv, axis, index):
    return pltpu.make_async_remote_copy(
        src_ref=src,
        dst_ref=dst,
        send_sem=send,
        recv_sem=recv,
        device_id={axis: index},
        device_id_type=MESH,
    )


def frame_peers():
    frames = lax.axis_size("frame")
    me = lax.axis_index("frame")
    chips = frames // 2
    chip, core = me // 2, me % 2
    partner = chip * 2 + (1 - core)
    ahead = [((chip + dx) % chips) * 2 + core for dx in range(1, chips)]
    behind = [((chip + chips - dx) % chips) * 2 + core for dx in range(1, chips)]
    return me, partner, ahead, behind


def greet(barrier, axis, index):
    pl.semaphore_signal(barrier, inc=1, device_id={axis: index}, device_id_type=MESH)


class FrameSpread:
    def __init__(self, view, sems, direct=True):
        self.view = view
        self.send, self.recv = sems
        self.me, self.partner, self.ahead, self.behind = frame_peers()
        self.n = len(self.ahead)
        self.direct = direct

    def copy(self, src, slot, part, k, target):
        return remote(
            src, self.view(slot, part), self.send.at[k, part], self.recv.at[k, part], "frame", target
        )

    def arrived(self, slot, part, k):
        self.copy(self.view(slot, part), slot, part, k, self.partner).wait_recv()

    def publish(self, src, part=0):
        for i, target in enumerate(self.ahead):
            self.copy(src, self.me, part, 1 + i, target).start()
        if self.direct:
            self.copy(src, self.me, part, 0, self.partner).start()

    def forward(self, part=0):
        for i, source in enumerate(self.behind):
            self.arrived(source, part, 1 + i)
            self.copy(self.view(source, part), source, part, 1 + self.n + i, self.partner).start()

    def settle(self, part=0):
        if self.direct:
            self.arrived(self.partner, part, 0)
        for i, source in enumerate(self.behind):
            self.arrived(source + 1 - 2 * (self.me % 2), part, 1 + self.n + i)

    def drain(self, parts=1):
        for part in range(parts):
            for k in range(0 if self.direct else 1, 2 * self.n + 1):
                self.copy(self.view(self.me, part), self.me, part, k, self.partner).wait_send()


def relay_scratch(chunks):
    seqs = lax.axis_size("seq")
    length = seqs // 2 if seqs % 2 == 0 else seqs
    return [pltpu.SemaphoreType.DMA((chunks, length))] * 6 + [pltpu.SemaphoreType.DMA((2,))] * 2


def vision_kernel(
    facts_ref,
    w_ref,
    states_ref,
    text_ref,
    params_ref,
    table_out,
    text_out,
    w_all,
    states_all,
    pair,
    normed,
    ctx_all,
    pooled,
    outgoing,
    local,
    pair_sems,
    state_a,
    state_b,
    text_a,
    text_b,
    ctx_a,
    ctx_b,
    table_a,
    table_b,
    seq_send,
    seq_recv,
    *relay_sems,
    heads,
    head_size,
    chunks,
):
    frames, seqs = lax.axis_size("frame"), lax.axis_size("seq")
    seq = lax.axis_index("seq")
    me, partner, ahead, behind = frame_peers()
    core = me % 2
    slots, rows, width = states_ref.shape
    cols = heads * head_size
    vis_max = rows // 4
    depth = w_ref.shape[0]
    first_cols = ceil_to(3 * cols, 128)
    relay = SeqRelay(w_ref, w_all, relay_sems[:8], chunks, 0, first_cols)
    relay_rest = SeqRelay(w_ref, w_all, relay_sems[8:], 2, first_cols, 4 * cols - first_cols)
    states = FrameSpread(lambda slot, part: states_all.at[slot], (state_a, state_b), False)
    pieces = text_a.shape[1]
    piece = text_ref.shape[0] // pieces

    def piece_of(part):
        return pl.ds(pl.multiple_of(part * piece, piece), piece)

    text = FrameSpread(lambda slot, part: text_out.at[slot, piece_of(part)], (text_a, text_b))

    def publish_text(part):
        text.publish(text_ref.at[piece_of(part)], part)

    context = FrameSpread(lambda slot, part: ctx_all.at[slot, part], (ctx_a, ctx_b))
    share = vis_max // seqs * frames
    laps = share // frames

    def part_of(index):
        return pl.ds(pl.multiple_of(index * share, share), share)

    table = FrameSpread(lambda slot, part: table_out.at[slot, part_of(part)], (table_a, table_b))
    others = [(seq + d) % seqs for d in range(1, seqs)]
    barrier = pltpu.get_barrier_semaphore()
    for other in others:
        greet(barrier, "seq", other)
    for peer in [partner] + ahead:
        greet(barrier, "frame", peer)
    pl.semaphore_wait(barrier, seqs - 1 + frames // 2)
    swap = remote(states_ref, pair, pair_sems.at[0], pair_sems.at[1], "frame", partner)
    swap.start()
    relay.first()
    keep_w = pltpu.make_async_copy(w_ref, w_all.at[seq], local.at[0])
    keep_w.start()
    keep_text = pltpu.make_async_copy(text_ref, text_out.at[me], local.at[1])
    keep_text.start()
    swap.wait()
    step = math.gcd(rows, 32)
    keep = [
        [
            jnp.where(facts_ref[j] == side * slots + k, 1.0, 0.0)
            for side in (core, 1 - core)
            for k in range(slots)
        ]
        for j in range(2)
    ]

    def choose(i, carry):
        at = pl.ds(pl.multiple_of(i * step, step), step)
        values = [states_ref[k, at].astype(jnp.float32) for k in range(slots)]
        values += [pair[k, at].astype(jnp.float32) for k in range(slots)]
        for j, slot in enumerate((me, partner)):
            total = keep[j][0] * values[0]
            for weight, value in zip(keep[j][1:], values[1:]):
                total = total + weight * value
            states_all[slot, at] = total.astype(states_all.dtype)
        return carry

    lax.fori_loop(0, rows // step, choose, 0)
    states.publish(states_all.at[me])
    early = max(pieces - 1, 1)
    for part in range(early):
        publish_text(part)
    gain, shift = params_ref[:, :width], params_ref[:, width : 2 * width]

    def own_part(at):
        total = jnp.zeros((1, cols), jnp.float32)
        for f in range(frames):
            low = at + f * cols
            total = total + jnp.where(me == f, 1.0, 0.0) * params_ref[:, low : low + cols]
        return total

    qkv_bias = jnp.concatenate([own_part((2 + i) * width) for i in range(3)], axis=1)
    out_bias = own_part(5 * width)

    def normalize(slot):
        def one(i, carry):
            at = pl.ds(pl.multiple_of(i * step, step), step)
            wide = states_all[slot, at].astype(jnp.float32)
            average = jnp.mean(wide, axis=1, keepdims=True)
            centred = wide - average
            spread = jnp.mean(centred * centred, axis=1, keepdims=True)
            value = centred * lax.rsqrt(spread + vit_epsilon) * gain + shift
            normed[slot, at] = value.astype(jnp.bfloat16)
            return carry

        lax.fori_loop(0, rows // step, one, 0)

    normalize(me)
    relay.step(1)
    normalize(partner)
    for k in range(2, relay.length):
        relay.step(k)
        if k == 2:
            states.forward()
            for source in behind:
                normalize(source)
    if relay.length <= 2:
        states.forward()
        for source in behind:
            normalize(source)
    relay_rest.first()
    states.settle()
    for source in behind:
        normalize(source + 1 - 2 * core)
    keep_w.wait()
    relay.settle()

    pr = lax.broadcasted_iota(jnp.int32, (vis_max, rows), 0)
    pc = lax.broadcasted_iota(jnp.int32, (vis_max, rows), 1)
    pool = jnp.where(pc // 4 == pr, 0.25, 0.0).astype(jnp.bfloat16)

    batch = 2 if frames % 2 == 0 else 1

    def some_frames(step_at, carry):
        f0 = step_at * batch
        w = w_all[:, :, : 3 * cols].reshape(width, 3 * cols)
        contexts, totals = [], []
        for i in range(batch):
            f = f0 + i
            result = encode(normed[f], w, qkv_bias, facts_ref[2 + f], heads, head_size)
            contexts.append(dot32(pool, result).astype(jnp.bfloat16))
            averaged = dot32(pool, states_all[f])
            total = jnp.zeros((vis_max, cols), jnp.float32)
            for g in range(frames):
                mask = jnp.where(me == g, 1.0, 0.0)
                total = total + mask * averaged[:, g * cols : (g + 1) * cols]
            totals.append(total)
        for i in range(batch):
            ctx_all[me, f0 + i] = contexts[i]
            pooled[f0 + i] = totals[i]
        for i in range(batch):
            context.publish(ctx_all.at[me, f0 + i], f0 + i)
        if early < pieces:
            pl.when(step_at == frames // batch - 1)(lambda: publish_text(pieces - 1))
        for i in range(batch):
            k = f0 + i + 1
            pl.when(k < relay.length)(lambda: relay_rest.step(k))
        for i in range(batch):
            k = f0 + i - batch
            pl.when(k >= 0)(lambda: context.forward(k))
        return carry

    lax.fori_loop(0, frames // batch, some_frames, 0)
    for k in range(frames + 1, relay.length):
        relay_rest.step(k)
    r = lax.broadcasted_iota(jnp.int32, (seqs * share, 1), 0)
    dest, frame, lap = r // share, r // laps % frames, r % laps
    begin = jnp.zeros((seqs * share, 1), jnp.int32)
    for f in range(frames):
        begin = begin + jnp.where(frame == f, facts_ref[2 + frames + f], 0)
    token = (dest + seqs - begin % seqs) % seqs + lap * seqs + frame * vis_max
    c = lax.broadcasted_iota(jnp.int32, (1, frames * vis_max), 1)
    pick = jnp.where(token == c, 1.0, 0.0).astype(jnp.bfloat16)
    for f in range(frames - batch, frames):
        context.forward(f)
    relay_rest.settle()
    total = pooled[...].reshape(frames * vis_max, cols) + out_bias
    for f in range(frames):
        context.settle(f)
    per = cols // depth if cols % depth == 0 else 0
    for g in range(frames):
        ctx = ctx_all[g].reshape(frames * vis_max, cols)
        if per:
            w = w_all[g * per : (g + 1) * per, :, 3 * cols :].reshape(cols, cols)
        else:
            w = w_all[:, :, 3 * cols :].reshape(width, cols)[g * cols : (g + 1) * cols]
        total = total + dot32(ctx, w)
    outgoing[...] = dot32(pick, total.astype(jnp.bfloat16)).astype(jnp.bfloat16)

    mine = table_out.at[me]
    sends = []
    for d, other in enumerate(others):
        copy = remote(
            outgoing.at[part_of(other)],
            mine.at[part_of(seq)],
            seq_send.at[d],
            seq_recv.at[d],
            "seq",
            other,
        )
        copy.start()
        sends.append(copy)
    own = pltpu.make_async_copy(outgoing.at[part_of(seq)], mine.at[part_of(seq)], local.at[2])
    own.start()
    table.publish(outgoing.at[part_of(seq)], seq)
    for part in range(pieces):
        text.forward(part)
    for d in range(seqs - 1):
        source = (seq + seqs - 1 - d) % seqs
        ref = mine.at[part_of(source)]
        remote(ref, ref, seq_send.at[d], seq_recv.at[d], "seq", source).wait_recv()
        table.publish(ref, source)
    own.wait()
    keep_text.wait()
    for d in range(seqs):
        table.forward((seq + seqs - d) % seqs)
    for part in range(seqs):
        table.settle(part)
    for part in range(pieces):
        text.settle(part)
    for copy in sends:
        copy.wait_send()
    states.drain()
    text.drain(pieces)
    context.drain(frames)
    table.drain(seqs)
    relay.drain()
    relay_rest.drain()


def vision(facts, weights, states, text, params, cols, heads):
    seqs, frames = lax.axis_size("seq"), lax.axis_size("frame")
    slots, rows, width = states.shape
    vis_max = rows // 4
    vmem = pl.BlockSpec(memory_space=pltpu.VMEM)
    smem = pl.BlockSpec(memory_space=pltpu.SMEM)
    dma = pltpu.SemaphoreType.DMA
    links = max(1, frames - 1)
    chunks = 2
    return pl.pallas_call(
        functools.partial(
            vision_kernel, heads=heads, head_size=cols // heads, chunks=chunks
        ),
        in_specs=[smem] + [vmem] * 4,
        out_specs=[vmem, pl.BlockSpec(memory_space=pl.ANY)],
        out_shape=[
            jax.ShapeDtypeStruct((frames, frames * vis_max, cols), jnp.bfloat16),
            jax.ShapeDtypeStruct((frames,) + text.shape, text.dtype),
        ],
        scratch_shapes=[
            pltpu.VMEM((seqs,) + weights.shape, weights.dtype),
            pltpu.VMEM((frames, rows, width), states.dtype),
            pltpu.VMEM(states.shape, states.dtype),
            pltpu.VMEM((frames, rows, width), jnp.bfloat16),
            pltpu.VMEM((frames, frames, vis_max, cols), jnp.bfloat16),
            pltpu.VMEM((frames, vis_max, cols), jnp.float32),
            pltpu.VMEM((frames * vis_max, cols), jnp.bfloat16),
            dma((3,)),
            dma((2,)),
        ]
        + [dma((links, 1))] * 2
        + [dma((links, math.gcd(text.shape[0], 4)))] * 2
        + [dma((links, frames))] * 2
        + [dma((links, seqs))] * 2
        + [dma((seqs - 1,))] * 2
        + relay_scratch(chunks)
        + relay_scratch(2),
        compiler_params=pltpu.CompilerParams(
            collective_id=1, has_side_effects=True, vmem_limit_bytes=48 * 1024 * 1024
        ),
        cost_estimate=pl.CostEstimate(
            flops=40_000_000_000, bytes_accessed=0, transcendentals=0
        ),
        name="vision",
    )(facts, weights, states, text, params)


def exchange_slots(index, frames):
    return [(index + d) % frames for d in range(1, frames)], [
        (index + frames - d) % frames for d in range(1, frames)
    ]


def attend_kernel(
    info_ref,
    table_ref,
    pw_ref,
    pb_ref,
    text_ref,
    gain_ref,
    wq_ref,
    wk_ref,
    wv_ref,
    base_turns_ref,
    seq_turns_ref,
    wo_ref,
    mixed_ref,
    pw,
    tokens,
    hot,
    joined,
    visual_mask,
    squares,
    wk,
    wv,
    wq,
    turns,
    sums,
    kv,
    qs,
    highest,
    acc,
    heads_out,
    context,
    shared,
    near_context,
    wo_all,
    wo_rest,
    arriving,
    local,
    wo_sems_a,
    wo_sems_b,
    rest_sems,
    ctx_send,
    ctx_recv,
    near_sems_a,
    near_sems_b,
    part_send,
    part_recv,
    *relay_sems,
    count,
    kv_heads,
    group,
    sub,
):
    frames, seqs = lax.axis_size("frame"), lax.axis_size("seq")
    devices = frames * seqs
    my_seq = lax.axis_index("seq")
    me, partner, ahead, behind = frame_peers()
    head = HEAD_WIDTH
    own_rows = text_ref.shape[1]
    group_rows = frames * own_rows
    steps, block = tokens.shape[0], tokens.shape[3]
    model_width = steps * block
    blocks = own_rows // sub
    q_rows = frames * sub
    rows = group * q_rows
    cut = wo_all.shape[2]
    relay = SeqRelay(kv.at[my_seq], kv, relay_sems[1:], count)
    loads = relay_sems[0]
    kv_acc, q_acc = sums.at[:, : 2 * wk.shape[1]], sums.at[:, : wq.shape[1]]
    spread = FrameSpread(lambda slot, part: wo_all.at[slot], (wo_sems_a, wo_sems_b))
    barrier = pltpu.get_barrier_semaphore()
    relay.greet(barrier)
    for d in range(1, frames):
        greet(barrier, "frame", (me + d) % frames)

    def load(i, which):
        at = pl.ds(pl.multiple_of(i * block, block), block)
        if which:
            return pltpu.make_async_copy(text_ref.at[:, :, at], tokens.at[i], loads.at[1, i])
        return pltpu.make_async_copy(pw_ref.at[:, at], pw.at[i], loads.at[0, i])

    fetch_turns = pltpu.make_async_copy(base_turns_ref, turns, local.at[6])
    fetch_turns.start()
    for i in range(steps):
        load(i, 0).start()
        load(i, 1).start()
    fetch = [
        pltpu.make_async_copy(src, dst, local.at[3 + i])
        for i, (src, dst) in enumerate(((wk_ref, wk), (wv_ref, wv), (wq_ref, wq)))
    ]
    for copy in fetch:
        copy.start()

    i = lax.broadcasted_iota(jnp.int32, (group_rows, 1), 0)
    position = i % own_rows * devices + i // own_rows * seqs + my_seq
    t = lax.broadcasted_iota(jnp.int32, (1, info_ref.shape[1]), 1)
    within_frame = position // own_rows == t

    def of_frame(k):
        return jnp.sum(jnp.where(within_frame, info_ref[k : k + 1], 0), axis=1, keepdims=True)

    within = position - of_frame(0)
    visual = (within >= 0) & (within < of_frame(1) // 4)
    row = of_frame(2) + jnp.maximum(within, 0) // seqs
    c = lax.broadcasted_iota(jnp.int32, (1, hot.shape[1]), 1)
    hot[...] = jnp.where(visual & (row == c), 1.0, 0.0).astype(jnp.bfloat16)
    visual_mask[...] = jnp.where(visual, 1.0, 0.0)
    squares[...] = jnp.zeros(squares.shape, jnp.float32)
    kv_acc[...] = jnp.zeros(kv_acc.shape, jnp.float32)
    joined[...] = jnp.concatenate([table_ref[f] for f in range(frames)], axis=1)
    pl.semaphore_wait(barrier, relay.peers() + (frames - 1))
    wo_cut, wo_tail = wo_ref.at[:, pl.ds(0, cut)], wo_ref.at[:, pl.ds(cut, wo_rest.shape[2])]
    spread.publish(wo_cut)
    rest = remote(wo_tail, wo_rest.at[1], rest_sems.at[0], rest_sems.at[1], "frame", partner)
    rest.start()
    keep_cut = pltpu.make_async_copy(wo_cut, wo_all.at[me], local.at[1])
    keep_cut.start()
    keep_tail = pltpu.make_async_copy(wo_tail, wo_rest.at[0], local.at[2])
    keep_tail.start()

    def combine(i, carry):
        load(i, 0).wait()
        load(i, 1).wait()
        total = dot32(joined[...], pw[i]) + pb_ref[i]
        fetched = dot32(hot[...], total.astype(jnp.bfloat16))
        words = tokens[i].reshape(group_rows, block).astype(jnp.float32)
        value = jnp.where(visual_mask[...] > 0.5, fetched, words)
        squares[...] += jnp.sum(value * value, axis=1, keepdims=True)
        tokens[i] = value.astype(jnp.bfloat16).reshape(frames, own_rows, block)
        return carry

    lax.fori_loop(0, steps, combine, 0)
    seq_cos = jnp.zeros((1, head), jnp.float32)
    seq_sin = jnp.zeros((1, head), jnp.float32)
    for k in range(seqs):
        mask = jnp.where(my_seq == k, 1.0, 0.0)
        seq_cos = seq_cos + mask * seq_turns_ref[0, k : k + 1]
        seq_sin = seq_sin + mask * seq_turns_ref[1, k : k + 1]
    lane = lax.broadcasted_iota(jnp.int32, (1, head), 1)
    flip = jnp.where(lane < head // 2, -1.0, 1.0)
    fetch_turns.wait()
    base_cos, base_sin = turns[0], turns[1]
    turns[0] = base_cos * seq_cos - base_sin * seq_sin
    turns[1] = (base_sin * seq_cos + base_cos * seq_sin) * flip
    for copy in fetch[:2]:
        copy.wait()
    squares[...] = lax.rsqrt(squares[...] * (1.0 / model_width) + norm_epsilon)
    kw = wk.shape[1]

    share = frames // count
    for chunk in range(count):
        part = slice(chunk * share, (chunk + 1) * share)
        part_rows = slice(chunk * share * own_rows, (chunk + 1) * share * own_rows)

        def project_kv(i, carry):
            at = pl.ds(pl.multiple_of(i * block, block), block)
            value = tokens[i, part].reshape(share * own_rows, block).astype(jnp.float32)
            value = (value * squares[part_rows] * gain_ref[i]).astype(jnp.bfloat16)
            tokens[i, part] = value.reshape(share, own_rows, block)
            kv_acc[part_rows, :kw] += dot32(value, wk[at])
            kv_acc[part_rows, kw:] += dot32(value, wv[at])
            return carry

        lax.fori_loop(0, steps, project_kv, 0)
        for h in range(kv_heads):
            x = kv_acc[part_rows, h * head : (h + 1) * head]
            x = x * turns[0, part_rows] + pltpu.roll(x, head // 2, 1) * turns[1, part_rows]
            x = x.astype(jnp.bfloat16).reshape(share, own_rows, head)
            kv[my_seq, part, :, h * head : (h + 1) * head] = x
        x = kv_acc[part_rows, kw:].astype(jnp.bfloat16).reshape(share, own_rows, kw)
        kv[my_seq, part, :, kw:] = x
        relay.first_chunk(chunk)
    fetch[2].wait()
    q_acc[...] = jnp.zeros(q_acc.shape, jnp.float32)

    def project(i, carry):
        at = pl.ds(pl.multiple_of(i * block, block), block)
        q_acc[...] += dot32(tokens[i].reshape(group_rows, block), wq[at])
        return carry

    lax.fori_loop(0, tokens.shape[0], project, 0)
    for h in range(kv_heads * group):
        x = q_acc[:, h * head : (h + 1) * head]
        x = x * turns[0] + pltpu.roll(x, head // 2, 1) * turns[1]
        x = (x * (LOG2E / math.sqrt(head))).astype(jnp.bfloat16)
        heads_out[:, :, h * head : (h + 1) * head] = x.reshape(frames, own_rows, head)
    for h in range(kv_heads):
        for b in range(blocks):
            parts = [
                heads_out[:, b * sub : (b + 1) * sub, (h * group + g) * head : (h * group + g + 1) * head]
                .reshape(q_rows, head)
                for g in range(group)
            ]
            qs[h, b] = jnp.concatenate(parts, axis=0)
    highest[...] = jnp.full(highest.shape, masked_score, jnp.float32)
    acc[...] = jnp.zeros(acc.shape, jnp.float32)

    def process(source):
        for b in range(blocks):
            n = (b + 1) * sub
            keys_n = frames * n
            qi = lax.broadcasted_iota(jnp.int32, (rows, 1), 0) % q_rows
            q_at = (b * sub + qi % sub) * devices + (qi // sub) * seqs + my_seq
            ki = lax.broadcasted_iota(jnp.int32, (1, keys_n), 1)
            k_at = ki % n * devices + ki // n * seqs + source
            seen = k_at <= q_at
            ones = jnp.ones((keys_n, head), jnp.bfloat16)
            for h in range(kv_heads):
                k = kv[source, :, :n, h * head : (h + 1) * head].reshape(keys_n, head)
                v = kv[source, :, :n, (kv_heads + h) * head : (kv_heads + h + 1) * head]
                v = jnp.concatenate([v.reshape(keys_n, head), ones], axis=1)
                s = lax.dot_general(
                    qs[h, b], k, (((1,), (1,)), ((), ())), preferred_element_type=jnp.float32
                )
                s = jnp.where(seen, s, masked_score)
                m = highest[h, b]
                new = jnp.maximum(m, jnp.max(s, axis=1, keepdims=True))
                e = jnp.exp2(s - new).astype(jnp.bfloat16)
                acc[h, b] = acc[h, b] * jnp.exp2(m - new) + dot32(e, v)
                highest[h, b] = new

    def step(k, carry):
        pl.when((k > 0) & (k < relay.length))(lambda: relay.step(k))

        def one(i, c):
            crossed, side = i // 2, i % 2
            distance = k - crossed
            source = relay.a - distance + 2 * distance * side
            valid = (source >= 0) & (source < relay.length) & (distance >= 0)
            valid = valid & ((distance > 0) | (side == 0))

            @pl.when(valid)
            def _():
                if relay.breadth == 2:

                    @pl.when(crossed == 1)
                    def _():
                        relay.await_cross(source)

                row = relay.b + crossed * (1 - 2 * relay.b)
                process(source * relay.breadth + row)

            return c

        return lax.fori_loop(0, 2 * relay.breadth, one, carry)

    lax.fori_loop(0, relay.length + relay.breadth - 1, step, 0)
    for h in range(kv_heads):
        for b in range(blocks):
            out = (acc[h, b, :, :head] / acc[h, b, :, head:]).astype(jnp.bfloat16)
            for g in range(group):
                piece = out[g * q_rows : (g + 1) * q_rows].reshape(frames, sub, head)
                at = (h * group + g) * head
                heads_out[:, b * sub : (b + 1) * sub, at : at + head] = piece

    targets, sources = exchange_slots(me, frames)
    copies = []
    near = []
    for i, target in enumerate(ahead):
        near.append(
            remote(
                heads_out.at[target + 1 - 2 * (me % 2)],
                near_context.at[i],
                near_sems_a.at[i],
                near_sems_b.at[i],
                "frame",
                partner,
            )
        )
        near[-1].start()
    for d, target in enumerate(targets):
        copies.append(
            remote(
                heads_out.at[target],
                context.at[me],
                ctx_send.at[d],
                ctx_recv.at[d],
                "frame",
                target,
            )
        )
        copies[-1].start()
    keep_own = pltpu.make_async_copy(heads_out.at[me], context.at[me], local.at[0])
    keep_own.start()
    keep_tail.wait()
    rest.wait_recv()
    sent = []
    for i, target in enumerate(ahead):
        near[i].wait_recv()
        total = dot32(heads_out[target], wo_rest[0]) + dot32(near_context[i], wo_rest[1])
        shared[i] = total.astype(jnp.bfloat16)
        copy = remote(
            shared.at[i], arriving.at[i], part_send.at[i], part_recv.at[i], "frame", target
        )
        copy.start()
        sent.append(copy)
    keep_cut.wait()
    spread.forward()
    keep_own.wait()
    for d, source in enumerate(sources):
        ref = context.at[source]
        remote(ref, ref, ctx_send.at[d], ctx_recv.at[d], "frame", partner).wait_recv()
    spread.settle()
    wide = math.gcd(cut, 512)
    for c in range(cut // wide):
        total = dot32(context[0], wo_all[0, :, c * wide : (c + 1) * wide])
        for f in range(1, frames):
            total = total + dot32(context[f], wo_all[f, :, c * wide : (c + 1) * wide])
        mixed_ref[:, c * wide : (c + 1) * wide] = total.astype(mixed_ref.dtype)
    total = dot32(context[me], wo_rest[0]) + dot32(context[partner], wo_rest[1])
    for i in range(len(ahead)):
        ref = arriving.at[i]
        remote(ref, ref, part_send.at[i], part_recv.at[i], "frame", partner).wait_recv()
        total = total + arriving[i].astype(jnp.float32)
    mixed_ref[:, cut:] = total.astype(mixed_ref.dtype)
    rest.wait_send()
    spread.drain()
    for copy in copies + near + sent:
        copy.wait_send()
    relay.drain()


def attend(
    info, table, proj_w, proj_b, text, gain, wq, wk, wv, base_turns, seq_turns, wo
):
    frames, own_rows, model_width = text.shape
    width, kw = wq.shape[1], wk.shape[1]
    kv_heads = kw // HEAD_WIDTH
    group = width // kw
    group_rows = frames * own_rows
    block = math.gcd(model_width, 512)
    steps = model_width // block
    seqs = lax.axis_size("seq")
    depth, out_cols = wo.shape
    cut = ceil_to(out_cols * 5 // 8, 512) if frames <= 4 else out_cols // 4
    rest = out_cols - cut
    sub = math.gcd(own_rows, 32)
    blocks, rows = own_rows // sub, group * frames * sub
    head = HEAD_WIDTH
    others = max(1, frames // 2 - 1)
    chunks = 2
    dma = pltpu.SemaphoreType.DMA
    vmem = pl.BlockSpec(memory_space=pltpu.VMEM)
    anywhere = pl.BlockSpec(memory_space=pl.ANY)
    return pl.pallas_call(
        functools.partial(
            attend_kernel, count=chunks, kv_heads=kv_heads, group=group, sub=sub
        ),
        in_specs=[vmem] * 2
        + [anywhere, vmem, anywhere, vmem]
        + [anywhere] * 3
        + [anywhere, vmem, anywhere],
        out_specs=vmem,
        out_shape=jax.ShapeDtypeStruct((own_rows, out_cols), jnp.bfloat16),
        scratch_shapes=[
            pltpu.VMEM((steps, proj_w.shape[0], block), jnp.bfloat16),
            pltpu.VMEM((steps, frames, own_rows, block), jnp.bfloat16),
            pltpu.VMEM((group_rows, table.shape[1]), jnp.bfloat16),
            pltpu.VMEM((table.shape[1], frames * table.shape[2]), jnp.bfloat16),
            pltpu.VMEM((group_rows, 1), jnp.float32),
            pltpu.VMEM((group_rows, 1), jnp.float32),
            pltpu.VMEM(wk.shape, wk.dtype),
            pltpu.VMEM(wv.shape, wv.dtype),
            pltpu.VMEM(wq.shape, wq.dtype),
            pltpu.VMEM((2, group_rows, HEAD_WIDTH), jnp.float32),
            pltpu.VMEM((group_rows, max(width, 2 * kw)), jnp.float32),
            pltpu.VMEM((seqs, frames, own_rows, 2 * kw), jnp.bfloat16),
            pltpu.VMEM((kv_heads, blocks, rows, head), jnp.bfloat16),
            pltpu.VMEM((kv_heads, blocks, rows, 1), jnp.float32),
            pltpu.VMEM((kv_heads, blocks, rows, 2 * head), jnp.float32),
            pltpu.VMEM((frames, own_rows, width), jnp.bfloat16),
            pltpu.VMEM((frames, own_rows, width), jnp.bfloat16),
            pltpu.VMEM((others, own_rows, rest), jnp.bfloat16),
            pltpu.VMEM((others, own_rows, width), jnp.bfloat16),
            pltpu.VMEM((frames, depth, cut), jnp.bfloat16),
            pltpu.VMEM((2, depth, rest), jnp.bfloat16),
            pltpu.VMEM((others, own_rows, rest), jnp.bfloat16),
            dma((7,)),
            dma((frames - 1, 1)),
            dma((frames - 1, 1)),
            dma((2,)),
            dma((frames - 1,)),
            dma((frames - 1,)),
            dma((others,)),
            dma((others,)),
            dma((others,)),
            dma((others,)),
        ]
        + [dma((2, steps))]
        + relay_scratch(chunks),
        compiler_params=pltpu.CompilerParams(
            collective_id=3, has_side_effects=True, vmem_limit_bytes=63 * 1024 * 1024
        ),
        cost_estimate=pl.CostEstimate(
            flops=40_000_000_000, bytes_accessed=0, transcendentals=0
        ),
        name="attend",
    )(
        info,
        table,
        proj_w,
        proj_b.reshape(steps, 1, block),
        text,
        gain.reshape(steps, 1, block),
        wq,
        wk,
        wv,
        base_turns,
        seq_turns,
        wo,
    )


class SeqRelay:
    def __init__(self, x_ref, out_ref, sems, count, low=None, wide=None):
        seqs = lax.axis_size("seq")
        self.x, self.out, self.count = x_ref, out_ref, count
        self.send_r, self.recv_r, self.send_l, self.recv_l, self.send_y, self.recv_y = sems[:6]
        self.send_e, self.recv_e = sems[6:]
        self.depth = x_ref.shape[0] // count
        self.tail = () if low is None else (pl.ds(low, wide),)
        self.breadth = 2 if seqs % 2 == 0 else 1
        self.length = seqs // self.breadth
        self.me = lax.axis_index("seq")
        self.a, self.b = self.me // self.breadth, self.me % self.breadth
        self.across = self.a * self.breadth + (self.breadth - 1 - self.b)
        self.has_right, self.has_left = self.a + 1 < self.length, self.a > 0

    def greet(self, barrier):
        breadth = self.breadth
        pl.when(self.has_right)(lambda: greet(barrier, "seq", self.me + breadth))
        pl.when(self.has_left)(lambda: greet(barrier, "seq", self.me - breadth))
        if breadth == 2:
            greet(barrier, "seq", self.across)

    def peers(self):
        sides = self.has_right.astype(jnp.int32) + self.has_left.astype(jnp.int32)
        return sides + (self.breadth - 1)

    def cut(self, i):
        rows = pl.ds(i * self.depth, self.depth)
        return (rows, slice(None)) + self.tail if not self.tail else (rows,) + self.tail

    def slot(self, source, b, i):
        return self.out.at[(source * self.breadth + b,) + self.cut(i)]

    def own(self, i):
        return self.x.at[self.cut(i)]

    def shift(self, i, k, right, own=False):
        slot = self.slot(self.a - k if right else self.a + k, self.b, i)
        send, recv = (self.send_r, self.recv_r) if right else (self.send_l, self.recv_l)
        src = self.own(i) if own else slot
        target = self.me + self.breadth if right else self.me - self.breadth
        return remote(src, slot, send.at[i, k], recv.at[i, k], "seq", target)

    def cross(self, i, source, own):
        slot = self.slot(source, self.b, i)
        src = self.own(i) if own else slot
        return remote(src, slot, self.send_y.at[i, source], self.recv_y.at[i, source], "seq", self.across)

    def incoming(self, i, k, right):
        slot = self.slot(self.a - k if right else self.a + k, self.b, i)
        recv = self.recv_r if right else self.recv_l
        return remote(slot, slot, self.send_r.at[i, 0], recv.at[i, k - 1], "seq", self.across)

    def incoming_cross(self, i, source):
        slot = self.slot(source, self.breadth - 1 - self.b, i)
        return remote(slot, slot, self.send_r.at[i, 0], self.recv_y.at[i, source], "seq", self.across)

    def held(self, k, right):
        held = (self.a >= k) if right else (self.a + k < self.length)
        return held, held & (self.has_right if right else self.has_left)

    def first(self):
        for i in range(self.count):
            self.first_chunk(i)

    def first_chunk(self, i):
        for right in (True, False):
            pl.when(self.held(0, right)[1])(lambda: self.shift(i, 0, right, True).start())
        if self.breadth == 2:
            self.cross(i, self.a, True).start()

    def balanced(self):
        return self.breadth == 2 and self.length > 1

    def extra(self, right):
        source = 0 if right else self.length - 1
        slot = self.slot(source, self.breadth - 1 - self.b, self.count - 1)
        side = 0 if right else 1
        target = self.me + self.breadth if right else self.me - self.breadth
        return remote(slot, slot, self.send_e.at[side], self.recv_e.at[side], "seq", target)

    def at_end(self, right):
        return self.a == (0 if right else self.length - 1)

    def onward(self, i, source, start):
        if self.balanced() and i == self.count - 1:
            end = (source == 0) | (source == self.length - 1)
            pl.when(jnp.logical_not(end))(start)
        else:
            start()

    def step(self, k):
        for i in range(self.count):
            for right in (True, False):
                held, onward = self.held(k, right)
                source = self.a - k if right else self.a + k
                pl.when(held)(lambda: self.incoming(i, k, right).wait_recv())
                pl.when(onward)(lambda: self.shift(i, k, right).start())
                if self.breadth == 2:

                    @pl.when(held)
                    def _():
                        self.onward(i, source, lambda: self.cross(i, source, False).start())

        if self.balanced():
            for right in (True, False):
                distance = self.a if right else self.length - 1 - self.a

                @pl.when(distance == k - 1)
                def _():
                    @pl.when(distance == 0)
                    def _():
                        self.incoming_cross(self.count - 1, self.a).wait_recv()

                    pl.when(distance > 0)(lambda: self.extra(right).wait_recv())
                    self.extra(right).start()

    def await_cross(self, source):
        for i in range(self.count):
            if self.balanced() and i == self.count - 1:
                end = (source == 0) | (source == self.length - 1)
                pl.when(jnp.logical_not(end))(
                    lambda: self.incoming_cross(i, source).wait_recv()
                )
                for right in (True, False):
                    last = self.at_end(not right) & (source == (0 if right else self.length - 1))
                    pl.when(last)(lambda: self.extra(right).wait_recv())
            else:
                self.incoming_cross(i, source).wait_recv()

    def settle(self):
        if self.breadth == 2:
            for k in range(self.length):
                self.await_cross(k)

    def drain(self):
        for i in range(self.count):
            for k in range(self.length):
                for right in (True, False):
                    onward = self.held(k, right)[1]
                    pl.when(onward)(lambda: self.shift(i, k, right).wait_send())
                if self.breadth == 2:
                    if self.balanced() and i == self.count - 1:
                        end = k == 0 or k == self.length - 1
                        pl.when((self.a == k) | (not end))(
                            lambda: self.cross(i, k, False).wait_send()
                        )
                    else:
                        self.cross(i, k, False).wait_send()
        if self.balanced():
            for right in (True, False):
                far = self.at_end(not right)
                pl.when(jnp.logical_not(far))(lambda: self.extra(right).wait_send())


def per_device(
    vit_states,
    frame_slot,
    patch_count,
    vis_start,
    text_embed,
    vit_ln_gain,
    vit_ln_bias,
    vit_qkv_w,
    vit_qkv_b,
    vit_out_w,
    vit_out_b,
    proj_w,
    proj_b,
    attn_gain,
    wq,
    wk,
    wv,
    wo,
):
    frames_n = lax.axis_size("frame")
    seqs_n = lax.axis_size("seq")
    chips = frames_n // 2
    devices_n = frames_n * seqs_n
    me = lax.axis_index("frame")
    my_seq = lax.axis_index("seq")
    slots_held, frame_max, width_vit = vit_states.shape
    vis_max = frame_max // 4
    own_rows, model_width = text_embed.shape[0], text_embed.shape[2]
    head_size = width_vit // VHEADS
    my_heads = VHEADS // frames_n
    cols = width_vit // frames_n

    w_parts = [
        lax.dynamic_slice_in_dim(vit_qkv_w, i * width_vit + me * cols, cols, 1) for i in range(3)
    ]
    out_own = lax.dynamic_slice_in_dim(vit_out_w, me * cols, cols, 1)
    own_weights = jnp.concatenate(w_parts + [out_own], 1)
    params = jnp.concatenate([vit_ln_gain, vit_ln_bias, vit_qkv_b, vit_out_b]).reshape(1, -1)

    holder = frame_slot // slots_held
    holder_frame = holder // seqs_n
    pair_low = (holder_frame - holder_frame % 2) * seqs_n + holder % seqs_n
    pair_order = holder_frame % 2 * slots_held + frame_slot % slots_held
    same_pair = pair_low[:, None] == pair_low[None, :]
    earlier = pair_order[None, :] < pair_order[:, None]
    pair_rank = jnp.sum((same_pair & earlier).astype(jnp.int32), axis=1)
    source_frame = pair_low // seqs_n + pair_rank
    source_seq = pair_low % seqs_n
    entry = jnp.arange(2 + 2 * frames_n)[:, None]
    wanted = jnp.where(entry < 2, me - me % 2 + (me % 2 + entry) % 2, (entry - 2) % frames_n)
    chosen = (source_frame[None, :] == wanted) & (source_seq[None, :] == my_seq)
    kind = jnp.where(
        entry < 2,
        pair_order[None, :],
        jnp.where(entry < 2 + frames_n, patch_count[None, :], vis_start[None, :]),
    )
    facts = jnp.sum(jnp.where(chosen, kind, 0), axis=1)

    table, text_rows = vision(
        facts,
        own_weights,
        vit_states,
        text_embed.reshape(own_rows, model_width),
        params,
        cols,
        my_heads,
    )
    laps = vis_max // seqs_n
    group_rows = frames_n * own_rows
    row_ids = np.arange(group_rows)
    base = row_ids % own_rows * devices_n + row_ids // own_rows * seqs_n
    inverse = rope_theta ** (-np.arange(0, HEAD_WIDTH, 2) / HEAD_WIDTH)

    def turns(positions):
        angles = np.tile(positions[:, None] * inverse[None, :], (1, 2))
        return jnp.asarray(np.stack([np.cos(angles), np.sin(angles)]), jnp.float32)

    base_turns, seq_turns = turns(base), turns(np.arange(seqs_n))
    info = jnp.stack([vis_start, patch_count, (source_seq * frames_n + source_frame) * laps])
    mixed = attend(
        info,
        table,
        proj_w,
        proj_b,
        text_rows,
        attn_gain,
        wq,
        wk,
        wv,
        base_turns,
        seq_turns,
        wo,
    )
    return mixed.reshape(own_rows, 1, wo.shape[1])


def solution(mesh):
    return jax.shard_map(
        per_device,
        mesh=mesh,
        in_specs=(
            P(("frame", "seq"), None, None),
            P(),
            P(),
            P(),
            P(None, ("frame", "seq"), None),
            P(),
            P(),
            P("seq", None),
            P(),
            P("seq", None),
            P(),
            P(),
            P(),
            P(),
            P(None, "frame"),
            P(None, "frame"),
            P(None, "frame"),
            P("frame", None),
        ),
        out_specs=P(None, ("frame", "seq"), None),
        check_vma=False,
    )
```
